128 devices in a mesh: gx: 8 (over y, core), gy: 16 (over z, x).
Axes of the slice: x: 4, y: 4, z: 4, core: 2. Of those that a mesh axis runs over, the one named last changes fastest.
Arguments:
- forcing: float32 [16, 512, 2048], P(None, 'gy', 'gx'), may hold values from -6 to 6
- damping: float32 [16, 512, 2048], P(None, 'gy', 'gx'), may hold values from 0.5 to 4
- coupling: float32 [16, 16], replicated, may hold values from -1.5 to 1.5
- wind_lon: float32 [512, 2048], P('gy', 'gx'), may hold values from -0.5 to 0.5
- wind_lat: float32 [512, 2048], P('gy', 'gx'), may hold values from -0.5 to 0.5
Outputs:
- solution: float32 [16, 512, 2048], P(None, 'gy', 'gx')
- residual: float32 [16, 512, 2048], P(None, 'gy', 'gx')
The draws below stay inside these ranges and needn't reach their ends.
All inputs are finite; a program needn't handle non-finite values.
Results may differ from the reference program's by a relative error of at most 0.0003.
Values sent between devices are 32-bit elements; how exact they have to be, the bound alone decides.
A program may use at most 64 MiB of HBM per device.

```python
import math
import jax
import jax.numpy as jnp
from jax import lax

CH = 16
ITERS = 8
NLAT = 512
NLON = 2048


def block_scale(stream_key, dims, cuts, smallest, high):
    def one(position, parts):
        steps = jax.random.uniform(jax.random.fold_in(jax.random.fold_in(stream_key, 6), position), (parts,), jnp.float32, smallest / len(cuts), high / len(cuts))
        return jnp.repeat(jnp.exp(steps), dims[position] // parts).reshape((-1,) + (1,) * (len(dims) - position - 1))

    factor_of = one(*cuts[0])
    for cut in cuts[1:]:
        factor_of = factor_of * one(*cut)
    return factor_of


def scatter_about(own_key, extent, scale, limit, pieces=(), held_as=jnp.bfloat16):
    factor_of = block_scale(own_key, extent, pieces, -0.22, 0.18) if pieces else 1.0
    drawn = jax.random.normal(own_key, extent, jnp.float32) * scale * factor_of
    return jnp.minimum(jnp.maximum(drawn, -limit), limit).astype(held_as)


def setup_inputs(seed: int = 0) -> dict:
    seeds = jax.random.split(jax.random.key(seed), 6)
    return {
        "forcing": scatter_about(seeds[0], (CH, NLAT, NLON), 1.0, 6.0, ((1, 16), (2, 8)), jnp.float32),
        "damping": jnp.clip(jnp.exp(math.log(4.0) - 2.0794415 * jax.random.uniform(seeds[1], (CH, NLAT, NLON), jnp.float32) ** block_scale(seeds[1], (CH, NLAT, NLON), ((1, 16), (2, 8)), -0.2, 0.2)), 0.5, 4.0),
        "coupling": scatter_about(seeds[2], (CH, CH), CH ** -0.5, 1.5, (), jnp.float32),
        "wind_lon": jnp.clip(jax.random.uniform(seeds[3], (NLAT, NLON), jnp.float32, -0.5, 0.5) * block_scale(seeds[3], (NLAT, NLON), ((0, 16), (1, 8)), -0.4, 0.0), -0.5, 0.5),
        "wind_lat": jnp.clip(jax.random.uniform(seeds[4], (NLAT, NLON), jnp.float32, -0.5, 0.5) * block_scale(seeds[4], (NLAT, NLON), ((0, 16), (1, 8)), -0.4, 0.0), -0.5, 0.5),
    }


COUPLE = 0.25
DIFF_LAT = 0.5
DIFF_LON = 0.5
GUARD = 1.0

def apply_core(padded, damping, coupling, wind_lon, wind_lat, diffuse_lon):
    centre = padded[:, 2:-2, 2:-2]
    east_one = padded[:, 2:-2, 3:-1]
    west_one = padded[:, 2:-2, 1:-3]
    east_two = padded[:, 2:-2, 4:]
    west_two = padded[:, 2:-2, :-4]
    north_one = padded[:, 3:-1, 2:-2]
    south_one = padded[:, 1:-3, 2:-2]
    north_two = padded[:, 4:, 2:-2]
    south_two = padded[:, :-4, 2:-2]
    slope_lon = (8.0 * (east_one - west_one) - (east_two - west_two)) / 12.0
    slope_lat = (8.0 * (north_one - south_one) - (north_two - south_two)) / 12.0
    coupled = COUPLE * jnp.einsum('ij,jab->iab', coupling, centre, precision=lax.Precision.HIGHEST)
    return (1.0 + damping) * centre + coupled + diffuse_lon * (2.0 * centre - east_one - west_one) + DIFF_LAT * (2.0 * centre - north_one - south_one) + wind_lon * slope_lon + wind_lat * slope_lat

def lon_diffusion(row_pos, lat_total):
    phi = -math.pi / 2 + (row_pos + 0.5) * (math.pi / lat_total)
    return DIFF_LON / (jnp.cos(phi) ** 2 + 0.1)

def operate(source, damping, coupling, wind_lon, wind_lat):
    padded = jnp.pad(source, ((0, 0), (2, 2), (0, 0)))
    padded = jnp.concatenate([padded[:, :, -2:], padded, padded[:, :, :2]], axis=2)
    row_pos = jnp.arange(NLAT).astype(jnp.float32)
    diffuse = lon_diffusion(row_pos, NLAT)[:, None]
    return apply_core(padded, damping, coupling, wind_lon, wind_lat, diffuse)

def least_squares(heights, first):
    num_steps = heights.shape[1]
    target = jnp.zeros((num_steps + 1,), jnp.float32).at[0].set(first)
    rotated = heights
    cosines = []
    sines = []
    for column in range(num_steps):
        column_vec = rotated[:, column]
        for earlier in range(column):
            upper_val = column_vec[earlier]
            lower_val = column_vec[earlier + 1]
            column_vec = column_vec.at[earlier].set(cosines[earlier] * upper_val + sines[earlier] * lower_val)
            column_vec = column_vec.at[earlier + 1].set(-sines[earlier] * upper_val + cosines[earlier] * lower_val)
        upper_val = column_vec[column]
        lower_val = column_vec[column + 1]
        radius = jnp.sqrt(upper_val * upper_val + lower_val * lower_val)
        cosine = upper_val / radius
        sine_val = lower_val / radius
        column_vec = column_vec.at[column].set(radius).at[column + 1].set(0.0)
        rotated = rotated.at[:, column].set(column_vec)
        upper_val = target[column]
        lower_val = target[column + 1]
        target = target.at[column].set(cosine * upper_val + sine_val * lower_val)
        target = target.at[column + 1].set(-sine_val * upper_val + cosine * lower_val)
        cosines.append(cosine)
        sines.append(sine_val)
    weights = [None] * num_steps
    for column in reversed(range(num_steps)):
        partial_value = target[column]
        for later_col in range(column + 1, num_steps):
            partial_value = partial_value - rotated[column, later_col] * weights[later_col]
        weights[column] = partial_value / rotated[column, column]
    return weights

def reference(forcing, damping, coupling, wind_lon, wind_lat):
    scale_first = jnp.sqrt(jnp.sum(forcing * forcing) + GUARD)
    krylov = [forcing / scale_first]
    heights = jnp.zeros((ITERS + 1, ITERS), jnp.float32)
    for column in range(ITERS):
        applied = operate(krylov[column], damping, coupling, wind_lon, wind_lat)
        coeffs = jnp.stack([jnp.sum(vector * applied) for vector in krylov])
        for earlier in range(len(krylov)):
            applied = applied - coeffs[earlier] * krylov[earlier]
        subdiag = jnp.sqrt(jnp.sum(applied * applied) + GUARD)
        heights = heights.at[:column + 1, column].set(coeffs).at[column + 1, column].set(subdiag)
        if column + 1 < ITERS:
            krylov.append(applied / subdiag)
    weights = least_squares(heights, scale_first)
    solution = weights[0] * krylov[0]
    for column in range(1, ITERS):
        solution = solution + weights[column] * krylov[column]
    residual = forcing - operate(solution, damping, coupling, wind_lon, wind_lat)
    return (solution, residual)
```

```python
import functools
import math

import jax
import jax.numpy as jnp
from jax import lax
from jax.experimental import pallas as pl
from jax.experimental.pallas import tpu as pltpu
from jax.sharding import PartitionSpec as P

ITERS = 8
COUPLE = 0.25
DIFF_LAT = 0.5
DIFF_LON = 0.5
GUARD = 1.0
MESH = pl.DeviceIdType.MESH
HI = lax.Precision.HIGHEST

MIDDLE = 9.0
RADIUS = 6.0
WIDTH = 3.0
THETA = [MIDDLE + RADIUS * math.cos(math.pi * (2 * k + 1) / (2 * ITERS)) for k in (7, 0, 4, 2, 6, 1, 5, 3)]
PAIRS = [(k, i) for k in range(ITERS + 1) for i in range(k + 1)]
GROUP = 4
HALO = 2 * ITERS
HALF = 8
WINDOWS = 3


def apply_to(coords):
    out = [None] * (len(coords) + 1)
    for k, value in enumerate(coords):
        low = THETA[k] * value if k < ITERS else value
        out[k] = low if out[k] is None else out[k] + low
        out[k + 1] = WIDTH * value
    return out


def small_solve(gram):
    first = jnp.sqrt(gram[0][0] + GUARD)
    coords = [[1.0 / first]]
    images = [[gram[i][0] * coords[0][0] for i in range(ITERS + 1)]]
    heights = []
    for j in range(ITERS):
        moved = apply_to(coords[j])
        column = []
        for i in range(j + 1):
            column.append(functools.reduce(lambda a, b: a + b, [images[i][k] * moved[k] for k in range(j + 2)]))
        left = list(moved)
        for i in range(j + 1):
            for k in range(i + 1):
                left[k] = left[k] - column[i] * coords[i][k]
        image = [
            functools.reduce(lambda a, b: a + b, [gram[r][k] * left[k] for k in range(j + 2)])
            for r in range(ITERS + 1)
        ]
        norm_sq = functools.reduce(lambda a, b: a + b, [image[k] * left[k] for k in range(j + 2)])
        subdiag = jnp.sqrt(jnp.maximum(norm_sq, 0.0) + GUARD)
        column.append(subdiag)
        heights.append(column)
        inverse = 1.0 / subdiag
        coords.append([v * inverse for v in left])
        images.append([v * inverse for v in image])
    cosines, sines, target, rotated = [], [], [first], []
    for j in range(ITERS):
        column = list(heights[j])
        for e in range(j):
            upper, lower = column[e], column[e + 1]
            column[e] = cosines[e] * upper + sines[e] * lower
            column[e + 1] = cosines[e] * lower - sines[e] * upper
        upper, lower = column[j], column[j + 1]
        radius = jnp.sqrt(upper * upper + lower * lower)
        inverse = 1.0 / radius
        cosine, sine = upper * inverse, lower * inverse
        column[j] = radius
        kept = target[j]
        target[j] = cosine * kept
        target.append(-sine * kept)
        cosines.append(cosine)
        sines.append(sine)
        rotated.append(column)
    weights = [None] * ITERS
    for j in reversed(range(ITERS)):
        value = target[j]
        for later in range(j + 1, ITERS):
            value = value - rotated[later][j] * weights[later]
        weights[j] = value / rotated[j][j]
    answer = [None] * ITERS
    for j in range(ITERS):
        for k in range(j + 1):
            term = weights[j] * coords[j][k]
            answer[k] = term if answer[k] is None else answer[k] + term
    return answer, apply_to(answer)


def distance(n, o):
    return min(o, n - o)


def peers(nx, ny):
    inner = 4 if ny % 4 == 0 else 1
    offsets = [(a, b) for a in range(nx) for b in range(ny) if (a, b) != (0, 0)]

    def hops(offset):
        a, b = offset
        return distance(nx // 2 or 1, a // 2) + distance(inner, b % inner) + distance(ny // inner, b // inner)

    return sorted(offsets, key=lambda offset: (-hops(offset), offset))


def kernel(nx, ny, f_hbm, d_hbm, c_ref, wl_hbm, wa_hbm, sol_hbm, res_hbm,
           basis, diag, coef, kxs, block, band, own, near_lat, near_lon, own_w, near_lat_w, near_lon_w, corner_out, corner_in,
           gram_acc, mine, slots, splats, outs,
           load_sem, wind_sem, out_sem, lat_send, lat_recv, lon_send, lon_recv, cor_send, cor_recv, red_sem, known):
    channels, lat, lon = f_hbm.shape
    total = nx * ny
    f32, bf16 = jnp.float32, jnp.bfloat16
    ix, iy = lax.axis_index("gx"), lax.axis_index("gy")
    me = ix * ny + iy
    east, west = lax.rem(ix + 1, nx), lax.rem(ix + nx - 1, nx)
    scale = 1.0 / WIDTH
    size = GROUP * channels
    edge = HALO
    rows_all = lat + 2 * HALO

    winds = [pltpu.make_async_copy(wl_hbm, own_w.at[0], wind_sem.at[0]), pltpu.make_async_copy(wa_hbm, own_w.at[1], wind_sem.at[1])]
    batches = (lat // HALF - 1, 0, lat // HALF - 2, 1)
    for b in batches:
        for r in range(HALF * b, HALF * b + HALF):
            for q, src in enumerate((f_hbm, d_hbm)):
                pltpu.make_async_copy(src.at[:, r, :], own.at[r, pl.ds(q * channels, channels), :], load_sem.at[b]).start()
    for copy in winds:
        copy.start()

    barrier = pltpu.get_barrier_semaphore()

    def greet(sem, a, b):
        pl.semaphore_signal(sem, inc=1, device_id=(lax.rem(ix + a, nx), lax.rem(iy + b, ny)), device_id_type=MESH)

    greeted = [(1, 0), (nx - 1, 0), (0, 1), (0, ny - 1), (1, 1), (1, ny - 1), (nx - 1, 1), (nx - 1, ny - 1)]
    greeted += [(a, 0) for a in range(2, nx - 1)] + [(0, b) for b in range(2, ny - 1)]
    for a, b in greeted:
        greet(barrier, a, b)

    def spread(n):
        row = lax.broadcasted_iota(jnp.int32, (n, channels), 0)
        col = lax.broadcasted_iota(jnp.int32, (n, channels), 1)
        return jnp.where(lax.rem(row, channels) == col, 1.0, 0.0).astype(f32)

    wide = lax.dot_general(spread(size), c_ref[...], (((1,), (0,)), ((), ())), precision=HI, preferred_element_type=f32)
    wide = lax.dot_general(wide, spread(3 * size), (((1,), (1,)), ((), ())), precision=HI,
                           preferred_element_type=f32) * (COUPLE * scale)
    down = lax.broadcasted_iota(jnp.int32, (size, 3 * size), 0)
    across = lax.broadcasted_iota(jnp.int32, (size, 3 * size), 1)
    high = wide.astype(bf16).astype(f32)
    wide = jnp.where(across < 2 * size, high, wide - high)
    block[...] = jnp.where(down // channels == lax.rem(across, size) // channels, wide, 0.0).astype(bf16)
    down = lax.broadcasted_iota(jnp.int32, (256, 256), 0)
    across = lax.broadcasted_iota(jnp.int32, (256, 256), 1)
    shift = lax.rem(down, 128) - lax.rem(across, 128)
    sums = jnp.where((shift == 1) | (shift == -1), 1.0, 0.0)
    slopes = jnp.where(shift == 1, 8.0, 0.0) + jnp.where(shift == -1, -8.0, 0.0)
    slopes = slopes + jnp.where(shift == 2, -1.0, 0.0) + jnp.where(shift == -2, 1.0, 0.0)
    band[...] = jnp.where(across < 128, sums, slopes).astype(bf16)
    row_pos = (lax.broadcasted_iota(jnp.int32, (rows_all, 128), 0) + (iy * lat - edge)).astype(f32)
    phi = -math.pi / 2 + (row_pos + 0.5) * (math.pi / (lat * ny))
    kxs[...] = (DIFF_LON * scale) / (jnp.cos(phi) ** 2 + 0.1)

    @pl.when(iy == 0)
    def _():
        near_lat[0] = jnp.zeros(near_lat.shape[1:], f32)
        near_lat_w[0] = jnp.zeros(near_lat_w.shape[1:], f32)
        corner_in[0] = jnp.zeros(corner_in.shape[1:], f32)
        corner_in[1] = jnp.zeros(corner_in.shape[1:], f32)

    @pl.when(iy == ny - 1)
    def _():
        near_lat[1] = jnp.zeros(near_lat.shape[1:], f32)
        near_lat_w[1] = jnp.zeros(near_lat_w.shape[1:], f32)
        corner_in[2] = jnp.zeros(corner_in.shape[1:], f32)
        corner_in[3] = jnp.zeros(corner_in.shape[1:], f32)

    pl.semaphore_wait(barrier, len(greeted))

    def lat_copies(side, c):
        first = HALF * (1 - c) if side == 0 else HALF * c
        base = lat - HALO if side == 0 else 0
        to = (ix, iy + 1) if side == 0 else (ix, iy - 1)
        kept = (first, HALF, 0, 2 * channels)
        if c == 0:
            parts = [kept]
        elif side == 0:
            parts = [(first + 2, HALF - 2, 0, 2 * channels), (first, 2, 0, channels)]
        else:
            parts = [(first, HALF - 2, 0, 2 * channels), (first + HALF - 2, 2, 0, channels)]
        out = []
        for n, (start, count, sub, subs) in enumerate(parts):
            out.append(pltpu.make_async_remote_copy(
                src_ref=own.at[pl.ds(base + start, count), pl.ds(sub, subs), :],
                dst_ref=near_lat.at[side, pl.ds(start, count), pl.ds(sub, subs), :],
                send_sem=lat_send.at[side, c, n], recv_sem=lat_recv.at[side, c, n], device_id=to, device_id_type=MESH))
        out.append(pltpu.make_async_remote_copy(
            src_ref=own_w.at[:, pl.ds(base + first, HALF), :], dst_ref=near_lat_w.at[side, :, pl.ds(first, HALF), :],
            send_sem=lat_send.at[side, c, 2], recv_sem=lat_recv.at[side, c, 2], device_id=to, device_id_type=MESH))
        return out

    def corner_copy(side, ew, c):
        slot = 2 * side + ew
        tile = 1 - c if side == 0 else c
        return pltpu.make_async_remote_copy(
            src_ref=corner_out.at[slot, tile], dst_ref=corner_in.at[slot, tile],
            send_sem=cor_send.at[slot, c], recv_sem=cor_recv.at[slot, c],
            device_id=(east if ew == 0 else west, iy + 1 if side == 0 else iy - 1), device_id_type=MESH)

    def lon_copies(ew):
        cut = pl.ds(lon - 128, 128) if ew == 0 else pl.ds(0, 128)
        to = (east if ew == 0 else west, iy)
        return [
            pltpu.make_async_remote_copy(
                src_ref=own.at[:, :, cut], dst_ref=near_lon.at[ew], send_sem=lon_send.at[ew, 0], recv_sem=lon_recv.at[ew, 0],
                device_id=to, device_id_type=MESH),
            pltpu.make_async_remote_copy(
                src_ref=own_w.at[:, :, cut], dst_ref=near_lon_w.at[ew], send_sem=lon_send.at[ew, 1], recv_sem=lon_recv.at[ew, 1],
                device_id=to, device_id_type=MESH),
        ]

    def has(side):
        return iy < ny - 1 if side == 0 else iy > 0

    def from_side(side):
        return iy > 0 if side == 0 else iy < ny - 1

    lane = lax.broadcasted_iota(jnp.int32, (2 * channels, 128), 1)
    lane8 = lax.broadcasted_iota(jnp.int32, (8, 128), 1)

    def turn(x, n):
        n = n % 128
        return pltpu.roll(x, n, 1) if n else x

    def pack_corner(side, ew, c):
        slot = 2 * side + ew
        tile = 1 - c if side == 0 else c
        base = (lat - HALO if side == 0 else 0) + HALF * tile
        cut = slice(lon - 128, lon) if ew == 0 else slice(0, 128)
        start = 112 if ew == 0 else 0
        packed = turn(own[base, :, cut], -start)
        for j in range(1, HALF):
            packed = jnp.where((lane >= 16 * j) & (lane < 16 * j + 16), turn(own[base + j, :, cut], 16 * j - start), packed)
        corner_out[slot, tile, 0:2 * channels, :] = packed
        corner_out[slot, tile, 2 * channels:2 * channels + 8, :] = jnp.where(
            lane8 < 16, turn(own_w[0, base:base + 8, cut], -start), turn(own_w[1, base:base + 8, cut], 16 - start))

    def loaded(b):
        part = own.at[pl.ds(HALF * b, HALF)]
        pltpu.make_async_copy(part, part, load_sem.at[b]).wait()

    for copy in winds:
        copy.wait()
    for c in range(2):
        for side in range(2):
            loaded(batches[2 * c + side])

            @pl.when(has(side))
            def _():
                copies = lat_copies(side, c)
                copies[0].start()
                for ew in range(2):
                    pack_corner(side, ew, c)
                    corner_copy(side, ew, c).start()
                for copy in copies[1:]:
                    if copy is not None and not (c == 0 and copy is copies[0]):
                        copy.start()

    for ew in range(2):
        for copy in lon_copies(ew):
            copy.start()
    for b in range(1, ny):
        greet(known, 0, b)

    def place_coef(e0, wl, wa, inside):
        kx = kxs[pl.ds(e0, 8), :]
        for t in range(WINDOWS):
            cut = slice(128 * t, 128 * t + 128)
            l, a = wl[t] * (scale / 12.0), wa[t] * (scale / 12.0)
            planes = [-kx, l, 8.0 * a - DIFF_LAT * scale, -8.0 * a - DIFF_LAT * scale, a]
            for q, plane in enumerate(planes):
                if inside is not None:
                    plane = plane * inside
                for j in range(8):
                    coef[e0 + j, q:q + 1, cut] = plane[j:j + 1, :]

    def place_row(e, pieces):
        centre = (1.0 + 2.0 * DIFF_LAT) * scale - 2.0 * coef[e, 0:1, 0:128]
        for t in range(WINDOWS):
            cut = slice(128 * t, 128 * t + 128)
            basis[0, e, :, cut] = pieces[t][0:channels]
            diag[e, :, cut] = pieces[t][channels:] * scale + centre

    def cuts(lanes, a, b, w, e):
        return (turn(jnp.where(lanes >= 112, w, a), 16), turn(jnp.where(lanes >= 64, a, b), 64),
                turn(jnp.where(lanes >= 16, b, e), 112))

    for ew in range(2):
        for copy in lon_copies(ew):
            copy.wait_recv()
    for n in range(lat // 8):
        at = slice(8 * n, 8 * n + 8)
        wl, wa = (cuts(lane8, own_w[q, at, 0:128], own_w[q, at, 128:256], near_lon_w[0, q, at, :], near_lon_w[1, q, at, :])
                  for q in range(2))
        place_coef(edge + 8 * n, wl, wa, None)

    def place_own(r, _):
        place_row(edge + r, cuts(lane, own[r, :, 0:128], own[r, :, 128:256], near_lon[0, r], near_lon[1, r]))
        return 0

    lax.fori_loop(0, lat, place_own, 0)

    def place_halo(side, c):
        first = HALF * (1 - c) if side == 0 else HALF * c
        tile = 1 - c if side == 0 else c
        e0 = first if side == 0 else edge + lat + first
        inside = jnp.where(from_side(side), 1.0, 0.0).astype(f32)

        @pl.when(from_side(side))
        def _():
            for copy in lat_copies(side, c):
                copy.wait_recv()
            for ew in range(2):
                corner_copy(side, ew, c).wait_recv()

        def pair(q):
            a, b = near_lat_w[side, q, first:first + 8, 0:128], near_lat_w[side, q, first:first + 8, 128:256]
            w = corner_in[2 * side, tile, 2 * channels:2 * channels + 8, :]
            e = corner_in[2 * side + 1, tile, 2 * channels:2 * channels + 8, :]
            return (jnp.where(lane8 < 16, turn(w, -16 * q), turn(a, 16)), turn(jnp.where(lane8 >= 64, a, b), 64),
                    jnp.where(lane8 >= 112, turn(e, 112 - 16 * q), turn(b, 112)))

        place_coef(e0, pair(0), pair(1), inside)
        for j in range(HALF):
            a, b = near_lat[side, first + j, :, 0:128], near_lat[side, first + j, :, 128:256]
            w, e = corner_in[2 * side, tile, 0:2 * channels, :], corner_in[2 * side + 1, tile, 0:2 * channels, :]
            place_row(e0 + j, (
                jnp.where(lane < 16, turn(w, -16 * j), turn(a, 16)), turn(jnp.where(lane >= 64, a, b), 64),
                jnp.where(lane >= 112, turn(e, 112 - 16 * j), turn(b, 112))))

    def advance(k, starts):
        theta = jnp.float32(THETA[0] * scale)
        for i in range(1, ITERS):
            theta = jnp.where(k == i, jnp.float32(THETA[i] * scale), theta)
        for e0 in starts:
            for g in range(HALF // GROUP):
                picked = [e0 + GROUP * g + j for j in range(GROUP)]
                stack = jnp.concatenate([basis[k, e] for e in picked], axis=0)
                high = stack.astype(bf16)
                low = (stack - high.astype(f32)).astype(bf16)
                mixed = lax.dot_general(block[...], jnp.concatenate([high, low, high], axis=0), (((1,), (0,)), ((), ())),
                                        preferred_element_type=f32)
                sides = jnp.concatenate(
                    [jnp.concatenate([high[:, 128 * t:128 * t + 128], low[:, 128 * t:128 * t + 128]], axis=1)
                     for t in range(WINDOWS)], axis=0)
                moved = lax.dot_general(sides, band[...], (((1,), (0,)), ((), ())), preferred_element_type=f32)
                for j, e in enumerate(picked):
                    for t in range(WINDOWS):
                        cut = slice(128 * t, 128 * t + 128)
                        at = slice(size * t + channels * j, size * t + channels * (j + 1))

                        def weight(q):
                            return coef[e, q:q + 1, cut]

                        value = (diag[e, :, cut] - theta) * basis[k, e, :, cut] + mixed[channels * j:channels * (j + 1), cut]
                        value = value + (coef[e, 0:1, 0:128] * moved[at, 0:128] + weight(1) * moved[at, 128:256])
                        value = value + weight(2) * basis[k, e + 1, :, cut] + weight(3) * basis[k, e - 1, :, cut]
                        value = value + weight(4) * (basis[k, e - 2, :, cut] - basis[k, e + 2, :, cut])
                        basis[k + 1, e, :, cut] = value

    def interior(k, _):
        def some(n, _):
            advance(k, (edge + 2 + 2 * k + HALF * n, edge + lat - 2 - HALF - 2 * k - HALF * n))
            return 0

        lax.fori_loop(0, jnp.where(k < 3, 2, 1), some, 0)
        return 0

    def dots(lo, hi, spans):
        pairs = [(k, i) for k, i in PAIRS if lo <= k <= hi]

        def one(t, _):
            cut = pl.ds(pl.multiple_of(t * 128, 128), 128)
            acc = (jnp.zeros((8, 128), f32),) * len(pairs)
            for start, stop in spans:
                def part(e, acc):
                    acc = list(acc)
                    for h in range(channels // 8):
                        x = [basis[k, e, 8 * h:8 * h + 8, cut] for k in range(hi + 1)]
                        for n, (k, i) in enumerate(pairs):
                            acc[n] = acc[n] + x[k] * x[i]
                    return tuple(acc)

                acc = lax.fori_loop(start, stop, part, acc)
            low = jnp.where(t == 1, 32, 16)
            kept = (lane8 >= low) & (lane8 < 128 - low)
            for n, (k, i) in enumerate(pairs):
                at = k * (k + 1) // 2 + i
                gram_acc[at] = gram_acc[at] + jnp.where(kept, acc[n], 0.0)
            return 0

        lax.fori_loop(0, WINDOWS, one, 0)

    gram_acc[...] = jnp.zeros(gram_acc.shape, f32)
    lax.fori_loop(0, ITERS - 1, interior, 0)
    ready = ITERS // 2
    for c in range(2):
        for side in range(2):
            place_halo(side, c)

        def wedge(k, _):
            low = edge - HALF * (c + 1) + 2 + 2 * k
            advance(k, (low, rows_all - HALF - low))
            return 0

        lax.fori_loop(0, ITERS, wedge, 0)
        if c == 0:
            dots(0, ready, ((edge, edge + lat),))
            dots(ready + 1, ITERS, ((edge + HALF, edge + lat - HALF),))
    dots(ready + 1, ITERS, ((edge, edge + HALF), (edge + lat - HALF, edge + lat)))

    pl.semaphore_wait(known, ny - 1)
    sums = jnp.concatenate(
        [jnp.sum(gram_acc[n], axis=0, keepdims=True) for n in range(len(PAIRS))]
        + [jnp.zeros((128 - len(PAIRS), 128), f32)], axis=0)
    flat = lax.dot_general(jnp.ones((8, 128), f32), sums, (((1,), (1,)), ((), ())), precision=HI,
                           preferred_element_type=f32)
    mine[...] = flat[0:1, :]
    slots[total - 1] = flat[0:1, :]

    for n, (a, b) in enumerate(peers(nx, ny)):
        pltpu.make_async_remote_copy(
            src_ref=mine, dst_ref=slots.at[n], send_sem=red_sem.at[0], recv_sem=red_sem.at[1],
            device_id=(lax.rem(ix + a, nx), lax.rem(iy + b, ny)), device_id_type=MESH).start()
    arrived = slots.at[pl.ds(0, total - 1)]
    pltpu.make_async_copy(arrived, arrived, red_sem.at[1]).wait()
    pltpu.make_async_copy(arrived, arrived, red_sem.at[0]).wait()
    parts = [slots[n] for n in range(4)]
    for n in range(4, total):
        parts[n % 4] = parts[n % 4] + slots[n]
    whole = (parts[0] + parts[1]) + (parts[2] + parts[3])
    gram = [[None] * (ITERS + 1) for _ in range(ITERS + 1)]
    for n, (k, i) in enumerate(PAIRS):
        gram[k][i] = gram[i][k] = jnp.broadcast_to(whole[:, n:n + 1], (8, 128))
    answer, applied = small_solve(gram)
    for k in range(ITERS):
        splats[k] = answer[k]
    for k in range(ITERS + 1):
        splats[ITERS + k] = applied[k]

    def finish(r, _):
        for h in range(channels // 8):
            sub = slice(8 * h, 8 * h + 8)
            best, rest = [], []
            for t in range(WINDOWS):
                cut = slice(128 * t, 128 * t + 128)
                x = basis[0, edge + r, sub, cut]
                up = splats[0] * x
                down = x - splats[ITERS] * x
                for k in range(1, ITERS + 1):
                    x = basis[k, edge + r, sub, cut]
                    if k < ITERS:
                        up = up + splats[k] * x
                    down = down - splats[ITERS + k] * x
                best.append(up)
                rest.append(down)
            for q, (a, b, c) in enumerate((best, rest)):
                b = turn(b, 64)
                outs[q, r, sub, 0:128] = jnp.where(lane8 < 96, turn(a, 112), b)
                outs[q, r, sub, 128:256] = jnp.where(lane8 < 32, b, turn(c, 16))
        return 0

    lax.fori_loop(0, lat, finish, 0)
    for c in range(channels):
        for q, dst in enumerate((sol_hbm, res_hbm)):
            pltpu.make_async_copy(outs.at[q, :, c, :], dst.at[c], out_sem.at[q]).start()
    for ew in range(2):
        for copy in lon_copies(ew):
            copy.wait_send()
    for side in range(2):
        @pl.when(has(side))
        def _():
            for c in range(2):
                for copy in lat_copies(side, c):
                    copy.wait_send()
                for ew in range(2):
                    corner_copy(side, ew, c).wait_send()
    for q, dst in enumerate((sol_hbm, res_hbm)):
        pltpu.make_async_copy(dst, dst, out_sem.at[q]).wait()


def solution(mesh):
    nx, ny = mesh.shape["gx"], mesh.shape["gy"]

    def per_device(forcing, damping, coupling, wind_lon, wind_lat):
        channels, lat, lon = forcing.shape
        f32 = jnp.float32
        vmem = pl.BlockSpec(memory_space=pltpu.VMEM)
        hbm = pl.BlockSpec(memory_space=pl.ANY)
        dma = pltpu.SemaphoreType.DMA
        shape = jax.ShapeDtypeStruct((channels, lat, lon), f32)
        rows_all, lanes = lat + 2 * HALO, 128 * WINDOWS
        packed = 2 * channels + 8
        return pl.pallas_call(
            functools.partial(kernel, nx, ny),
            out_shape=(shape, shape),
            in_specs=[hbm, hbm, vmem, hbm, hbm],
            out_specs=(hbm, hbm),
            scratch_shapes=[
                pltpu.VMEM((ITERS + 1, rows_all, channels, lanes), f32),
                pltpu.VMEM((rows_all, channels, lanes), f32),
                pltpu.VMEM((rows_all, 8, lanes), f32),
                pltpu.VMEM((rows_all, 128), f32),
                pltpu.VMEM((GROUP * channels, 3 * GROUP * channels), jnp.bfloat16),
                pltpu.VMEM((256, 256), jnp.bfloat16),
                pltpu.VMEM((lat, 2 * channels, lon), f32),
                pltpu.VMEM((2, HALO, 2 * channels, lon), f32),
                pltpu.VMEM((2, lat, 2 * channels, 128), f32),
                pltpu.VMEM((2, lat, lon), f32),
                pltpu.VMEM((2, 2, HALO, lon), f32),
                pltpu.VMEM((2, 2, lat, 128), f32),
                pltpu.VMEM((4, 2, packed, 128), f32),
                pltpu.VMEM((4, 2, packed, 128), f32),
                pltpu.VMEM((len(PAIRS), 8, 128), f32),
                pltpu.VMEM((1, 128), f32),
                pltpu.VMEM((nx * ny, 1, 128), f32),
                pltpu.VMEM((2 * ITERS + 1, 8, 128), f32),
                pltpu.VMEM((2, lat, channels, lon), f32),
                dma((lat // HALF,)), dma((2,)), dma((2,)),
                dma((2, 2, 3)), dma((2, 2, 3)), dma((2, 2)), dma((2, 2)), dma((4, 2)), dma((4, 2)), dma((2,)),
                pltpu.SemaphoreType.REGULAR,
            ],
            compiler_params=pltpu.CompilerParams(
                collective_id=0, has_side_effects=True, vmem_limit_bytes=63 * 1024 * 1024),
        )(forcing, damping, coupling, wind_lon, wind_lat)

    return jax.shard_map(
        per_device,
        mesh=mesh,
        in_specs=(P(None, "gy", "gx"), P(None, "gy", "gx"), P(), P("gy", "gx"), P("gy", "gx")),
        out_specs=(P(None, "gy", "gx"), P(None, "gy", "gx")),
        check_vma=False,
    )
```

```python
import functools
import math

import jax
import jax.numpy as jnp
from jax import lax
from jax.experimental import pallas as pl
from jax.experimental.pallas import tpu as pltpu
from jax.sharding import PartitionSpec as P

ITERS = 8
COUPLE = 0.25
DIFF_LAT = 0.5
DIFF_LON = 0.5
GUARD = 1.0
MESH = pl.DeviceIdType.MESH
HI = lax.Precision.HIGHEST

MIDDLE = 9.0
RADIUS = 6.0
WIDTH = 3.0
THETA = [MIDDLE + RADIUS * math.cos(math.pi * (2 * k + 1) / (2 * ITERS)) for k in (7, 0, 4, 2, 6, 1, 5, 3)]
PAIRS = [(k, i) for k in range(ITERS + 1) for i in range(k + 1)]
GROUP = 4
HALO = 2 * ITERS
HALF = 8
WINDOWS = 3


def apply_to(coords):
    out = [None] * (len(coords) + 1)
    for k, value in enumerate(coords):
        low = THETA[k] * value if k < ITERS else value
        out[k] = low if out[k] is None else out[k] + low
        out[k + 1] = WIDTH * value
    return out


def small_solve(gram):
    first = jnp.sqrt(gram[0][0] + GUARD)
    coords = [[1.0 / first]]
    images = [[gram[i][0] * coords[0][0] for i in range(ITERS + 1)]]
    heights = []
    for j in range(ITERS):
        moved = apply_to(coords[j])
        column = []
        for i in range(j + 1):
            column.append(functools.reduce(lambda a, b: a + b, [images[i][k] * moved[k] for k in range(j + 2)]))
        left = list(moved)
        for i in range(j + 1):
            for k in range(i + 1):
                left[k] = left[k] - column[i] * coords[i][k]
        image = [
            functools.reduce(lambda a, b: a + b, [gram[r][k] * left[k] for k in range(j + 2)])
            for r in range(ITERS + 1)
        ]
        norm_sq = functools.reduce(lambda a, b: a + b, [image[k] * left[k] for k in range(j + 2)])
        subdiag = jnp.sqrt(jnp.maximum(norm_sq, 0.0) + GUARD)
        column.append(subdiag)
        heights.append(column)
        inverse = 1.0 / subdiag
        coords.append([v * inverse for v in left])
        images.append([v * inverse for v in image])
    cosines, sines, target, rotated = [], [], [first], []
    for j in range(ITERS):
        column = list(heights[j])
        for e in range(j):
            upper, lower = column[e], column[e + 1]
            column[e] = cosines[e] * upper + sines[e] * lower
            column[e + 1] = cosines[e] * lower - sines[e] * upper
        upper, lower = column[j], column[j + 1]
        radius = jnp.sqrt(upper * upper + lower * lower)
        inverse = 1.0 / radius
        cosine, sine = upper * inverse, lower * inverse
        column[j] = radius
        kept = target[j]
        target[j] = cosine * kept
        target.append(-sine * kept)
        cosines.append(cosine)
        sines.append(sine)
        rotated.append(column)
    weights = [None] * ITERS
    for j in reversed(range(ITERS)):
        value = target[j]
        for later in range(j + 1, ITERS):
            value = value - rotated[later][j] * weights[later]
        weights[j] = value / rotated[j][j]
    answer = [None] * ITERS
    for j in range(ITERS):
        for k in range(j + 1):
            term = weights[j] * coords[j][k]
            answer[k] = term if answer[k] is None else answer[k] + term
    return answer, apply_to(answer)


def distance(n, o):
    return min(o, n - o)


def peers(nx, ny):
    inner = 4 if ny % 4 == 0 else 1
    offsets = [(a, b) for a in range(nx) for b in range(ny) if (a, b) != (0, 0)]

    def hops(offset):
        a, b = offset
        return distance(nx // 2 or 1, a // 2) + distance(inner, b % inner) + distance(ny // inner, b // inner)

    return sorted(offsets, key=lambda offset: (-hops(offset), offset))


def kernel(nx, ny, f_hbm, d_hbm, c_ref, wl_hbm, wa_hbm, sol_hbm, res_hbm,
           even, odd, diag, coef, kxs, block, band, own, near_lat, own_w, near_lat_w, packed, near_lon, near_corner,
           gram_acc, mine, slots, splats, outs,
           load_sem, wind_sem, out_sem, lat_send, lat_recv, lon_send, lon_recv, cor_send, cor_recv, red_sem, known):
    channels, lat, lon = f_hbm.shape
    both = 2 * channels
    total = nx * ny
    f32, bf16 = jnp.float32, jnp.bfloat16
    ix, iy = lax.axis_index("gx"), lax.axis_index("gy")
    east, west = lax.rem(ix + 1, nx), lax.rem(ix + nx - 1, nx)
    scale = 1.0 / WIDTH
    size = GROUP * channels
    edge = HALO
    rows_all = lat + 2 * HALO
    tiles = lat // HALF

    def field(k):
        return even.at[k // 2] if k % 2 == 0 else odd.at[k // 2]

    barrier = pltpu.get_barrier_semaphore()

    def greet(sem, a, b):
        pl.semaphore_signal(sem, inc=1, device_id=(lax.rem(ix + a, nx), lax.rem(iy + b, ny)), device_id_type=MESH)

    greeted = [(1, 1), (1, ny - 1), (nx - 1, 1), (nx - 1, ny - 1), (0, 1), (0, ny - 1), (1, 0), (nx - 1, 0)]
    greeted += [(a, 0) for a in range(2, nx - 1)] + [(0, b) for b in range(2, ny - 1)]
    for a, b in greeted:
        greet(barrier, a, b)

    winds = [pltpu.make_async_copy(wl_hbm, own_w.at[0], wind_sem.at[0]), pltpu.make_async_copy(wa_hbm, own_w.at[1], wind_sem.at[1])]
    for copy in winds:
        copy.start()
    for c in range(channels):
        for q, src in enumerate((f_hbm, d_hbm)):
            pltpu.make_async_copy(src.at[c], own.at[:, q * channels + c, :], load_sem.at[q]).start()

    def spread(n):
        row = lax.broadcasted_iota(jnp.int32, (n, channels), 0)
        col = lax.broadcasted_iota(jnp.int32, (n, channels), 1)
        return jnp.where(lax.rem(row, channels) == col, 1.0, 0.0).astype(f32)

    wide = lax.dot_general(spread(size), c_ref[...], (((1,), (0,)), ((), ())), precision=HI, preferred_element_type=f32)
    wide = lax.dot_general(wide, spread(3 * size), (((1,), (1,)), ((), ())), precision=HI,
                           preferred_element_type=f32) * (COUPLE * scale)
    down = lax.broadcasted_iota(jnp.int32, (size, 3 * size), 0)
    across = lax.broadcasted_iota(jnp.int32, (size, 3 * size), 1)
    high = wide.astype(bf16).astype(f32)
    wide = jnp.where(across < 2 * size, high, wide - high)
    block[...] = jnp.where(down // channels == lax.rem(across, size) // channels, wide, 0.0).astype(bf16)
    down = lax.broadcasted_iota(jnp.int32, (256, 256), 0)
    across = lax.broadcasted_iota(jnp.int32, (256, 256), 1)
    shift = lax.rem(down, 128) - lax.rem(across, 128)
    sums = jnp.where((shift == 1) | (shift == -1), 1.0, 0.0)
    slopes = jnp.where(shift == 1, 8.0, 0.0) + jnp.where(shift == -1, -8.0, 0.0)
    slopes = slopes + jnp.where(shift == 2, -1.0, 0.0) + jnp.where(shift == -2, 1.0, 0.0)
    band[...] = jnp.where(across < 128, sums, slopes).astype(bf16)
    row_pos = (lax.broadcasted_iota(jnp.int32, (rows_all, 128), 0) + (iy * lat - edge)).astype(f32)
    phi = -math.pi / 2 + (row_pos + 0.5) * (math.pi / (lat * ny))
    kxs[...] = (DIFF_LON * scale) / (jnp.cos(phi) ** 2 + 0.1)
    gram_acc[...] = jnp.zeros(gram_acc.shape, f32)

    @pl.when(iy == 0)
    def _():
        near_lat[0] = jnp.zeros(near_lat.shape[1:], f32)
        near_lat_w[0] = jnp.zeros(near_lat_w.shape[1:], f32)
        near_corner[0] = jnp.zeros(near_corner.shape[1:], f32)
        near_corner[1] = jnp.zeros(near_corner.shape[1:], f32)

    @pl.when(iy == ny - 1)
    def _():
        near_lat[1] = jnp.zeros(near_lat.shape[1:], f32)
        near_lat_w[1] = jnp.zeros(near_lat_w.shape[1:], f32)
        near_corner[2] = jnp.zeros(near_corner.shape[1:], f32)
        near_corner[3] = jnp.zeros(near_corner.shape[1:], f32)

    def lat_copies(side, c):
        first = HALF * (1 - c) if side == 0 else HALF * c
        base = lat - HALO if side == 0 else 0
        to = (ix, iy + 1) if side == 0 else (ix, iy - 1)
        if c == 0:
            parts = [(first, HALF, 0, both)]
        elif side == 0:
            parts = [(first + 2, HALF - 2, 0, both), (first, 2, 0, channels)]
        else:
            parts = [(first, HALF - 2, 0, both), (first + HALF - 2, 2, 0, channels)]
        out = []
        for n, (start, count, sub, subs) in enumerate(parts):
            out.append(pltpu.make_async_remote_copy(
                src_ref=own.at[pl.ds(base + start, count), pl.ds(sub, subs), :],
                dst_ref=near_lat.at[side, pl.ds(start, count), pl.ds(sub, subs), :],
                send_sem=lat_send.at[side, c, n], recv_sem=lat_recv.at[side, c, n], device_id=to, device_id_type=MESH))
        out.append(pltpu.make_async_remote_copy(
            src_ref=own_w.at[:, pl.ds(base + first, HALF), :], dst_ref=near_lat_w.at[side, :, pl.ds(first, HALF), :],
            send_sem=lat_send.at[side, c, 2], recv_sem=lat_recv.at[side, c, 2], device_id=to, device_id_type=MESH))
        return out

    def tile_of(side, c):
        return 1 - c if side == 0 else c

    def corner_copy(side, ew, c):
        slot, tile = 2 * side + ew, tile_of(side, c)
        return pltpu.make_async_remote_copy(
            src_ref=packed.at[ew, tile + (tiles - 2 if side == 0 else 0)], dst_ref=near_corner.at[slot, tile],
            send_sem=cor_send.at[slot, c], recv_sem=cor_recv.at[slot, c],
            device_id=(east if ew == 0 else west, iy + 1 if side == 0 else iy - 1), device_id_type=MESH)

    def lon_copy(ew):
        return pltpu.make_async_remote_copy(
            src_ref=packed.at[ew], dst_ref=near_lon.at[ew], send_sem=lon_send.at[ew], recv_sem=lon_recv.at[ew],
            device_id=(east if ew == 0 else west, iy), device_id_type=MESH)

    def has(side):
        return iy < ny - 1 if side == 0 else iy > 0

    def from_side(side):
        return iy > 0 if side == 0 else iy < ny - 1

    lane = lax.broadcasted_iota(jnp.int32, (both, 128), 1)
    lane8 = lax.broadcasted_iota(jnp.int32, (8, 128), 1)

    def turn(x, n):
        n = n % 128
        return pltpu.roll(x, n, 1) if n else x

    def pack(n, _):
        for ew in range(2):
            cut = slice(lon - 128, lon) if ew == 0 else slice(0, 128)
            start = 112 if ew == 0 else 0
            base = HALF * n
            strip = turn(own[base, :, cut], -start)
            for j in range(1, HALF):
                strip = jnp.where((lane >= 16 * j) & (lane < 16 * j + 16), turn(own[base + j, :, cut], 16 * j - start), strip)
            packed[ew, n, 0:both, :] = strip
            rows = pl.ds(pl.multiple_of(base, 8), 8)
            packed[ew, n, both:both + 8, :] = jnp.where(
                lane8 < 16, turn(own_w[0, rows, cut], -start), turn(own_w[1, rows, cut], 16 - start))
        return 0

    def place_coef(e0, wl, wa, inside, chosen):
        kx = kxs[pl.ds(e0, 8), :]
        for t in chosen:
            cut = slice(128 * t, 128 * t + 128)
            l, a = wl[t] * (scale / 12.0), wa[t] * (scale / 12.0)
            planes = [-kx, l, 8.0 * a - DIFF_LAT * scale, -8.0 * a - DIFF_LAT * scale, a]
            for q, plane in enumerate(planes):
                if q == 0 and t != 1:
                    continue
                if inside is not None:
                    plane = plane * inside
                for j in range(8):
                    coef[e0 + j, q:q + 1, cut] = plane[j:j + 1, :]

    def centre(e):
        return (1.0 + 2.0 * DIFF_LAT) * scale - 2.0 * coef[e, 0:1, 128:256]

    def place_own(n, _):
        base = HALF * n
        rows = pl.ds(pl.multiple_of(base, 8), 8)
        wl, wa = ([None, turn(jnp.where(lane8 >= 64, own_w[q, rows, 0:128], own_w[q, rows, 128:256]), 64), None] for q in range(2))
        place_coef(pl.multiple_of(edge + base, 8), wl, wa, None, (1,))
        for j in range(HALF):
            r = base + j
            e = edge + r
            a, b = own[r, :, 0:128], own[r, :, 128:256]
            middle = centre(e)
            for t, piece in enumerate((turn(a, 16), turn(jnp.where(lane >= 64, a, b), 64), turn(b, 112))):
                cut = slice(128 * t, 128 * t + 128)
                even[0, e, :, cut] = piece[0:channels]
                diag[e, :, cut] = piece[channels:] * scale + middle
        return 0

    def place_lon(n, _):
        base = HALF * n
        rows = pl.ds(pl.multiple_of(base, 8), 8)
        w, e = near_lon[0, n, both:both + 8, :], near_lon[1, n, both:both + 8, :]
        wl, wa = ([jnp.where(lane8 < 16, turn(w, -16 * q), turn(own_w[q, rows, 0:128], 16)), None,
                   jnp.where(lane8 >= 112, turn(e, 112 - 16 * q), turn(own_w[q, rows, 128:256], 112))] for q in range(2))
        place_coef(pl.multiple_of(edge + base, 8), wl, wa, None, (0, 2))
        w, e = near_lon[0, n, 0:both, :], near_lon[1, n, 0:both, :]
        for j in range(HALF):
            r = edge + base + j
            middle = centre(r)
            for cut, keep, piece in ((slice(0, 128), lane < 16, turn(w, -16 * j)), (slice(256, 384), lane >= 112, turn(e, 112 - 16 * j))):
                even[0, r, :, cut] = jnp.where(keep[0:channels], piece[0:channels], even[0, r, :, cut])
                diag[r, :, cut] = jnp.where(keep[0:channels], piece[channels:] * scale + middle, diag[r, :, cut])
        return 0

    def place_halo(side, c):
        first = HALF * (1 - c) if side == 0 else HALF * c
        tile = tile_of(side, c)
        e0 = first if side == 0 else edge + lat + first
        inside = jnp.where(from_side(side), 1.0, 0.0).astype(f32)

        @pl.when(from_side(side))
        def _():
            for copy in lat_copies(side, c):
                copy.wait_recv()
            for ew in range(2):
                corner_copy(side, ew, c).wait_recv()

        def three(a, b, w, e, lanes, at):
            return (jnp.where(lanes < 16, turn(w, -at), turn(a, 16)), turn(jnp.where(lanes >= 64, a, b), 64),
                    jnp.where(lanes >= 112, turn(e, 112 - at), turn(b, 112)))

        west_strip, east_strip = near_corner.at[2 * side, tile], near_corner.at[2 * side + 1, tile]
        span = slice(first, first + 8)
        wl, wa = (three(near_lat_w[side, q, span, 0:128], near_lat_w[side, q, span, 128:256],
                        west_strip[both:both + 8, :], east_strip[both:both + 8, :], lane8, 16 * q) for q in range(2))
        place_coef(e0, wl, wa, inside, range(WINDOWS))
        for j in range(HALF):
            middle = centre(e0 + j)
            pieces = three(near_lat[side, first + j, :, 0:128], near_lat[side, first + j, :, 128:256],
                           west_strip[0:both, :], east_strip[0:both, :], lane, 16 * j)
            for t, piece in enumerate(pieces):
                cut = slice(128 * t, 128 * t + 128)
                even[0, e0 + j, :, cut] = piece[0:channels]
                diag[e0 + j, :, cut] = piece[channels:] * scale + middle

    def shift_of(k):
        theta = jnp.float32(THETA[0] * scale)
        for i in range(1, ITERS):
            theta = jnp.where(k == i, jnp.float32(THETA[i] * scale), theta)
        return theta

    def advance(src, dst, theta, starts):
        groups = [[e0 + GROUP * g + j for j in range(GROUP)] for e0 in starts for g in range(HALF // GROUP)]
        mixed, moved = [], []
        for picked in groups:
            stack = jnp.concatenate([src[e] for e in picked], axis=0)
            high = stack.astype(bf16)
            low = (stack - high.astype(f32)).astype(bf16)
            mixed.append(lax.dot_general(block[...], jnp.concatenate([high, low, high], axis=0), (((1,), (0,)), ((), ())),
                                         preferred_element_type=f32))
            sides = jnp.concatenate(
                [jnp.concatenate([high[:, 128 * t:128 * t + 128], low[:, 128 * t:128 * t + 128]], axis=1)
                 for t in range(WINDOWS)], axis=0)
            moved.append(lax.dot_general(sides, band[...], (((1,), (0,)), ((), ())), preferred_element_type=f32))
        for g, picked in enumerate(groups):
            for j, e in enumerate(picked):
                for t in range(WINDOWS):
                    cut = slice(128 * t, 128 * t + 128)
                    at = slice(size * t + channels * j, size * t + channels * (j + 1))

                    def weight(q):
                        return coef[e, q:q + 1, cut]

                    value = (diag[e, :, cut] - theta) * src[e, :, cut] + mixed[g][channels * j:channels * (j + 1), cut]
                    value = value + (coef[e, 0:1, 128:256] * moved[g][at, 0:128] + weight(1) * moved[g][at, 128:256])
                    value = value + weight(2) * src[e + 1, :, cut] + weight(3) * src[e - 1, :, cut]
                    dst[e, :, cut] = value + weight(4) * (src[e - 2, :, cut] - src[e + 2, :, cut])

    def two_levels(some):
        def run(n, _):
            some(2 * n, even.at[n], odd.at[n])
            some(2 * n + 1, odd.at[n], even.at[n + 1])
            return 0
        return run

    def interior(k, src, dst):
        theta = shift_of(k)

        def some(n, _):
            advance(src, dst, theta, (edge + 2 + 2 * k + HALF * n, edge + lat - 2 - HALF - 2 * k - HALF * n))
            return 0

        lax.fori_loop(0, jnp.where(k < 3, 2, 1), some, 0)

    def wedge(c):
        def some(k, src, dst):
            low = edge - HALF * (c + 1) + 2 + 2 * k
            advance(src, dst, shift_of(k), (low, rows_all - HALF - low))
        return some

    def dots(lo, hi, spans):
        pairs = [(k, i) for k, i in PAIRS if lo <= k <= hi]

        def one(t, _):
            cut = pl.ds(pl.multiple_of(t * 128, 128), 128)
            acc = (jnp.zeros((8, 128), f32),) * len(pairs)
            for start, stop in spans:
                def part(n, acc):
                    acc = list(acc)
                    for j in range(2):
                        e = start + 2 * n + j
                        for h in range(channels // 8):
                            x = [field(k)[e, 8 * h:8 * h + 8, cut] for k in range(hi + 1)]
                            for n_, (k, i) in enumerate(pairs):
                                acc[n_] = acc[n_] + x[k] * x[i]
                    return tuple(acc)

                acc = lax.fori_loop(0, (stop - start) // 2, part, acc)
            low = jnp.where(t == 1, 32, 16)
            kept = (lane8 >= low) & (lane8 < 128 - low)
            for n, (k, i) in enumerate(pairs):
                at = k * (k + 1) // 2 + i
                gram_acc[at] = gram_acc[at] + jnp.where(kept, acc[n], 0.0)
            return 0

        lax.fori_loop(0, WINDOWS, one, 0)

    for copy in winds:
        copy.wait()
    for q in range(2):
        half = own.at[:, pl.ds(q * channels, channels), :]
        pltpu.make_async_copy(half, half, load_sem.at[q]).wait()
    lax.fori_loop(0, tiles, pack, 0)
    pl.semaphore_wait(barrier, len(greeted))
    for c in range(2):
        for side in range(2):
            @pl.when(has(side))
            def _():
                copies = lat_copies(side, c)
                copies[0].start()
                for ew in range(2):
                    corner_copy(side, ew, c).start()
                for copy in copies[1:]:
                    copy.start()
        if c == 0:
            for ew in range(2):
                lon_copy(ew).start()
    for b in range(1, ny):
        greet(known, 0, b)
    lax.fori_loop(0, tiles, place_own, 0)
    for ew in range(2):
        lon_copy(ew).wait_recv()
    lax.fori_loop(0, tiles, place_lon, 0)
    lax.fori_loop(0, ITERS // 2, two_levels(interior), 0)
    ready = ITERS // 2
    for c in range(2):
        for side in range(2):
            place_halo(side, c)
        lax.fori_loop(0, ITERS // 2, two_levels(wedge(c)), 0)
        if c == 0:
            dots(0, ready, ((edge, edge + lat),))
            dots(ready + 1, ITERS, ((edge + HALF, edge + lat - HALF),))
    dots(ready + 1, ITERS, ((edge, edge + HALF), (edge + lat - HALF, edge + lat)))

    pl.semaphore_wait(known, ny - 1)
    sums = jnp.concatenate(
        [jnp.sum(gram_acc[n], axis=0, keepdims=True) for n in range(len(PAIRS))]
        + [jnp.zeros((128 - len(PAIRS), 128), f32)], axis=0)
    flat = lax.dot_general(jnp.ones((8, 128), f32), sums, (((1,), (1,)), ((), ())), precision=HI,
                           preferred_element_type=f32)
    mine[...] = flat[0:1, :]
    slots[total - 1] = flat[0:1, :]

    for n, (a, b) in enumerate(peers(nx, ny)):
        pltpu.make_async_remote_copy(
            src_ref=mine, dst_ref=slots.at[n], send_sem=red_sem.at[0], recv_sem=red_sem.at[1],
            device_id=(lax.rem(ix + a, nx), lax.rem(iy + b, ny)), device_id_type=MESH).start()
    arrived = slots.at[pl.ds(0, total - 1)]
    pltpu.make_async_copy(arrived, arrived, red_sem.at[1]).wait()
    pltpu.make_async_copy(arrived, arrived, red_sem.at[0]).wait()
    parts = [slots[n] for n in range(4)]
    for n in range(4, total):
        parts[n % 4] = parts[n % 4] + slots[n]
    whole = (parts[0] + parts[1]) + (parts[2] + parts[3])
    gram = [[None] * (ITERS + 1) for _ in range(ITERS + 1)]
    for n, (k, i) in enumerate(PAIRS):
        gram[k][i] = gram[i][k] = jnp.broadcast_to(whole[:, n:n + 1], (8, 128))
    answer, applied = small_solve(gram)
    for k in range(ITERS):
        splats[k] = answer[k]
    for k in range(ITERS + 1):
        splats[ITERS + k] = applied[k]

    def finish(n, _):
        for j in range(4):
            r = 4 * n + j
            for h in range(channels // 8):
                sub = slice(8 * h, 8 * h + 8)
                best, rest = [], []
                for t in range(WINDOWS):
                    cut = slice(128 * t, 128 * t + 128)
                    x = even[0, edge + r, sub, cut]
                    up = splats[0] * x
                    down = x - splats[ITERS] * x
                    for k in range(1, ITERS + 1):
                        x = field(k)[edge + r, sub, cut]
                        if k < ITERS:
                            up = up + splats[k] * x
                        down = down - splats[ITERS + k] * x
                    best.append(up)
                    rest.append(down)
                for q, (a, b, c) in enumerate((best, rest)):
                    b = turn(b, 64)
                    outs[q, r, sub, 0:128] = jnp.where(lane8 < 96, turn(a, 112), b)
                    outs[q, r, sub, 128:256] = jnp.where(lane8 < 32, b, turn(c, 16))
        return 0

    quarter = lat // 4
    for p in range(4):
        lax.fori_loop(quarter // 4 * p, quarter // 4 * (p + 1), finish, 0)
        for c in range(channels):
            for q, dst in enumerate((sol_hbm, res_hbm)):
                pltpu.make_async_copy(outs.at[q, pl.ds(quarter * p, quarter), c, :], dst.at[c, pl.ds(quarter * p, quarter), :],
                                      out_sem.at[q]).start()
    for ew in range(2):
        lon_copy(ew).wait_send()
    for side in range(2):
        @pl.when(has(side))
        def _():
            for c in range(2):
                for copy in lat_copies(side, c):
                    copy.wait_send()
                for ew in range(2):
                    corner_copy(side, ew, c).wait_send()
    for q, dst in enumerate((sol_hbm, res_hbm)):
        pltpu.make_async_copy(dst, dst, out_sem.at[q]).wait()


def solution(mesh):
    nx, ny = mesh.shape["gx"], mesh.shape["gy"]

    def per_device(forcing, damping, coupling, wind_lon, wind_lat):
        channels, lat, lon = forcing.shape
        f32 = jnp.float32
        vmem = pl.BlockSpec(memory_space=pltpu.VMEM)
        hbm = pl.BlockSpec(memory_space=pl.ANY)
        dma = pltpu.SemaphoreType.DMA
        shape = jax.ShapeDtypeStruct((channels, lat, lon), f32)
        rows_all, lanes = lat + 2 * HALO, 128 * WINDOWS
        packed = 2 * channels + 8
        return pl.pallas_call(
            functools.partial(kernel, nx, ny),
            out_shape=(shape, shape),
            in_specs=[hbm, hbm, vmem, hbm, hbm],
            out_specs=(hbm, hbm),
            scratch_shapes=[
                pltpu.VMEM((ITERS // 2 + 1, rows_all, channels, lanes), f32),
                pltpu.VMEM((ITERS // 2, rows_all, channels, lanes), f32),
                pltpu.VMEM((rows_all, channels, lanes), f32),
                pltpu.VMEM((rows_all, 8, lanes), f32),
                pltpu.VMEM((rows_all, 128), f32),
                pltpu.VMEM((GROUP * channels, 3 * GROUP * channels), jnp.bfloat16),
                pltpu.VMEM((256, 256), jnp.bfloat16),
                pltpu.VMEM((lat, 2 * channels, lon), f32),
                pltpu.VMEM((2, HALO, 2 * channels, lon), f32),
                pltpu.VMEM((2, lat, lon), f32),
                pltpu.VMEM((2, 2, HALO, lon), f32),
                pltpu.VMEM((2, lat // HALF, packed, 128), f32),
                pltpu.VMEM((2, lat // HALF, packed, 128), f32),
                pltpu.VMEM((4, 2, packed, 128), f32),
                pltpu.VMEM((len(PAIRS), 8, 128), f32),
                pltpu.VMEM((1, 128), f32),
                pltpu.VMEM((nx * ny, 1, 128), f32),
                pltpu.VMEM((2 * ITERS + 1, 8, 128), f32),
                pltpu.VMEM((2, lat, channels, lon), f32),
                dma((2,)), dma((2,)), dma((2,)),
                dma((2, 2, 3)), dma((2, 2, 3)), dma((2,)), dma((2,)), dma((4, 2)), dma((4, 2)), dma((2,)),
                pltpu.SemaphoreType.REGULAR,
            ],
            compiler_params=pltpu.CompilerParams(
                collective_id=0, has_side_effects=True, vmem_limit_bytes=63 * 1024 * 1024),
        )(forcing, damping, coupling, wind_lon, wind_lat)

    return jax.shard_map(
        per_device,
        mesh=mesh,
        in_specs=(P(None, "gy", "gx"), P(None, "gy", "gx"), P(), P("gy", "gx"), P("gy", "gx")),
        out_specs=(P(None, "gy", "gx"), P(None, "gy", "gx")),
        check_vma=False,
    )
```

```python
import functools
import math

import jax
import jax.numpy as jnp
from jax import lax
from jax.experimental import pallas as pl
from jax.experimental.pallas import tpu as pltpu
from jax.sharding import PartitionSpec as P

ITERS = 8
COUPLE = 0.25
DIFF_LAT = 0.5
DIFF_LON = 0.5
GUARD = 1.0
MESH = pl.DeviceIdType.MESH
HI = lax.Precision.HIGHEST

MIDDLE = 9.0
RADIUS = 6.0
WIDTH = 3.0
THETA = [MIDDLE + RADIUS * math.cos(math.pi * (2 * k + 1) / (2 * ITERS)) for k in (7, 0, 4, 2, 6, 1, 5, 3)]
PAIRS = [(k, i) for k in range(ITERS + 1) for i in range(k + 1)]
GROUP = 4
HALO = 2 * ITERS
HALF = 8
WINDOWS = 3


def apply_to(coords):
    out = [None] * (len(coords) + 1)
    for k, value in enumerate(coords):
        low = THETA[k] * value if k < ITERS else value
        out[k] = low if out[k] is None else out[k] + low
        out[k + 1] = WIDTH * value
    return out


def small_solve(gram):
    first = jnp.sqrt(gram[0][0] + GUARD)
    coords = [[1.0 / first]]
    images = [[gram[i][0] * coords[0][0] for i in range(ITERS + 1)]]
    heights = []
    for j in range(ITERS):
        moved = apply_to(coords[j])
        column = []
        for i in range(j + 1):
            column.append(functools.reduce(lambda a, b: a + b, [images[i][k] * moved[k] for k in range(j + 2)]))
        left = list(moved)
        for i in range(j + 1):
            for k in range(i + 1):
                left[k] = left[k] - column[i] * coords[i][k]
        image = [
            functools.reduce(lambda a, b: a + b, [gram[r][k] * left[k] for k in range(j + 2)])
            for r in range(ITERS + 1)
        ]
        norm_sq = functools.reduce(lambda a, b: a + b, [image[k] * left[k] for k in range(j + 2)])
        subdiag = jnp.sqrt(jnp.maximum(norm_sq, 0.0) + GUARD)
        column.append(subdiag)
        heights.append(column)
        inverse = 1.0 / subdiag
        coords.append([v * inverse for v in left])
        images.append([v * inverse for v in image])
    cosines, sines, target, rotated = [], [], [first], []
    for j in range(ITERS):
        column = list(heights[j])
        for e in range(j):
            upper, lower = column[e], column[e + 1]
            column[e] = cosines[e] * upper + sines[e] * lower
            column[e + 1] = cosines[e] * lower - sines[e] * upper
        upper, lower = column[j], column[j + 1]
        radius = jnp.sqrt(upper * upper + lower * lower)
        inverse = 1.0 / radius
        cosine, sine = upper * inverse, lower * inverse
        column[j] = radius
        kept = target[j]
        target[j] = cosine * kept
        target.append(-sine * kept)
        cosines.append(cosine)
        sines.append(sine)
        rotated.append(column)
    weights = [None] * ITERS
    for j in reversed(range(ITERS)):
        value = target[j]
        for later in range(j + 1, ITERS):
            value = value - rotated[later][j] * weights[later]
        weights[j] = value / rotated[j][j]
    answer = [None] * ITERS
    for j in range(ITERS):
        for k in range(j + 1):
            term = weights[j] * coords[j][k]
            answer[k] = term if answer[k] is None else answer[k] + term
    return answer, apply_to(answer)


def distance(n, o):
    return min(o, n - o)


def peers(nx, ny):
    inner = 4 if ny % 4 == 0 else 1
    offsets = [(a, b) for a in range(nx) for b in range(ny) if (a, b) != (0, 0)]

    def hops(offset):
        a, b = offset
        return distance(nx // 2 or 1, a // 2) + distance(inner, b % inner) + distance(ny // inner, b // inner)

    return sorted(offsets, key=lambda offset: (-hops(offset), offset))


def kernel(nx, ny, f_hbm, d_hbm, c_ref, wl_hbm, wa_hbm, even, odd, splats,
           diag, coef, kxs, block, band, own, near_lat, own_w, near_lat_w, packed, near_lon, near_corner,
           gram_acc, mine, slots,
           load_sem, wind_sem, lat_send, lat_recv, lon_send, lon_recv, cor_send, cor_recv, red_sem, known):
    channels, lat, lon = f_hbm.shape
    both = 2 * channels
    total = nx * ny
    f32, bf16 = jnp.float32, jnp.bfloat16
    ix, iy = lax.axis_index("gx"), lax.axis_index("gy")
    east, west = lax.rem(ix + 1, nx), lax.rem(ix + nx - 1, nx)
    scale = 1.0 / WIDTH
    size = GROUP * channels
    edge = HALO
    rows_all = lat + 2 * HALO
    tiles = lat // HALF

    def field(k):
        return even.at[k // 2] if k % 2 == 0 else odd.at[k // 2]

    barrier = pltpu.get_barrier_semaphore()

    def greet(sem, a, b):
        pl.semaphore_signal(sem, inc=1, device_id=(lax.rem(ix + a, nx), lax.rem(iy + b, ny)), device_id_type=MESH)

    greeted = [(1, 1), (1, ny - 1), (nx - 1, 1), (nx - 1, ny - 1), (0, 1), (0, ny - 1), (1, 0), (nx - 1, 0)]
    greeted += [(a, 0) for a in range(2, nx - 1)] + [(0, b) for b in range(2, ny - 1)]
    for a, b in greeted:
        greet(barrier, a, b)

    winds = [pltpu.make_async_copy(wl_hbm, own_w.at[0], wind_sem.at[0]), pltpu.make_async_copy(wa_hbm, own_w.at[1], wind_sem.at[1])]
    for copy in winds:
        copy.start()
    for c in range(channels):
        for q, src in enumerate((f_hbm, d_hbm)):
            pltpu.make_async_copy(src.at[c], own.at[:, q * channels + c, :], load_sem.at[q]).start()

    def spread(n):
        row = lax.broadcasted_iota(jnp.int32, (n, channels), 0)
        col = lax.broadcasted_iota(jnp.int32, (n, channels), 1)
        return jnp.where(lax.rem(row, channels) == col, 1.0, 0.0).astype(f32)

    wide = lax.dot_general(spread(size), c_ref[...], (((1,), (0,)), ((), ())), precision=HI, preferred_element_type=f32)
    wide = lax.dot_general(wide, spread(3 * size), (((1,), (1,)), ((), ())), precision=HI,
                           preferred_element_type=f32) * (COUPLE * scale)
    down = lax.broadcasted_iota(jnp.int32, (size, 3 * size), 0)
    across = lax.broadcasted_iota(jnp.int32, (size, 3 * size), 1)
    high = wide.astype(bf16).astype(f32)
    wide = jnp.where(across < 2 * size, high, wide - high)
    block[...] = jnp.where(down // channels == lax.rem(across, size) // channels, wide, 0.0).astype(bf16)
    down = lax.broadcasted_iota(jnp.int32, (256, 256), 0)
    across = lax.broadcasted_iota(jnp.int32, (256, 256), 1)
    shift = lax.rem(down, 128) - lax.rem(across, 128)
    sums = jnp.where((shift == 1) | (shift == -1), 1.0, 0.0)
    slopes = jnp.where(shift == 1, 8.0, 0.0) + jnp.where(shift == -1, -8.0, 0.0)
    slopes = slopes + jnp.where(shift == 2, -1.0, 0.0) + jnp.where(shift == -2, 1.0, 0.0)
    band[...] = jnp.where(across < 128, sums, slopes).astype(bf16)
    row_pos = (lax.broadcasted_iota(jnp.int32, (rows_all, 128), 0) + (iy * lat - edge)).astype(f32)
    phi = -math.pi / 2 + (row_pos + 0.5) * (math.pi / (lat * ny))
    kxs[...] = (DIFF_LON * scale) / (jnp.cos(phi) ** 2 + 0.1)
    gram_acc[...] = jnp.zeros(gram_acc.shape, f32)

    @pl.when(iy == 0)
    def _():
        near_lat[0] = jnp.zeros(near_lat.shape[1:], f32)
        near_lat_w[0] = jnp.zeros(near_lat_w.shape[1:], f32)
        near_corner[0] = jnp.zeros(near_corner.shape[1:], f32)
        near_corner[1] = jnp.zeros(near_corner.shape[1:], f32)

    @pl.when(iy == ny - 1)
    def _():
        near_lat[1] = jnp.zeros(near_lat.shape[1:], f32)
        near_lat_w[1] = jnp.zeros(near_lat_w.shape[1:], f32)
        near_corner[2] = jnp.zeros(near_corner.shape[1:], f32)
        near_corner[3] = jnp.zeros(near_corner.shape[1:], f32)

    def lat_copies(side, c):
        first = HALF * (1 - c) if side == 0 else HALF * c
        base = lat - HALO if side == 0 else 0
        to = (ix, iy + 1) if side == 0 else (ix, iy - 1)
        if c == 0:
            parts = [(first, HALF, 0, both)]
        elif side == 0:
            parts = [(first + 2, HALF - 2, 0, both), (first, 2, 0, channels)]
        else:
            parts = [(first, HALF - 2, 0, both), (first + HALF - 2, 2, 0, channels)]
        out = []
        for n, (start, count, sub, subs) in enumerate(parts):
            out.append(pltpu.make_async_remote_copy(
                src_ref=own.at[pl.ds(base + start, count), pl.ds(sub, subs), :],
                dst_ref=near_lat.at[side, pl.ds(start, count), pl.ds(sub, subs), :],
                send_sem=lat_send.at[side, c, n], recv_sem=lat_recv.at[side, c, n], device_id=to, device_id_type=MESH))
        out.append(pltpu.make_async_remote_copy(
            src_ref=own_w.at[:, pl.ds(base + first, HALF), :], dst_ref=near_lat_w.at[side, :, pl.ds(first, HALF), :],
            send_sem=lat_send.at[side, c, 2], recv_sem=lat_recv.at[side, c, 2], device_id=to, device_id_type=MESH))
        return out

    def tile_of(side, c):
        return 1 - c if side == 0 else c

    def corner_copy(side, ew, c):
        slot, tile = 2 * side + ew, tile_of(side, c)
        return pltpu.make_async_remote_copy(
            src_ref=packed.at[ew, tile + (tiles - 2 if side == 0 else 0)], dst_ref=near_corner.at[slot, tile],
            send_sem=cor_send.at[slot, c], recv_sem=cor_recv.at[slot, c],
            device_id=(east if ew == 0 else west, iy + 1 if side == 0 else iy - 1), device_id_type=MESH)

    def lon_copy(ew):
        return pltpu.make_async_remote_copy(
            src_ref=packed.at[ew], dst_ref=near_lon.at[ew], send_sem=lon_send.at[ew], recv_sem=lon_recv.at[ew],
            device_id=(east if ew == 0 else west, iy), device_id_type=MESH)

    def has(side):
        return iy < ny - 1 if side == 0 else iy > 0

    def from_side(side):
        return iy > 0 if side == 0 else iy < ny - 1

    lane = lax.broadcasted_iota(jnp.int32, (both, 128), 1)
    lane8 = lax.broadcasted_iota(jnp.int32, (8, 128), 1)

    def turn(x, n):
        n = n % 128
        return pltpu.roll(x, n, 1) if n else x

    def pack(n, _):
        for ew in range(2):
            cut = slice(lon - 128, lon) if ew == 0 else slice(0, 128)
            start = 112 if ew == 0 else 0
            base = HALF * n
            strip = turn(own[base, :, cut], -start)
            for j in range(1, HALF):
                strip = jnp.where((lane >= 16 * j) & (lane < 16 * j + 16), turn(own[base + j, :, cut], 16 * j - start), strip)
            packed[ew, n, 0:both, :] = strip
            rows = pl.ds(pl.multiple_of(base, 8), 8)
            packed[ew, n, both:both + 8, :] = jnp.where(
                lane8 < 16, turn(own_w[0, rows, cut], -start), turn(own_w[1, rows, cut], 16 - start))
        return 0

    def place_coef(e0, wl, wa, inside, chosen):
        kx = kxs[pl.ds(e0, 8), :]
        for t in chosen:
            cut = slice(128 * t, 128 * t + 128)
            l, a = wl[t] * (scale / 12.0), wa[t] * (scale / 12.0)
            planes = [-kx, l, 8.0 * a - DIFF_LAT * scale, -8.0 * a - DIFF_LAT * scale, a]
            for q, plane in enumerate(planes):
                if q == 0 and t != 1:
                    continue
                if inside is not None:
                    plane = plane * inside
                for j in range(8):
                    coef[e0 + j, q:q + 1, cut] = plane[j:j + 1, :]

    def centre(e):
        return (1.0 + 2.0 * DIFF_LAT) * scale - 2.0 * coef[e, 0:1, 128:256]

    def place_own(n, _):
        base = HALF * n
        rows = pl.ds(pl.multiple_of(base, 8), 8)
        wl, wa = ([None, turn(jnp.where(lane8 >= 64, own_w[q, rows, 0:128], own_w[q, rows, 128:256]), 64), None] for q in range(2))
        place_coef(pl.multiple_of(edge + base, 8), wl, wa, None, (1,))
        for j in range(HALF):
            r = base + j
            e = edge + r
            a, b = own[r, :, 0:128], own[r, :, 128:256]
            middle = centre(e)
            for t, piece in enumerate((turn(a, 16), turn(jnp.where(lane >= 64, a, b), 64), turn(b, 112))):
                cut = slice(128 * t, 128 * t + 128)
                even[0, e, :, cut] = piece[0:channels]
                diag[e, :, cut] = piece[channels:] * scale + middle
        return 0

    def place_lon(n, _):
        base = HALF * n
        rows = pl.ds(pl.multiple_of(base, 8), 8)
        w, e = near_lon[0, n, both:both + 8, :], near_lon[1, n, both:both + 8, :]
        wl, wa = ([jnp.where(lane8 < 16, turn(w, -16 * q), turn(own_w[q, rows, 0:128], 16)), None,
                   jnp.where(lane8 >= 112, turn(e, 112 - 16 * q), turn(own_w[q, rows, 128:256], 112))] for q in range(2))
        place_coef(pl.multiple_of(edge + base, 8), wl, wa, None, (0, 2))
        w, e = near_lon[0, n, 0:both, :], near_lon[1, n, 0:both, :]
        for j in range(HALF):
            r = edge + base + j
            middle = centre(r)
            for cut, keep, piece in ((slice(0, 128), lane < 16, turn(w, -16 * j)), (slice(256, 384), lane >= 112, turn(e, 112 - 16 * j))):
                even[0, r, :, cut] = jnp.where(keep[0:channels], piece[0:channels], even[0, r, :, cut])
                diag[r, :, cut] = jnp.where(keep[0:channels], piece[channels:] * scale + middle, diag[r, :, cut])
        return 0

    def place_halo(side, c):
        first = HALF * (1 - c) if side == 0 else HALF * c
        tile = tile_of(side, c)
        e0 = first if side == 0 else edge + lat + first
        inside = jnp.where(from_side(side), 1.0, 0.0).astype(f32)

        @pl.when(from_side(side))
        def _():
            for copy in lat_copies(side, c):
                copy.wait_recv()
            for ew in range(2):
                corner_copy(side, ew, c).wait_recv()

        def three(a, b, w, e, lanes, at):
            return (jnp.where(lanes < 16, turn(w, -at), turn(a, 16)), turn(jnp.where(lanes >= 64, a, b), 64),
                    jnp.where(lanes >= 112, turn(e, 112 - at), turn(b, 112)))

        west_strip, east_strip = near_corner.at[2 * side, tile], near_corner.at[2 * side + 1, tile]
        span = slice(first, first + 8)
        wl, wa = (three(near_lat_w[side, q, span, 0:128], near_lat_w[side, q, span, 128:256],
                        west_strip[both:both + 8, :], east_strip[both:both + 8, :], lane8, 16 * q) for q in range(2))
        place_coef(e0, wl, wa, inside, range(WINDOWS))
        for j in range(HALF):
            middle = centre(e0 + j)
            pieces = three(near_lat[side, first + j, :, 0:128], near_lat[side, first + j, :, 128:256],
                           west_strip[0:both, :], east_strip[0:both, :], lane, 16 * j)
            for t, piece in enumerate(pieces):
                cut = slice(128 * t, 128 * t + 128)
                even[0, e0 + j, :, cut] = piece[0:channels]
                diag[e0 + j, :, cut] = piece[channels:] * scale + middle

    def shift_of(k):
        theta = jnp.float32(THETA[0] * scale)
        for i in range(1, ITERS):
            theta = jnp.where(k == i, jnp.float32(THETA[i] * scale), theta)
        return theta

    def advance(src, dst, theta, starts):
        groups = [[e0 + GROUP * g + j for j in range(GROUP)] for e0 in starts for g in range(HALF // GROUP)]
        mixed, moved = [], []
        for picked in groups:
            stack = jnp.concatenate([src[e] for e in picked], axis=0)
            high = stack.astype(bf16)
            low = (stack - high.astype(f32)).astype(bf16)
            mixed.append(lax.dot_general(block[...], jnp.concatenate([high, low, high], axis=0), (((1,), (0,)), ((), ())),
                                         preferred_element_type=f32))
            sides = jnp.concatenate(
                [jnp.concatenate([high[:, 128 * t:128 * t + 128], low[:, 128 * t:128 * t + 128]], axis=1)
                 for t in range(WINDOWS)], axis=0)
            moved.append(lax.dot_general(sides, band[...], (((1,), (0,)), ((), ())), preferred_element_type=f32))
        for g, picked in enumerate(groups):
            for j, e in enumerate(picked):
                for t in range(WINDOWS):
                    cut = slice(128 * t, 128 * t + 128)
                    at = slice(size * t + channels * j, size * t + channels * (j + 1))

                    def weight(q):
                        return coef[e, q:q + 1, cut]

                    value = (diag[e, :, cut] - theta) * src[e, :, cut] + mixed[g][channels * j:channels * (j + 1), cut]
                    value = value + (coef[e, 0:1, 128:256] * moved[g][at, 0:128] + weight(1) * moved[g][at, 128:256])
                    value = value + weight(2) * src[e + 1, :, cut] + weight(3) * src[e - 1, :, cut]
                    dst[e, :, cut] = value + weight(4) * (src[e - 2, :, cut] - src[e + 2, :, cut])

    def two_levels(some):
        def run(n, _):
            some(2 * n, even.at[n], odd.at[n])
            some(2 * n + 1, odd.at[n], even.at[n + 1])
            return 0
        return run

    def interior(k, src, dst):
        theta = shift_of(k)

        def some(n, _):
            advance(src, dst, theta, (edge + 2 + 2 * k + HALF * n, edge + lat - 2 - HALF - 2 * k - HALF * n))
            return 0

        lax.fori_loop(0, jnp.where(k < 3, 2, 1), some, 0)

    def wedge(c):
        for k in range(ITERS):
            low = edge - HALF * (c + 1) + 2 + 2 * k
            for e0 in (low, rows_all - HALF - low):
                advance(field(k), field(k + 1), THETA[k] * scale, (e0,))

    def dots(lo, hi, spans):
        pairs = [(k, i) for k, i in PAIRS if lo <= k <= hi]

        def one(t, _):
            cut = pl.ds(pl.multiple_of(t * 128, 128), 128)
            acc = (jnp.zeros((8, 128), f32),) * len(pairs)
            for start, stop in spans:
                def part(n, acc):
                    acc = list(acc)
                    for j in range(4):
                        e = start + 4 * n + j
                        for h in range(channels // 8):
                            x = [field(k)[e, 8 * h:8 * h + 8, cut] for k in range(hi + 1)]
                            for n_, (k, i) in enumerate(pairs):
                                acc[n_] = acc[n_] + x[k] * x[i]
                    return tuple(acc)

                acc = lax.fori_loop(0, (stop - start) // 4, part, acc)
            low = jnp.where(t == 1, 32, 16)
            kept = (lane8 >= low) & (lane8 < 128 - low)
            for n, (k, i) in enumerate(pairs):
                at = k * (k + 1) // 2 + i
                gram_acc[at] = gram_acc[at] + jnp.where(kept, acc[n], 0.0)
            return 0

        lax.fori_loop(0, WINDOWS, one, 0)

    for copy in winds:
        copy.wait()
    for q in range(2):
        half = own.at[:, pl.ds(q * channels, channels), :]
        pltpu.make_async_copy(half, half, load_sem.at[q]).wait()
    lax.fori_loop(0, tiles, pack, 0)
    pl.semaphore_wait(barrier, len(greeted))
    for c in range(2):
        for side in range(2):
            @pl.when(has(side))
            def _():
                copies = lat_copies(side, c)
                copies[0].start()
                for ew in range(2):
                    corner_copy(side, ew, c).start()
                for copy in copies[1:]:
                    copy.start()
        if c == 0:
            for ew in range(2):
                lon_copy(ew).start()
    for b in range(1, ny):
        greet(known, 0, b)
    lax.fori_loop(0, tiles, place_own, 0)
    for ew in range(2):
        lon_copy(ew).wait_recv()
    lax.fori_loop(0, tiles, place_lon, 0)
    lax.fori_loop(0, ITERS // 2, two_levels(interior), 0)
    ready = ITERS // 2
    dots(0, ready, ((edge + HALF, edge + lat - HALF),))
    for c in range(2):
        for side in range(2):
            place_halo(side, c)
        wedge(c)
        if c == 0:
            dots(0, ready, ((edge, edge + HALF), (edge + lat - HALF, edge + lat)))
            dots(ready + 1, ITERS, ((edge + HALF, edge + lat - HALF),))
    dots(ready + 1, ITERS, ((edge, edge + HALF), (edge + lat - HALF, edge + lat)))

    pl.semaphore_wait(known, ny - 1)
    sums = jnp.concatenate(
        [jnp.sum(gram_acc[n], axis=0, keepdims=True) for n in range(len(PAIRS))]
        + [jnp.zeros((128 - len(PAIRS), 128), f32)], axis=0)
    flat = lax.dot_general(jnp.ones((8, 128), f32), sums, (((1,), (1,)), ((), ())), precision=HI,
                           preferred_element_type=f32)
    mine[...] = flat[0:1, :]
    slots[total - 1] = flat[0:1, :]

    for n, (a, b) in enumerate(peers(nx, ny)):
        pltpu.make_async_remote_copy(
            src_ref=mine, dst_ref=slots.at[n], send_sem=red_sem.at[0], recv_sem=red_sem.at[1],
            device_id=(lax.rem(ix + a, nx), lax.rem(iy + b, ny)), device_id_type=MESH).start()
    arrived = slots.at[pl.ds(0, total - 1)]
    pltpu.make_async_copy(arrived, arrived, red_sem.at[1]).wait()
    pltpu.make_async_copy(arrived, arrived, red_sem.at[0]).wait()
    parts = [slots[n] for n in range(4)]
    for n in range(4, total):
        parts[n % 4] = parts[n % 4] + slots[n]
    whole = (parts[0] + parts[1]) + (parts[2] + parts[3])
    gram = [[None] * (ITERS + 1) for _ in range(ITERS + 1)]
    for n, (k, i) in enumerate(PAIRS):
        gram[k][i] = gram[i][k] = jnp.broadcast_to(whole[:, n:n + 1], (8, 128))
    answer, applied = small_solve(gram)
    for k in range(ITERS):
        splats[k] = answer[k]
    for k in range(ITERS + 1):
        splats[ITERS + k] = applied[k]

    for ew in range(2):
        lon_copy(ew).wait_send()
    for side in range(2):
        @pl.when(has(side))
        def _():
            for c in range(2):
                for copy in lat_copies(side, c):
                    copy.wait_send()
                for ew in range(2):
                    corner_copy(side, ew, c).wait_send()


def finish(even, odd, splats, sol_hbm, res_hbm, outs, out_sem):
    channels, lat, _ = sol_hbm.shape
    lane = lax.broadcasted_iota(jnp.int32, (8, 128), 1)
    quarter = lat // 4
    for r in range(lat):
        for h in range(channels // 8):
            sub = slice(8 * h, 8 * h + 8)
            best, rest = [], []
            for t in range(WINDOWS):
                cut = slice(128 * t, 128 * t + 128)
                x = even[0, HALO + r, sub, cut]
                up = splats[0] * x
                down = x - splats[ITERS] * x
                for k in range(1, ITERS + 1):
                    x = (odd if k % 2 else even)[k // 2, HALO + r, sub, cut]
                    if k < ITERS:
                        up = up + splats[k] * x
                    down = down - splats[ITERS + k] * x
                best.append(up)
                rest.append(down)
            for q, (a, b, c) in enumerate((best, rest)):
                b = pltpu.roll(b, 64, 1)
                outs[q, r, sub, 0:128] = jnp.where(lane < 96, pltpu.roll(a, 112, 1), b)
                outs[q, r, sub, 128:256] = jnp.where(lane < 32, b, pltpu.roll(c, 16, 1))
        if (r + 1) % quarter == 0:
            rows = pl.ds(r + 1 - quarter, quarter)
            for c in range(channels):
                for q, dst in enumerate((sol_hbm, res_hbm)):
                    pltpu.make_async_copy(outs.at[q, rows, c, :], dst.at[c, rows, :], out_sem.at[q]).start()
    for q, dst in enumerate((sol_hbm, res_hbm)):
        pltpu.make_async_copy(dst, dst, out_sem.at[q]).wait()


def solution(mesh):
    nx, ny = mesh.shape["gx"], mesh.shape["gy"]

    def per_device(forcing, damping, coupling, wind_lon, wind_lat):
        channels, lat, lon = forcing.shape
        f32 = jnp.float32
        vmem = pl.BlockSpec(memory_space=pltpu.VMEM)
        hbm = pl.BlockSpec(memory_space=pltpu.HBM)
        dma = pltpu.SemaphoreType.DMA
        shape = jax.ShapeDtypeStruct((channels, lat, lon), f32)
        rows_all, lanes = lat + 2 * HALO, 128 * WINDOWS
        packed = 2 * channels + 8
        even, odd, splats = pl.pallas_call(
            functools.partial(kernel, nx, ny),
            out_shape=(
                pltpu.VMEM((ITERS // 2 + 1, rows_all, channels, lanes), f32),
                pltpu.VMEM((ITERS // 2, rows_all, channels, lanes), f32),
                pltpu.VMEM((2 * ITERS + 1, 8, 128), f32),
            ),
            in_specs=[hbm, hbm, vmem, hbm, hbm],
            out_specs=(vmem, vmem, vmem),
            scratch_shapes=[
                pltpu.VMEM((rows_all, channels, lanes), f32),
                pltpu.VMEM((rows_all, 8, lanes), f32),
                pltpu.VMEM((rows_all, 128), f32),
                pltpu.VMEM((GROUP * channels, 3 * GROUP * channels), jnp.bfloat16),
                pltpu.VMEM((256, 256), jnp.bfloat16),
                pltpu.VMEM((lat, 2 * channels, lon), f32),
                pltpu.VMEM((2, HALO, 2 * channels, lon), f32),
                pltpu.VMEM((2, lat, lon), f32),
                pltpu.VMEM((2, 2, HALO, lon), f32),
                pltpu.VMEM((2, lat // HALF, packed, 128), f32),
                pltpu.VMEM((2, lat // HALF, packed, 128), f32),
                pltpu.VMEM((4, 2, packed, 128), f32),
                pltpu.VMEM((len(PAIRS), 8, 128), f32),
                pltpu.VMEM((1, 128), f32),
                pltpu.VMEM((nx * ny, 1, 128), f32),
                dma((2,)), dma((2,)),
                dma((2, 2, 3)), dma((2, 2, 3)), dma((2,)), dma((2,)), dma((4, 2)), dma((4, 2)), dma((2,)),
                pltpu.SemaphoreType.REGULAR,
            ],
            compiler_params=pltpu.CompilerParams(
                collective_id=0, has_side_effects=True, vmem_limit_bytes=52_800_000),
        )(forcing, damping, coupling, wind_lon, wind_lat)
        return pl.pallas_call(
            finish,
            out_shape=(shape, shape),
            in_specs=[vmem, vmem, vmem],
            out_specs=(hbm, hbm),
            scratch_shapes=[pltpu.VMEM((2, lat, channels, lon), f32), dma((2,))],
            compiler_params=pltpu.CompilerParams(vmem_limit_bytes=16 * 1024 * 1024),
        )(even, odd, splats)

    return jax.shard_map(
        per_device,
        mesh=mesh,
        in_specs=(P(None, "gy", "gx"), P(None, "gy", "gx"), P(), P("gy", "gx"), P("gy", "gx")),
        out_specs=(P(None, "gy", "gx"), P(None, "gy", "gx")),
        check_vma=False,
    )
```

```python
import functools
import math

import jax
import jax.numpy as jnp
from jax import lax
from jax.experimental import pallas as pl
from jax.experimental.pallas import tpu as pltpu
from jax.sharding import PartitionSpec as P

ITERS = 8
COUPLE = 0.25
DIFF_LAT = 0.5
DIFF_LON = 0.5
GUARD = 1.0
MESH = pl.DeviceIdType.MESH
HI = lax.Precision.HIGHEST

MIDDLE = 9.0
RADIUS = 6.0
WIDTH = 3.0
THETA = [MIDDLE + RADIUS * math.cos(math.pi * (2 * k + 1) / (2 * ITERS)) for k in (7, 0, 4, 2, 6, 1, 5, 3)]
PAIRS = [(k, i) for k in range(ITERS + 1) for i in range(k + 1)]
GROUP = 4
HALO = 2 * ITERS
HALF = 8
WINDOWS = 3


def apply_to(coords):
    out = [None] * (len(coords) + 1)
    for k, value in enumerate(coords):
        low = THETA[k] * value if k < ITERS else value
        out[k] = low if out[k] is None else out[k] + low
        out[k + 1] = WIDTH * value
    return out


def small_solve(gram):
    first = jnp.sqrt(gram[0][0] + GUARD)
    coords = [[1.0 / first]]
    images = [[gram[i][0] * coords[0][0] for i in range(ITERS + 1)]]
    heights = []
    for j in range(ITERS):
        moved = apply_to(coords[j])
        column = []
        for i in range(j + 1):
            column.append(functools.reduce(lambda a, b: a + b, [images[i][k] * moved[k] for k in range(j + 2)]))
        left = list(moved)
        for i in range(j + 1):
            for k in range(i + 1):
                left[k] = left[k] - column[i] * coords[i][k]
        image = [
            functools.reduce(lambda a, b: a + b, [gram[r][k] * left[k] for k in range(j + 2)])
            for r in range(ITERS + 1)
        ]
        norm_sq = functools.reduce(lambda a, b: a + b, [image[k] * left[k] for k in range(j + 2)])
        subdiag = jnp.sqrt(jnp.maximum(norm_sq, 0.0) + GUARD)
        column.append(subdiag)
        heights.append(column)
        inverse = 1.0 / subdiag
        coords.append([v * inverse for v in left])
        images.append([v * inverse for v in image])
    cosines, sines, target, rotated = [], [], [first], []
    for j in range(ITERS):
        column = list(heights[j])
        for e in range(j):
            upper, lower = column[e], column[e + 1]
            column[e] = cosines[e] * upper + sines[e] * lower
            column[e + 1] = cosines[e] * lower - sines[e] * upper
        upper, lower = column[j], column[j + 1]
        radius = jnp.sqrt(upper * upper + lower * lower)
        inverse = 1.0 / radius
        cosine, sine = upper * inverse, lower * inverse
        column[j] = radius
        kept = target[j]
        target[j] = cosine * kept
        target.append(-sine * kept)
        cosines.append(cosine)
        sines.append(sine)
        rotated.append(column)
    weights = [None] * ITERS
    for j in reversed(range(ITERS)):
        value = target[j]
        for later in range(j + 1, ITERS):
            value = value - rotated[later][j] * weights[later]
        weights[j] = value / rotated[j][j]
    answer = [None] * ITERS
    for j in range(ITERS):
        for k in range(j + 1):
            term = weights[j] * coords[j][k]
            answer[k] = term if answer[k] is None else answer[k] + term
    return answer, apply_to(answer)


def distance(n, o):
    return min(o, n - o)


def peers(nx, ny):
    inner = 4 if ny % 4 == 0 else 1
    offsets = [(a, b) for a in range(nx) for b in range(ny) if (a, b) != (0, 0)]

    def hops(offset):
        a, b = offset
        return distance(nx // 2 or 1, a // 2) + distance(inner, b % inner) + distance(ny // inner, b // inner)

    return sorted(offsets, key=lambda offset: (-hops(offset), offset))


def kernel(nx, ny, f_hbm, d_hbm, c_ref, wl_hbm, wa_hbm, even, odd, splats,
           diag, coef, kxs, block, band, own, near_lat, own_w, near_lat_w, packed, near_lon, near_corner,
           gram_acc, mine, slots,
           load_sem, wind_sem, lat_send, lat_recv, lon_send, lon_recv, cor_send, cor_recv, red_sem, known):
    channels, lat, lon = f_hbm.shape
    both = 2 * channels
    total = nx * ny
    f32, bf16 = jnp.float32, jnp.bfloat16
    ix, iy = lax.axis_index("gx"), lax.axis_index("gy")
    east, west = lax.rem(ix + 1, nx), lax.rem(ix + nx - 1, nx)
    scale = 1.0 / WIDTH
    size = GROUP * channels
    edge = HALO
    rows_all = lat + 2 * HALO
    tiles = lat // HALF

    def field(k):
        return even.at[k // 2] if k % 2 == 0 else odd.at[k // 2]

    barrier = pltpu.get_barrier_semaphore()

    def greet(sem, a, b):
        pl.semaphore_signal(sem, inc=1, device_id=(lax.rem(ix + a, nx), lax.rem(iy + b, ny)), device_id_type=MESH)

    close = [(0, 1), (0, ny - 1), (1, 0), (nx - 1, 0)]
    rounds = [
        close,
        close + [(0, 2), (0, ny - 2), (2, 0), (nx - 2, 0)],
        [(0, b) for b in range(1, 5)] + [(0, ny - b) for b in range(1, 5)],
        [(a, 0) for a in range(1, nx)],
    ]
    for a, b in close:
        greet(barrier, a, b)

    def tell(n):
        for a, b in rounds[n]:
            greet(known.at[n], a, b)

    def hear(n):
        pl.semaphore_wait(known.at[n], len(rounds[n]))

    winds = [pltpu.make_async_copy(wl_hbm, own_w.at[0], wind_sem.at[0]), pltpu.make_async_copy(wa_hbm, own_w.at[1], wind_sem.at[1])]
    for copy in winds:
        copy.start()
    for c in range(channels):
        for q, src in enumerate((f_hbm, d_hbm)):
            pltpu.make_async_copy(src.at[c], own.at[:, q * channels + c, :], load_sem.at[q]).start()

    def spread(n):
        row = lax.broadcasted_iota(jnp.int32, (n, channels), 0)
        col = lax.broadcasted_iota(jnp.int32, (n, channels), 1)
        return jnp.where(lax.rem(row, channels) == col, 1.0, 0.0).astype(f32)

    wide = lax.dot_general(spread(size), c_ref[...], (((1,), (0,)), ((), ())), precision=HI, preferred_element_type=f32)
    wide = lax.dot_general(wide, spread(3 * size), (((1,), (1,)), ((), ())), precision=HI,
                           preferred_element_type=f32) * (COUPLE * scale)
    down = lax.broadcasted_iota(jnp.int32, (size, 3 * size), 0)
    across = lax.broadcasted_iota(jnp.int32, (size, 3 * size), 1)
    high = wide.astype(bf16).astype(f32)
    wide = jnp.where(across < 2 * size, high, wide - high)
    block[...] = jnp.where(down // channels == lax.rem(across, size) // channels, wide, 0.0).astype(bf16)
    down = lax.broadcasted_iota(jnp.int32, (256, 256), 0)
    across = lax.broadcasted_iota(jnp.int32, (256, 256), 1)
    shift = lax.rem(down, 128) - lax.rem(across, 128)
    sums = jnp.where((shift == 1) | (shift == -1), 1.0, 0.0)
    slopes = jnp.where(shift == 1, 8.0, 0.0) + jnp.where(shift == -1, -8.0, 0.0)
    slopes = slopes + jnp.where(shift == 2, -1.0, 0.0) + jnp.where(shift == -2, 1.0, 0.0)
    band[...] = jnp.where(across < 128, sums, slopes).astype(bf16)
    row_pos = (lax.broadcasted_iota(jnp.int32, (rows_all, 128), 0) + (iy * lat - edge)).astype(f32)
    phi = -math.pi / 2 + (row_pos + 0.5) * (math.pi / (lat * ny))
    kxs[...] = (DIFF_LON * scale) / (jnp.cos(phi) ** 2 + 0.1)
    gram_acc[...] = jnp.zeros(gram_acc.shape, f32)

    @pl.when(iy == 0)
    def _():
        near_lat[0] = jnp.zeros(near_lat.shape[1:], f32)
        near_lat_w[0] = jnp.zeros(near_lat_w.shape[1:], f32)
        near_corner[0] = jnp.zeros(near_corner.shape[1:], f32)
        near_corner[1] = jnp.zeros(near_corner.shape[1:], f32)

    @pl.when(iy == ny - 1)
    def _():
        near_lat[1] = jnp.zeros(near_lat.shape[1:], f32)
        near_lat_w[1] = jnp.zeros(near_lat_w.shape[1:], f32)
        near_corner[2] = jnp.zeros(near_corner.shape[1:], f32)
        near_corner[3] = jnp.zeros(near_corner.shape[1:], f32)

    def lat_copies(side, c):
        first = HALF * (1 - c) if side == 0 else HALF * c
        base = lat - HALO if side == 0 else 0
        to = (ix, iy + 1) if side == 0 else (ix, iy - 1)
        if c == 0:
            parts = [(first, HALF, 0, both)]
        elif side == 0:
            parts = [(first + 2, HALF - 2, 0, both), (first, 2, 0, channels)]
        else:
            parts = [(first, HALF - 2, 0, both), (first + HALF - 2, 2, 0, channels)]
        out = []
        for n, (start, count, sub, subs) in enumerate(parts):
            out.append(pltpu.make_async_remote_copy(
                src_ref=own.at[pl.ds(base + start, count), pl.ds(sub, subs), :],
                dst_ref=near_lat.at[side, pl.ds(start, count), pl.ds(sub, subs), :],
                send_sem=lat_send.at[side, c, n], recv_sem=lat_recv.at[side, c, n], device_id=to, device_id_type=MESH))
        out.append(pltpu.make_async_remote_copy(
            src_ref=own_w.at[:, pl.ds(base + first, HALF), :], dst_ref=near_lat_w.at[side, :, pl.ds(first, HALF), :],
            send_sem=lat_send.at[side, c, 2], recv_sem=lat_recv.at[side, c, 2], device_id=to, device_id_type=MESH))
        return out

    def tile_of(side, c):
        return 1 - c if side == 0 else c

    def corner_copy(side, ew, c):
        slot, tile = 2 * side + ew, tile_of(side, c)
        return pltpu.make_async_remote_copy(
            src_ref=packed.at[ew, tile + (tiles - 2 if side == 0 else 0)], dst_ref=near_corner.at[slot, tile],
            send_sem=cor_send.at[slot, c], recv_sem=cor_recv.at[slot, c],
            device_id=(east if ew == 0 else west, iy + 1 if side == 0 else iy - 1), device_id_type=MESH)

    def lon_copy(ew):
        return pltpu.make_async_remote_copy(
            src_ref=packed.at[ew], dst_ref=near_lon.at[ew], send_sem=lon_send.at[ew], recv_sem=lon_recv.at[ew],
            device_id=(east if ew == 0 else west, iy), device_id_type=MESH)

    def has(side):
        return iy < ny - 1 if side == 0 else iy > 0

    def from_side(side):
        return iy > 0 if side == 0 else iy < ny - 1

    lane = lax.broadcasted_iota(jnp.int32, (both, 128), 1)
    lane8 = lax.broadcasted_iota(jnp.int32, (8, 128), 1)

    def turn(x, n):
        n = n % 128
        return pltpu.roll(x, n, 1) if n else x

    def pack(n, _):
        for ew in range(2):
            cut = slice(lon - 128, lon) if ew == 0 else slice(0, 128)
            start = 112 if ew == 0 else 0
            base = HALF * n
            strip = turn(own[base, :, cut], -start)
            for j in range(1, HALF):
                strip = jnp.where((lane >= 16 * j) & (lane < 16 * j + 16), turn(own[base + j, :, cut], 16 * j - start), strip)
            packed[ew, n, 0:both, :] = strip
            rows = pl.ds(pl.multiple_of(base, 8), 8)
            packed[ew, n, both:both + 8, :] = jnp.where(
                lane8 < 16, turn(own_w[0, rows, cut], -start), turn(own_w[1, rows, cut], 16 - start))
        return 0

    def place_coef(e0, wl, wa, inside, chosen):
        kx = kxs[pl.ds(e0, 8), :]
        for t in chosen:
            cut = slice(128 * t, 128 * t + 128)
            l, a = wl[t] * (scale / 12.0), wa[t] * (scale / 12.0)
            planes = [-kx, l, 8.0 * a - DIFF_LAT * scale, -8.0 * a - DIFF_LAT * scale, a]
            for q, plane in enumerate(planes):
                if q == 0 and t != 1:
                    continue
                if inside is not None:
                    plane = plane * inside
                for j in range(8):
                    coef[e0 + j, q:q + 1, cut] = plane[j:j + 1, :]

    def centre(e):
        return (1.0 + 2.0 * DIFF_LAT) * scale - 2.0 * coef[e, 0:1, 128:256]

    def place_own(n, _):
        base = HALF * n
        rows = pl.ds(pl.multiple_of(base, 8), 8)
        wl, wa = ([None, turn(jnp.where(lane8 >= 64, own_w[q, rows, 0:128], own_w[q, rows, 128:256]), 64), None] for q in range(2))
        place_coef(pl.multiple_of(edge + base, 8), wl, wa, None, (1,))
        for j in range(HALF):
            r = base + j
            e = edge + r
            a, b = own[r, :, 0:128], own[r, :, 128:256]
            middle = centre(e)
            for t, piece in enumerate((turn(a, 16), turn(jnp.where(lane >= 64, a, b), 64), turn(b, 112))):
                cut = slice(128 * t, 128 * t + 128)
                even[0, e, :, cut] = piece[0:channels]
                diag[e, :, cut] = piece[channels:] * scale + middle
        return 0

    def place_lon(n, _):
        base = HALF * n
        rows = pl.ds(pl.multiple_of(base, 8), 8)
        w, e = near_lon[0, n, both:both + 8, :], near_lon[1, n, both:both + 8, :]
        wl, wa = ([jnp.where(lane8 < 16, turn(w, -16 * q), turn(own_w[q, rows, 0:128], 16)), None,
                   jnp.where(lane8 >= 112, turn(e, 112 - 16 * q), turn(own_w[q, rows, 128:256], 112))] for q in range(2))
        place_coef(pl.multiple_of(edge + base, 8), wl, wa, None, (0, 2))
        w, e = near_lon[0, n, 0:both, :], near_lon[1, n, 0:both, :]
        for j in range(HALF):
            r = edge + base + j
            middle = centre(r)
            for cut, keep, piece in ((slice(0, 128), lane < 16, turn(w, -16 * j)), (slice(256, 384), lane >= 112, turn(e, 112 - 16 * j))):
                even[0, r, :, cut] = jnp.where(keep[0:channels], piece[0:channels], even[0, r, :, cut])
                diag[r, :, cut] = jnp.where(keep[0:channels], piece[channels:] * scale + middle, diag[r, :, cut])
        return 0

    def place_halo(side, c):
        first = HALF * (1 - c) if side == 0 else HALF * c
        tile = tile_of(side, c)
        e0 = first if side == 0 else edge + lat + first
        inside = jnp.where(from_side(side), 1.0, 0.0).astype(f32)

        @pl.when(from_side(side))
        def _():
            for copy in lat_copies(side, c):
                copy.wait_recv()
            for ew in range(2):
                corner_copy(side, ew, c).wait_recv()

        def three(a, b, w, e, lanes, at):
            return (jnp.where(lanes < 16, turn(w, -at), turn(a, 16)), turn(jnp.where(lanes >= 64, a, b), 64),
                    jnp.where(lanes >= 112, turn(e, 112 - at), turn(b, 112)))

        west_strip, east_strip = near_corner.at[2 * side, tile], near_corner.at[2 * side + 1, tile]
        span = slice(first, first + 8)
        wl, wa = (three(near_lat_w[side, q, span, 0:128], near_lat_w[side, q, span, 128:256],
                        west_strip[both:both + 8, :], east_strip[both:both + 8, :], lane8, 16 * q) for q in range(2))
        place_coef(e0, wl, wa, inside, range(WINDOWS))
        for j in range(HALF):
            middle = centre(e0 + j)
            pieces = three(near_lat[side, first + j, :, 0:128], near_lat[side, first + j, :, 128:256],
                           west_strip[0:both, :], east_strip[0:both, :], lane, 16 * j)
            for t, piece in enumerate(pieces):
                cut = slice(128 * t, 128 * t + 128)
                even[0, e0 + j, :, cut] = piece[0:channels]
                diag[e0 + j, :, cut] = piece[channels:] * scale + middle

    def shift_of(k):
        theta = jnp.float32(THETA[0] * scale)
        for i in range(1, ITERS):
            theta = jnp.where(k == i, jnp.float32(THETA[i] * scale), theta)
        return theta

    def advance(src, dst, theta, starts):
        groups = [[e0 + GROUP * g + j for j in range(GROUP)] for e0 in starts for g in range(HALF // GROUP)]
        mixed, moved = [], []
        for picked in groups:
            stack = jnp.concatenate([src[e] for e in picked], axis=0)
            high = stack.astype(bf16)
            low = (stack - high.astype(f32)).astype(bf16)
            mixed.append(lax.dot_general(block[...], jnp.concatenate([high, low, high], axis=0), (((1,), (0,)), ((), ())),
                                         preferred_element_type=f32))
            sides = jnp.concatenate(
                [jnp.concatenate([high[:, 128 * t:128 * t + 128], low[:, 128 * t:128 * t + 128]], axis=1)
                 for t in range(WINDOWS)], axis=0)
            moved.append(lax.dot_general(sides, band[...], (((1,), (0,)), ((), ())), preferred_element_type=f32))
        for g, picked in enumerate(groups):
            for j, e in enumerate(picked):
                for t in range(WINDOWS):
                    cut = slice(128 * t, 128 * t + 128)
                    at = slice(size * t + channels * j, size * t + channels * (j + 1))

                    def weight(q):
                        return coef[e, q:q + 1, cut]

                    value = (diag[e, :, cut] - theta) * src[e, :, cut] + mixed[g][channels * j:channels * (j + 1), cut]
                    value = value + (coef[e, 0:1, 128:256] * moved[g][at, 0:128] + weight(1) * moved[g][at, 128:256])
                    value = value + weight(2) * src[e + 1, :, cut] + weight(3) * src[e - 1, :, cut]
                    dst[e, :, cut] = value + weight(4) * (src[e - 2, :, cut] - src[e + 2, :, cut])

    def two_levels(some):
        def run(n, _):
            some(2 * n, even.at[n], odd.at[n])
            some(2 * n + 1, odd.at[n], even.at[n + 1])
            return 0
        return run

    def interior(k, src, dst):
        theta = shift_of(k)

        def some(n, _):
            advance(src, dst, theta, (edge + 2 + 2 * k + HALF * n, edge + lat - 2 - HALF - 2 * k - HALF * n))
            return 0

        lax.fori_loop(0, jnp.where(k < 3, 2, 1), some, 0)

    def wedge(c):
        for k in range(ITERS):
            low = edge - HALF * (c + 1) + 2 + 2 * k
            for e0 in (low, rows_all - HALF - low):
                advance(field(k), field(k + 1), THETA[k] * scale, (e0,))

    def dots(lo, hi, spans):
        pairs = [(k, i) for k, i in PAIRS if lo <= k <= hi]

        def one(t, _):
            cut = pl.ds(pl.multiple_of(t * 128, 128), 128)
            acc = (jnp.zeros((8, 128), f32),) * len(pairs)
            for start, stop in spans:
                def part(n, acc):
                    acc = list(acc)
                    for j in range(4):
                        e = start + 4 * n + j
                        for h in range(channels // 8):
                            x = [field(k)[e, 8 * h:8 * h + 8, cut] for k in range(hi + 1)]
                            for n_, (k, i) in enumerate(pairs):
                                acc[n_] = acc[n_] + x[k] * x[i]
                    return tuple(acc)

                acc = lax.fori_loop(0, (stop - start) // 4, part, acc)
            low = jnp.where(t == 1, 32, 16)
            kept = (lane8 >= low) & (lane8 < 128 - low)
            for n, (k, i) in enumerate(pairs):
                at = k * (k + 1) // 2 + i
                gram_acc[at] = gram_acc[at] + jnp.where(kept, acc[n], 0.0)
            return 0

        lax.fori_loop(0, WINDOWS, one, 0)

    def rim_dots(first, last):
        for t in range(WINDOWS):
            cut = slice(128 * t, 128 * t + 128)
            acc = {}
            for p in range(HALF // 2):
                for e in (edge + 2 * p, edge + 2 * p + 1, edge + lat - 1 - 2 * p, edge + lat - 2 - 2 * p):
                    for h in range(channels // 8):
                        levels = range(first(p), last(p) + 1)
                        if not len(levels):
                            continue
                        x = [field(k)[e, 8 * h:8 * h + 8, cut] for k in range(last(p) + 1)]
                        for k in levels:
                            for i in range(k + 1):
                                term = x[k] * x[i]
                                acc[k, i] = acc[k, i] + term if (k, i) in acc else term
            low = 32 if t == 1 else 16
            kept = (lane8 >= low) & (lane8 < 128 - low)
            for (k, i), value in acc.items():
                at = k * (k + 1) // 2 + i
                gram_acc[at] = gram_acc[at] + jnp.where(kept, value, 0.0)

    for copy in winds:
        copy.wait()
    for q in range(2):
        half = own.at[:, pl.ds(q * channels, channels), :]
        pltpu.make_async_copy(half, half, load_sem.at[q]).wait()
    pl.semaphore_wait(barrier, len(close))
    tell(0)

    def send_lat(c):
        for side in range(2):
            @pl.when(has(side))
            def _():
                for copy in lat_copies(side, c):
                    copy.start()

    def send_corners(c):
        for side in range(2):
            @pl.when(has(side))
            def _():
                for ew in range(2):
                    corner_copy(side, ew, c).start()

    send_lat(0)
    lax.fori_loop(0, tiles, pack, 0)
    for ew in range(2):
        lon_copy(ew).start()
    hear(0)
    tell(1)
    send_corners(0)
    send_lat(1)
    send_corners(1)
    lax.fori_loop(0, tiles, place_own, 0)
    hear(1)
    tell(2)
    for ew in range(2):
        lon_copy(ew).wait_recv()
    lax.fori_loop(0, tiles, place_lon, 0)
    hear(2)
    tell(3)
    lax.fori_loop(0, ITERS // 2, two_levels(interior), 0)
    ready = ITERS // 2
    dots(0, ready, ((edge + HALF, edge + lat - HALF),))
    for c in range(2):
        for side in range(2):
            place_halo(side, c)
        wedge(c)
        if c == 0:
            dots(0, ready, ((edge, edge + HALF), (edge + lat - HALF, edge + lat)))
            dots(ready + 1, ITERS, ((edge + HALF, edge + lat - HALF),))
            rim_dots(lambda p: ready + 1, lambda p: ready + p)
    rim_dots(lambda p: ready + 1 + p, lambda p: ITERS)

    hear(3)
    sums = jnp.concatenate(
        [jnp.sum(gram_acc[n], axis=0, keepdims=True) for n in range(len(PAIRS))]
        + [jnp.zeros((128 - len(PAIRS), 128), f32)], axis=0)
    flat = lax.dot_general(jnp.ones((8, 128), f32), sums, (((1,), (1,)), ((), ())), precision=HI,
                           preferred_element_type=f32)
    mine[...] = flat[0:1, :]
    slots[total - 1] = flat[0:1, :]

    for n, (a, b) in enumerate(peers(nx, ny)):
        pltpu.make_async_remote_copy(
            src_ref=mine, dst_ref=slots.at[n], send_sem=red_sem.at[0], recv_sem=red_sem.at[1],
            device_id=(lax.rem(ix + a, nx), lax.rem(iy + b, ny)), device_id_type=MESH).start()
    arrived = slots.at[pl.ds(0, total - 1)]
    pltpu.make_async_copy(arrived, arrived, red_sem.at[1]).wait()
    pltpu.make_async_copy(arrived, arrived, red_sem.at[0]).wait()
    parts = [slots[n] for n in range(4)]
    for n in range(4, total):
        parts[n % 4] = parts[n % 4] + slots[n]
    whole = (parts[0] + parts[1]) + (parts[2] + parts[3])
    gram = [[None] * (ITERS + 1) for _ in range(ITERS + 1)]
    for n, (k, i) in enumerate(PAIRS):
        gram[k][i] = gram[i][k] = jnp.broadcast_to(whole[:, n:n + 1], (8, 128))
    answer, applied = small_solve(gram)
    for k in range(ITERS):
        splats[k] = answer[k]
    for k in range(ITERS + 1):
        splats[ITERS + k] = applied[k]

    for ew in range(2):
        lon_copy(ew).wait_send()
    for side in range(2):
        @pl.when(has(side))
        def _():
            for c in range(2):
                for copy in lat_copies(side, c):
                    copy.wait_send()
                for ew in range(2):
                    corner_copy(side, ew, c).wait_send()


def finish(even, odd, splats, sol_hbm, res_hbm, outs, out_sem):
    channels, lat, _ = sol_hbm.shape
    lane = lax.broadcasted_iota(jnp.int32, (8, 128), 1)
    quarter = lat // 4
    for r in range(lat):
        for h in range(channels // 8):
            sub = slice(8 * h, 8 * h + 8)
            best, rest = [], []
            for t in range(WINDOWS):
                cut = slice(128 * t, 128 * t + 128)
                x = even[0, HALO + r, sub, cut]
                up = splats[0] * x
                down = x - splats[ITERS] * x
                for k in range(1, ITERS + 1):
                    x = (odd if k % 2 else even)[k // 2, HALO + r, sub, cut]
                    if k < ITERS:
                        up = up + splats[k] * x
                    down = down - splats[ITERS + k] * x
                best.append(up)
                rest.append(down)
            for q, (a, b, c) in enumerate((best, rest)):
                b = pltpu.roll(b, 64, 1)
                spread = pl.ds(8 * h * lat + r, 8, stride=lat)
                outs[q, 0, spread, :] = jnp.where(lane < 96, pltpu.roll(a, 112, 1), b)
                outs[q, 1, spread, :] = jnp.where(lane < 32, b, pltpu.roll(c, 16, 1))
        if (r + 1) % quarter == 0:
            rows = pl.ds(r + 1 - quarter, quarter)
            for q, dst in enumerate((sol_hbm, res_hbm)):
                for t in range(2):
                    src = outs.at[q, t].reshape(channels, lat, 128)
                    pltpu.make_async_copy(src.at[:, rows, :], dst.at[:, rows, pl.ds(128 * t, 128)], out_sem.at[q]).start()
    for q, dst in enumerate((sol_hbm, res_hbm)):
        pltpu.make_async_copy(dst, dst, out_sem.at[q]).wait()


def solution(mesh):
    nx, ny = mesh.shape["gx"], mesh.shape["gy"]

    def per_device(forcing, damping, coupling, wind_lon, wind_lat):
        channels, lat, lon = forcing.shape
        f32 = jnp.float32
        vmem = pl.BlockSpec(memory_space=pltpu.VMEM)
        hbm = pl.BlockSpec(memory_space=pltpu.HBM)
        dma = pltpu.SemaphoreType.DMA
        shape = jax.ShapeDtypeStruct((channels, lat, lon), f32)
        rows_all, lanes = lat + 2 * HALO, 128 * WINDOWS
        packed = 2 * channels + 8
        even, odd, splats = pl.pallas_call(
            functools.partial(kernel, nx, ny),
            out_shape=(
                pltpu.VMEM((ITERS // 2 + 1, rows_all, channels, lanes), f32),
                pltpu.VMEM((ITERS // 2, rows_all, channels, lanes), f32),
                pltpu.VMEM((2 * ITERS + 1, 8, 128), f32),
            ),
            in_specs=[hbm, hbm, vmem, hbm, hbm],
            out_specs=(vmem, vmem, vmem),
            scratch_shapes=[
                pltpu.VMEM((rows_all, channels, lanes), f32),
                pltpu.VMEM((rows_all, 8, lanes), f32),
                pltpu.VMEM((rows_all, 128), f32),
                pltpu.VMEM((GROUP * channels, 3 * GROUP * channels), jnp.bfloat16),
                pltpu.VMEM((256, 256), jnp.bfloat16),
                pltpu.VMEM((lat, 2 * channels, lon), f32),
                pltpu.VMEM((2, HALO, 2 * channels, lon), f32),
                pltpu.VMEM((2, lat, lon), f32),
                pltpu.VMEM((2, 2, HALO, lon), f32),
                pltpu.VMEM((2, lat // HALF, packed, 128), f32),
                pltpu.VMEM((2, lat // HALF, packed, 128), f32),
                pltpu.VMEM((4, 2, packed, 128), f32),
                pltpu.VMEM((len(PAIRS), 8, 128), f32),
                pltpu.VMEM((1, 128), f32),
                pltpu.VMEM((nx * ny, 1, 128), f32),
                dma((2,)), dma((2,)),
                dma((2, 2, 3)), dma((2, 2, 3)), dma((2,)), dma((2,)), dma((4, 2)), dma((4, 2)), dma((2,)),
                pltpu.SemaphoreType.REGULAR((4,)),
            ],
            compiler_params=pltpu.CompilerParams(
                collective_id=0, has_side_effects=True, vmem_limit_bytes=52_800_000),
        )(forcing, damping, coupling, wind_lon, wind_lat)
        return pl.pallas_call(
            finish,
            out_shape=(shape, shape),
            in_specs=[vmem, vmem, vmem],
            out_specs=(hbm, hbm),
            scratch_shapes=[pltpu.VMEM((2, 2, channels * lat, 128), f32), dma((2,))],
            compiler_params=pltpu.CompilerParams(vmem_limit_bytes=16 * 1024 * 1024),
        )(even, odd, splats)

    return jax.shard_map(
        per_device,
        mesh=mesh,
        in_specs=(P(None, "gy", "gx"), P(None, "gy", "gx"), P(), P("gy", "gx"), P("gy", "gx")),
        out_specs=(P(None, "gy", "gx"), P(None, "gy", "gx")),
        check_vma=False,
    )
```

```python
import functools
import math

import jax
import jax.numpy as jnp
from jax import lax
from jax.experimental import pallas as pl
from jax.experimental.pallas import tpu as pltpu
from jax.sharding import PartitionSpec as P

ITERS = 8
COUPLE = 0.25
DIFF_LAT = 0.5
DIFF_LON = 0.5
GUARD = 1.0
MESH = pl.DeviceIdType.MESH
HI = lax.Precision.HIGHEST

MIDDLE = 9.0
RADIUS = 6.0
WIDTH = 3.0
THETA = [MIDDLE + RADIUS * math.cos(math.pi * (2 * k + 1) / (2 * ITERS)) for k in (7, 0, 4, 2, 6, 1, 5, 3)]
PAIRS = [(k, i) for k in range(ITERS + 1) for i in range(k + 1)]
GROUP = 4
HALO = 2 * ITERS
HALF = 8
WINDOWS = 3


def apply_to(coords):
    out = [None] * (len(coords) + 1)
    for k, value in enumerate(coords):
        low = THETA[k] * value if k < ITERS else value
        out[k] = low if out[k] is None else out[k] + low
        out[k + 1] = WIDTH * value
    return out


def small_solve(gram):
    first = jnp.sqrt(gram[0][0] + GUARD)
    coords = [[1.0 / first]]
    images = [[gram[i][0] * coords[0][0] for i in range(ITERS + 1)]]
    heights = []
    for j in range(ITERS):
        moved = apply_to(coords[j])
        column = []
        for i in range(j + 1):
            column.append(functools.reduce(lambda a, b: a + b, [images[i][k] * moved[k] for k in range(j + 2)]))
        left = list(moved)
        for i in range(j + 1):
            for k in range(i + 1):
                left[k] = left[k] - column[i] * coords[i][k]
        image = [
            functools.reduce(lambda a, b: a + b, [gram[r][k] * left[k] for k in range(j + 2)])
            for r in range(ITERS + 1)
        ]
        norm_sq = functools.reduce(lambda a, b: a + b, [image[k] * left[k] for k in range(j + 2)])
        subdiag = jnp.sqrt(jnp.maximum(norm_sq, 0.0) + GUARD)
        column.append(subdiag)
        heights.append(column)
        inverse = 1.0 / subdiag
        coords.append([v * inverse for v in left])
        images.append([v * inverse for v in image])
    cosines, sines, target, rotated = [], [], [first], []
    for j in range(ITERS):
        column = list(heights[j])
        for e in range(j):
            upper, lower = column[e], column[e + 1]
            column[e] = cosines[e] * upper + sines[e] * lower
            column[e + 1] = cosines[e] * lower - sines[e] * upper
        upper, lower = column[j], column[j + 1]
        radius = jnp.sqrt(upper * upper + lower * lower)
        inverse = 1.0 / radius
        cosine, sine = upper * inverse, lower * inverse
        column[j] = radius
        kept = target[j]
        target[j] = cosine * kept
        target.append(-sine * kept)
        cosines.append(cosine)
        sines.append(sine)
        rotated.append(column)
    weights = [None] * ITERS
    for j in reversed(range(ITERS)):
        value = target[j]
        for later in range(j + 1, ITERS):
            value = value - rotated[later][j] * weights[later]
        weights[j] = value / rotated[j][j]
    answer = [None] * ITERS
    for j in range(ITERS):
        for k in range(j + 1):
            term = weights[j] * coords[j][k]
            answer[k] = term if answer[k] is None else answer[k] + term
    return answer, apply_to(answer)


def distance(n, o):
    return min(o, n - o)


def peers(nx, ny):
    inner = 4 if ny % 4 == 0 else 1
    offsets = [(a, b) for a in range(nx) for b in range(ny) if (a, b) != (0, 0)]

    def hops(offset):
        a, b = offset
        return distance(nx // 2 or 1, a // 2) + distance(inner, b % inner) + distance(ny // inner, b // inner)

    return sorted(offsets, key=lambda offset: (-hops(offset), offset))


def kernel(nx, ny, f_hbm, d_hbm, c_ref, wl_hbm, wa_hbm, even, odd, splats,
           diag, coef, kxs, block, band, own, near_lat, own_w, near_lat_w, packed, near_lon, near_corner,
           gram_acc, mine, slots,
           load_sem, lat_send, lat_recv, lon_send, lon_recv, red_sem, known):
    channels, lat, lon = f_hbm.shape
    both = 2 * channels
    total = nx * ny
    f32, bf16 = jnp.float32, jnp.bfloat16
    ix, iy = lax.axis_index("gx"), lax.axis_index("gy")
    east, west = lax.rem(ix + 1, nx), lax.rem(ix + nx - 1, nx)
    scale = 1.0 / WIDTH
    size = GROUP * channels
    edge = HALO
    rows_all = lat + 2 * HALO
    tiles = lat // HALF

    def field(k):
        return even.at[k // 2] if k % 2 == 0 else odd.at[k // 2]

    barrier = pltpu.get_barrier_semaphore()

    def greet(sem, a, b):
        pl.semaphore_signal(sem, inc=1, device_id=(lax.rem(ix + a, nx), lax.rem(iy + b, ny)), device_id_type=MESH)

    close = [(0, 1), (0, ny - 1), (1, 0), (nx - 1, 0)]
    rounds = [
        close,
        close + [(0, 2), (0, ny - 2), (2, 0), (nx - 2, 0)],
        [(0, b) for b in range(1, 5)] + [(0, ny - b) for b in range(1, 5)],
        [(a, 0) for a in range(1, nx)],
    ]
    for a, b in close:
        greet(barrier, a, b)

    def tell(n):
        for a, b in rounds[n]:
            greet(known.at[n], a, b)

    def hear(n):
        pl.semaphore_wait(known.at[n], len(rounds[n]))

    winds = [pltpu.make_async_copy(wl_hbm, own_w.at[0], load_sem.at[1]), pltpu.make_async_copy(wa_hbm, own_w.at[1], load_sem.at[1])]
    for copy in winds:
        copy.start()
    for c in range(channels):
        for q, src in enumerate((f_hbm, d_hbm)):
            pltpu.make_async_copy(src.at[c], own.at[:, q * channels + c, :], load_sem.at[0]).start()

    def spread(n):
        row = lax.broadcasted_iota(jnp.int32, (n, channels), 0)
        col = lax.broadcasted_iota(jnp.int32, (n, channels), 1)
        return jnp.where(lax.rem(row, channels) == col, 1.0, 0.0).astype(f32)

    wide = lax.dot_general(spread(size), c_ref[...], (((1,), (0,)), ((), ())), precision=HI, preferred_element_type=f32)
    wide = lax.dot_general(wide, spread(3 * size), (((1,), (1,)), ((), ())), precision=HI,
                           preferred_element_type=f32) * (COUPLE * scale)
    down = lax.broadcasted_iota(jnp.int32, (size, 3 * size), 0)
    across = lax.broadcasted_iota(jnp.int32, (size, 3 * size), 1)
    high = wide.astype(bf16).astype(f32)
    wide = jnp.where(across < 2 * size, high, wide - high)
    block[...] = jnp.where(down // channels == lax.rem(across, size) // channels, wide, 0.0).astype(bf16)
    down = lax.broadcasted_iota(jnp.int32, (256, 256), 0)
    across = lax.broadcasted_iota(jnp.int32, (256, 256), 1)
    shift = lax.rem(down, 128) - lax.rem(across, 128)
    sums = jnp.where((shift == 1) | (shift == -1), 1.0, 0.0)
    slopes = jnp.where(shift == 1, 8.0, 0.0) + jnp.where(shift == -1, -8.0, 0.0)
    slopes = slopes + jnp.where(shift == 2, -1.0, 0.0) + jnp.where(shift == -2, 1.0, 0.0)
    band[...] = jnp.where(across < 128, sums, slopes).astype(bf16)
    row_pos = (lax.broadcasted_iota(jnp.int32, (rows_all, 128), 0) + (iy * lat - edge)).astype(f32)
    phi = -math.pi / 2 + (row_pos + 0.5) * (math.pi / (lat * ny))
    kxs[...] = (DIFF_LON * scale) / (jnp.cos(phi) ** 2 + 0.1)
    gram_acc[...] = jnp.zeros(gram_acc.shape, f32)

    @pl.when(iy == 0)
    def _():
        near_lat[0] = jnp.zeros(near_lat.shape[1:], f32)
        near_lat_w[0] = jnp.zeros(near_lat_w.shape[1:], f32)
        near_corner[0] = jnp.zeros(near_corner.shape[1:], f32)
        near_corner[1] = jnp.zeros(near_corner.shape[1:], f32)

    @pl.when(iy == ny - 1)
    def _():
        near_lat[1] = jnp.zeros(near_lat.shape[1:], f32)
        near_lat_w[1] = jnp.zeros(near_lat_w.shape[1:], f32)
        near_corner[2] = jnp.zeros(near_corner.shape[1:], f32)
        near_corner[3] = jnp.zeros(near_corner.shape[1:], f32)

    def lat_copies(side, c):
        first = HALF * (1 - c) if side == 0 else HALF * c
        base = lat - HALO if side == 0 else 0
        to = (ix, iy + 1) if side == 0 else (ix, iy - 1)
        if c == 0:
            parts = [(first, HALF, 0, both)]
        elif side == 0:
            parts = [(first + 2, HALF - 2, 0, both), (first, 2, 0, channels)]
        else:
            parts = [(first, HALF - 2, 0, both), (first + HALF - 2, 2, 0, channels)]
        out = []
        for n, (start, count, sub, subs) in enumerate(parts):
            out.append(pltpu.make_async_remote_copy(
                src_ref=own.at[pl.ds(base + start, count), pl.ds(sub, subs), :],
                dst_ref=near_lat.at[side, pl.ds(start, count), pl.ds(sub, subs), :],
                send_sem=lat_send.at[side], recv_sem=lat_recv.at[side, c], device_id=to, device_id_type=MESH))
        out.append(pltpu.make_async_remote_copy(
            src_ref=own_w.at[:, pl.ds(base + first, HALF), :], dst_ref=near_lat_w.at[side, :, pl.ds(first, HALF), :],
            send_sem=lat_send.at[side], recv_sem=lat_recv.at[side, c], device_id=to, device_id_type=MESH))
        return out

    def tile_of(side, c):
        return 1 - c if side == 0 else c

    def corner_copy(side, ew, c):
        slot, tile = 2 * side + ew, tile_of(side, c)
        return pltpu.make_async_remote_copy(
            src_ref=packed.at[ew, tile + (tiles - 2 if side == 0 else 0)], dst_ref=near_corner.at[slot, tile],
            send_sem=lat_send.at[side], recv_sem=lat_recv.at[side, c],
            device_id=(east if ew == 0 else west, iy + 1 if side == 0 else iy - 1), device_id_type=MESH)

    def lon_copy(ew):
        return pltpu.make_async_remote_copy(
            src_ref=packed.at[ew], dst_ref=near_lon.at[ew], send_sem=lon_send.at[ew], recv_sem=lon_recv.at[ew],
            device_id=(east if ew == 0 else west, iy), device_id_type=MESH)

    def has(side):
        return iy < ny - 1 if side == 0 else iy > 0

    def from_side(side):
        return iy > 0 if side == 0 else iy < ny - 1

    lane = lax.broadcasted_iota(jnp.int32, (both, 128), 1)
    lane8 = lax.broadcasted_iota(jnp.int32, (8, 128), 1)

    def turn(x, n):
        n = n % 128
        return pltpu.roll(x, n, 1) if n else x

    def pack(n, _):
        for ew in range(2):
            cut = slice(lon - 128, lon) if ew == 0 else slice(0, 128)
            start = 112 if ew == 0 else 0
            base = HALF * n
            strip = turn(own[base, :, cut], -start)
            for j in range(1, HALF):
                strip = jnp.where((lane >= 16 * j) & (lane < 16 * j + 16), turn(own[base + j, :, cut], 16 * j - start), strip)
            packed[ew, n, 0:both, :] = strip
            rows = pl.ds(pl.multiple_of(base, 8), 8)
            packed[ew, n, both:both + 8, :] = jnp.where(
                lane8 < 16, turn(own_w[0, rows, cut], -start), turn(own_w[1, rows, cut], 16 - start))
        return 0

    def place_coef(e0, wl, wa, inside, chosen):
        kx = kxs[pl.ds(e0, 8), :]
        for t in chosen:
            cut = slice(128 * t, 128 * t + 128)
            l, a = wl[t] * (scale / 12.0), wa[t] * (scale / 12.0)
            planes = [-kx, l, 8.0 * a - DIFF_LAT * scale, -8.0 * a - DIFF_LAT * scale, a]
            for q, plane in enumerate(planes):
                if q == 0 and t != 1:
                    continue
                if inside is not None:
                    plane = plane * inside
                for j in range(8):
                    coef[e0 + j, q:q + 1, cut] = plane[j:j + 1, :]

    def centre(e):
        return (1.0 + 2.0 * DIFF_LAT) * scale - 2.0 * coef[e, 0:1, 128:256]

    def place_own(n, _):
        base = HALF * n
        rows = pl.ds(pl.multiple_of(base, 8), 8)
        wl, wa = ([None, turn(jnp.where(lane8 >= 64, own_w[q, rows, 0:128], own_w[q, rows, 128:256]), 64), None] for q in range(2))
        place_coef(pl.multiple_of(edge + base, 8), wl, wa, None, (1,))
        for j in range(HALF):
            r = base + j
            e = edge + r
            a, b = own[r, :, 0:128], own[r, :, 128:256]
            middle = centre(e)
            for t, piece in enumerate((turn(a, 16), turn(jnp.where(lane >= 64, a, b), 64), turn(b, 112))):
                cut = slice(128 * t, 128 * t + 128)
                even[0, e, :, cut] = piece[0:channels]
                diag[e, :, cut] = piece[channels:] * scale + middle
        return 0

    def place_lon(n, _):
        base = HALF * n
        rows = pl.ds(pl.multiple_of(base, 8), 8)
        w, e = near_lon[0, n, both:both + 8, :], near_lon[1, n, both:both + 8, :]
        wl, wa = ([jnp.where(lane8 < 16, turn(w, -16 * q), turn(own_w[q, rows, 0:128], 16)), None,
                   jnp.where(lane8 >= 112, turn(e, 112 - 16 * q), turn(own_w[q, rows, 128:256], 112))] for q in range(2))
        place_coef(pl.multiple_of(edge + base, 8), wl, wa, None, (0, 2))
        w, e = near_lon[0, n, 0:both, :], near_lon[1, n, 0:both, :]
        for j in range(HALF):
            r = edge + base + j
            middle = centre(r)
            for cut, keep, piece in ((slice(0, 128), lane < 16, turn(w, -16 * j)), (slice(256, 384), lane >= 112, turn(e, 112 - 16 * j))):
                even[0, r, :, cut] = jnp.where(keep[0:channels], piece[0:channels], even[0, r, :, cut])
                diag[r, :, cut] = jnp.where(keep[0:channels], piece[channels:] * scale + middle, diag[r, :, cut])
        return 0

    def place_halo(side, c):
        first = HALF * (1 - c) if side == 0 else HALF * c
        tile = tile_of(side, c)
        e0 = first if side == 0 else edge + lat + first
        inside = jnp.where(from_side(side), 1.0, 0.0).astype(f32)

        @pl.when(from_side(side))
        def _():
            whole = diag.at[pl.ds(0, 13)] if c == 0 else coef.at[pl.ds(0, 35), :, pl.ds(0, 256)]
            pltpu.make_async_copy(whole, whole, lat_recv.at[side, c]).wait()

        def three(a, b, w, e, lanes, at):
            return (jnp.where(lanes < 16, turn(w, -at), turn(a, 16)), turn(jnp.where(lanes >= 64, a, b), 64),
                    jnp.where(lanes >= 112, turn(e, 112 - at), turn(b, 112)))

        west_strip, east_strip = near_corner.at[2 * side, tile], near_corner.at[2 * side + 1, tile]
        span = slice(first, first + 8)
        wl, wa = (three(near_lat_w[side, q, span, 0:128], near_lat_w[side, q, span, 128:256],
                        west_strip[both:both + 8, :], east_strip[both:both + 8, :], lane8, 16 * q) for q in range(2))
        place_coef(e0, wl, wa, inside, range(WINDOWS))
        for j in range(HALF):
            middle = centre(e0 + j)
            pieces = three(near_lat[side, first + j, :, 0:128], near_lat[side, first + j, :, 128:256],
                           west_strip[0:both, :], east_strip[0:both, :], lane, 16 * j)
            for t, piece in enumerate(pieces):
                cut = slice(128 * t, 128 * t + 128)
                even[0, e0 + j, :, cut] = piece[0:channels]
                diag[e0 + j, :, cut] = piece[channels:] * scale + middle

    def shift_of(k):
        theta = jnp.float32(THETA[0] * scale)
        for i in range(1, ITERS):
            theta = jnp.where(k == i, jnp.float32(THETA[i] * scale), theta)
        return theta

    def advance(src, dst, theta, starts):
        groups = [[e0 + GROUP * g + j for j in range(GROUP)] for e0 in starts for g in range(HALF // GROUP)]
        mixed, moved = [], []
        for picked in groups:
            stack = jnp.concatenate([src[e] for e in picked], axis=0)
            high = stack.astype(bf16)
            low = (stack - high.astype(f32)).astype(bf16)
            mixed.append(lax.dot_general(block[...], jnp.concatenate([high, low, high], axis=0), (((1,), (0,)), ((), ())),
                                         preferred_element_type=f32))
            sides = jnp.concatenate(
                [jnp.concatenate([high[:, 128 * t:128 * t + 128], low[:, 128 * t:128 * t + 128]], axis=1)
                 for t in range(WINDOWS)], axis=0)
            moved.append(lax.dot_general(sides, band[...], (((1,), (0,)), ((), ())), preferred_element_type=f32))
        for g, picked in enumerate(groups):
            for j, e in enumerate(picked):
                for t in range(WINDOWS):
                    cut = slice(128 * t, 128 * t + 128)
                    at = slice(size * t + channels * j, size * t + channels * (j + 1))

                    def weight(q):
                        return coef[e, q:q + 1, cut]

                    value = (diag[e, :, cut] - theta) * src[e, :, cut] + mixed[g][channels * j:channels * (j + 1), cut]
                    value = value + (coef[e, 0:1, 128:256] * moved[g][at, 0:128] + weight(1) * moved[g][at, 128:256])
                    value = value + weight(2) * src[e + 1, :, cut] + weight(3) * src[e - 1, :, cut]
                    dst[e, :, cut] = value + weight(4) * (src[e - 2, :, cut] - src[e + 2, :, cut])

    def two_levels(some):
        def run(n, _):
            some(2 * n, even.at[n], odd.at[n])
            some(2 * n + 1, odd.at[n], even.at[n + 1])
            return 0
        return run

    def interior(k, src, dst):
        theta = shift_of(k)

        def some(n, _):
            advance(src, dst, theta, (edge + 2 + 2 * k + HALF * n, edge + lat - 2 - HALF - 2 * k - HALF * n))
            return 0

        lax.fori_loop(0, jnp.where(k < 3, 2, 1), some, 0)

    def wedge(c):
        for k in range(ITERS):
            low = edge - HALF * (c + 1) + 2 + 2 * k
            for e0 in (low, rows_all - HALF - low):
                advance(field(k), field(k + 1), THETA[k] * scale, (e0,))

    def dots(lo, hi, spans):
        pairs = [(k, i) for k, i in PAIRS if lo <= k <= hi]

        def one(t, _):
            cut = pl.ds(pl.multiple_of(t * 128, 128), 128)
            acc = (jnp.zeros((8, 128), f32),) * len(pairs)
            for start, stop in spans:
                def part(n, acc):
                    acc = list(acc)
                    for j in range(4):
                        e = start + 4 * n + j
                        for h in range(channels // 8):
                            x = [field(k)[e, 8 * h:8 * h + 8, cut] for k in range(hi + 1)]
                            for n_, (k, i) in enumerate(pairs):
                                acc[n_] = acc[n_] + x[k] * x[i]
                    return tuple(acc)

                acc = lax.fori_loop(0, (stop - start) // 4, part, acc)
            low = jnp.where(t == 1, 32, 16)
            kept = (lane8 >= low) & (lane8 < 128 - low)
            for n, (k, i) in enumerate(pairs):
                at = k * (k + 1) // 2 + i
                gram_acc[at] = gram_acc[at] + jnp.where(kept, acc[n], 0.0)
            return 0

        lax.fori_loop(0, WINDOWS, one, 0)

    def rim_dots(first, last):
        for t in range(WINDOWS):
            cut = slice(128 * t, 128 * t + 128)
            acc = {}
            for p in range(HALF // 2):
                for e in (edge + 2 * p, edge + 2 * p + 1, edge + lat - 1 - 2 * p, edge + lat - 2 - 2 * p):
                    for h in range(channels // 8):
                        levels = range(first(p), last(p) + 1)
                        if not len(levels):
                            continue
                        x = [field(k)[e, 8 * h:8 * h + 8, cut] for k in range(last(p) + 1)]
                        for k in levels:
                            for i in range(k + 1):
                                term = x[k] * x[i]
                                acc[k, i] = acc[k, i] + term if (k, i) in acc else term
            low = 32 if t == 1 else 16
            kept = (lane8 >= low) & (lane8 < 128 - low)
            for (k, i), value in acc.items():
                at = k * (k + 1) // 2 + i
                gram_acc[at] = gram_acc[at] + jnp.where(kept, value, 0.0)

    pltpu.make_async_copy(own_w, own_w, load_sem.at[1]).wait()
    pltpu.make_async_copy(own, own, load_sem.at[0]).wait()
    pl.semaphore_wait(barrier, len(close))
    tell(0)

    def send_lat(c):
        for side in range(2):
            @pl.when(has(side))
            def _():
                for copy in lat_copies(side, c):
                    copy.start()

    def send_corners(c):
        for side in range(2):
            @pl.when(has(side))
            def _():
                for ew in range(2):
                    corner_copy(side, ew, c).start()

    send_lat(0)
    lax.fori_loop(0, tiles, pack, 0)
    for ew in range(2):
        lon_copy(ew).start()
    hear(0)
    tell(1)
    send_corners(0)
    send_lat(1)
    send_corners(1)
    lax.fori_loop(0, tiles, place_own, 0)
    for ew in range(2):
        lon_copy(ew).wait_recv()
    lax.fori_loop(0, tiles, place_lon, 0)
    lax.fori_loop(0, ITERS // 2, two_levels(interior), 0)
    hear(1)
    tell(2)
    ready = ITERS // 2
    dots(0, ready, ((edge + HALF, edge + lat - HALF),))
    for c in range(2):
        for side in range(2):
            place_halo(side, c)
        wedge(c)
        if c == 0:
            hear(2)
            tell(3)
            dots(0, ready, ((edge, edge + HALF), (edge + lat - HALF, edge + lat)))
            dots(ready + 1, ITERS, ((edge + HALF, edge + lat - HALF),))
            rim_dots(lambda p: ready + 1, lambda p: ready + p)
    rim_dots(lambda p: ready + 1 + p, lambda p: ITERS)

    hear(3)
    sums = jnp.concatenate(
        [jnp.sum(gram_acc[n], axis=0, keepdims=True) for n in range(len(PAIRS))]
        + [jnp.zeros((128 - len(PAIRS), 128), f32)], axis=0)
    flat = lax.dot_general(jnp.ones((8, 128), f32), sums, (((1,), (1,)), ((), ())), precision=HI,
                           preferred_element_type=f32)
    mine[...] = flat[0:1, :]
    slots[total - 1] = flat[0:1, :]

    for n, (a, b) in enumerate(peers(nx, ny)):
        pltpu.make_async_remote_copy(
            src_ref=mine, dst_ref=slots.at[n], send_sem=red_sem.at[0], recv_sem=red_sem.at[1],
            device_id=(lax.rem(ix + a, nx), lax.rem(iy + b, ny)), device_id_type=MESH).start()
    arrived = slots.at[pl.ds(0, total - 1)]
    pltpu.make_async_copy(arrived, arrived, red_sem.at[1]).wait()
    pltpu.make_async_copy(arrived, arrived, red_sem.at[0]).wait()
    parts = [slots[n] for n in range(4)]
    for n in range(4, total):
        parts[n % 4] = parts[n % 4] + slots[n]
    whole = (parts[0] + parts[1]) + (parts[2] + parts[3])
    gram = [[None] * (ITERS + 1) for _ in range(ITERS + 1)]
    for n, (k, i) in enumerate(PAIRS):
        gram[k][i] = gram[i][k] = jnp.broadcast_to(whole[:, n:n + 1], (8, 128))
    answer, applied = small_solve(gram)
    for k in range(ITERS):
        splats[k] = answer[k]
    for k in range(ITERS + 1):
        splats[ITERS + k] = applied[k]

    for ew in range(2):
        lon_copy(ew).wait_send()
    for side in range(2):
        @pl.when(has(side))
        def _():
            whole = even.at[0, pl.ds(0, 37), :, pl.ds(0, 256)]
            pltpu.make_async_copy(whole, whole, lat_send.at[side]).wait()


def finish(even, odd, splats, sol_hbm, res_hbm, outs, out_sem):
    channels, lat, _ = sol_hbm.shape
    lane = lax.broadcasted_iota(jnp.int32, (8, 128), 1)
    quarter = lat // 4
    for r in range(lat):
        for h in range(channels // 8):
            sub = slice(8 * h, 8 * h + 8)
            best, rest = [], []
            for t in range(WINDOWS):
                cut = slice(128 * t, 128 * t + 128)
                x = even[0, HALO + r, sub, cut]
                up = splats[0] * x
                down = x - splats[ITERS] * x
                for k in range(1, ITERS + 1):
                    x = (odd if k % 2 else even)[k // 2, HALO + r, sub, cut]
                    if k < ITERS:
                        up = up + splats[k] * x
                    down = down - splats[ITERS + k] * x
                best.append(up)
                rest.append(down)
            for q, (a, b, c) in enumerate((best, rest)):
                b = pltpu.roll(b, 64, 1)
                spread = pl.ds(8 * h * lat + r, 8, stride=lat)
                outs[q, 0, spread, :] = jnp.where(lane < 96, pltpu.roll(a, 112, 1), b)
                outs[q, 1, spread, :] = jnp.where(lane < 32, b, pltpu.roll(c, 16, 1))
        if (r + 1) % quarter == 0:
            rows = pl.ds(r + 1 - quarter, quarter)
            for q, dst in enumerate((sol_hbm, res_hbm)):
                for t in range(2):
                    src = outs.at[q, t].reshape(channels, lat, 128)
                    pltpu.make_async_copy(src.at[:, rows, :], dst.at[:, rows, pl.ds(128 * t, 128)], out_sem.at[q]).start()
    for q, dst in enumerate((sol_hbm, res_hbm)):
        pltpu.make_async_copy(dst, dst, out_sem.at[q]).wait()


def solution(mesh):
    nx, ny = mesh.shape["gx"], mesh.shape["gy"]

    def per_device(forcing, damping, coupling, wind_lon, wind_lat):
        channels, lat, lon = forcing.shape
        f32 = jnp.float32
        vmem = pl.BlockSpec(memory_space=pltpu.VMEM)
        hbm = pl.BlockSpec(memory_space=pltpu.HBM)
        dma = pltpu.SemaphoreType.DMA
        shape = jax.ShapeDtypeStruct((channels, lat, lon), f32)
        rows_all, lanes = lat + 2 * HALO, 128 * WINDOWS
        packed = 2 * channels + 8
        even, odd, splats = pl.pallas_call(
            functools.partial(kernel, nx, ny),
            out_shape=(
                pltpu.VMEM((ITERS // 2 + 1, rows_all, channels, lanes), f32),
                pltpu.VMEM((ITERS // 2, rows_all, channels, lanes), f32),
                pltpu.VMEM((2 * ITERS + 1, 8, 128), f32),
            ),
            in_specs=[hbm, hbm, vmem, hbm, hbm],
            out_specs=(vmem, vmem, vmem),
            scratch_shapes=[
                pltpu.VMEM((rows_all, channels, lanes), f32),
                pltpu.VMEM((rows_all, 8, lanes), f32),
                pltpu.VMEM((rows_all, 128), f32),
                pltpu.VMEM((GROUP * channels, 3 * GROUP * channels), jnp.bfloat16),
                pltpu.VMEM((256, 256), jnp.bfloat16),
                pltpu.VMEM((lat, 2 * channels, lon), f32),
                pltpu.VMEM((2, HALO, 2 * channels, lon), f32),
                pltpu.VMEM((2, lat, lon), f32),
                pltpu.VMEM((2, 2, HALO, lon), f32),
                pltpu.VMEM((2, lat // HALF, packed, 128), f32),
                pltpu.VMEM((2, lat // HALF, packed, 128), f32),
                pltpu.VMEM((4, 2, packed, 128), f32),
                pltpu.VMEM((len(PAIRS), 8, 128), f32),
                pltpu.VMEM((1, 128), f32),
                pltpu.VMEM((nx * ny, 1, 128), f32),
                dma((2,)),
                dma((2,)), dma((2, 2)), dma((2,)), dma((2,)), dma((2,)),
                pltpu.SemaphoreType.REGULAR((4,)),
            ],
            compiler_params=pltpu.CompilerParams(
                collective_id=0, has_side_effects=True, vmem_limit_bytes=52_800_000),
        )(forcing, damping, coupling, wind_lon, wind_lat)
        return pl.pallas_call(
            finish,
            out_shape=(shape, shape),
            in_specs=[vmem, vmem, vmem],
            out_specs=(hbm, hbm),
            scratch_shapes=[pltpu.VMEM((2, 2, channels * lat, 128), f32), dma((2,))],
            compiler_params=pltpu.CompilerParams(vmem_limit_bytes=16 * 1024 * 1024),
        )(even, odd, splats)

    return jax.shard_map(
        per_device,
        mesh=mesh,
        in_specs=(P(None, "gy", "gx"), P(None, "gy", "gx"), P(), P("gy", "gx"), P("gy", "gx")),
        out_specs=(P(None, "gy", "gx"), P(None, "gy", "gx")),
        check_vma=False,
    )
```

```python
import functools
import math

import jax
import jax.numpy as jnp
from jax import lax
from jax.experimental import pallas as pl
from jax.experimental.pallas import tpu as pltpu
from jax.sharding import PartitionSpec as P

ITERS = 8
COUPLE = 0.25
DIFF_LAT = 0.5
DIFF_LON = 0.5
GUARD = 1.0
MESH = pl.DeviceIdType.MESH
HI = lax.Precision.HIGHEST

MIDDLE = 9.0
RADIUS = 6.0
WIDTH = 3.0
THETA = [MIDDLE + RADIUS * math.cos(math.pi * (2 * k + 1) / (2 * ITERS)) for k in (7, 0, 4, 2, 6, 1, 5, 3)]
PAIRS = [(k, i) for k in range(ITERS + 1) for i in range(k + 1)]
GROUP = 4
HALO = 2 * ITERS
HALF = 8
WINDOWS = 3


def apply_to(coords):
    out = [None] * (len(coords) + 1)
    for k, value in enumerate(coords):
        low = THETA[k] * value if k < ITERS else value
        out[k] = low if out[k] is None else out[k] + low
        out[k + 1] = WIDTH * value
    return out


def small_solve(gram):
    first = jnp.sqrt(gram[0][0] + GUARD)
    coords = [[1.0 / first]]
    images = [[gram[i][0] * coords[0][0] for i in range(ITERS + 1)]]
    heights = []
    for j in range(ITERS):
        moved = apply_to(coords[j])
        column = []
        for i in range(j + 1):
            column.append(functools.reduce(lambda a, b: a + b, [images[i][k] * moved[k] for k in range(j + 2)]))
        left = list(moved)
        for i in range(j + 1):
            for k in range(i + 1):
                left[k] = left[k] - column[i] * coords[i][k]
        image = [
            functools.reduce(lambda a, b: a + b, [gram[r][k] * left[k] for k in range(j + 2)])
            for r in range(ITERS + 1)
        ]
        norm_sq = functools.reduce(lambda a, b: a + b, [image[k] * left[k] for k in range(j + 2)])
        subdiag = jnp.sqrt(jnp.maximum(norm_sq, 0.0) + GUARD)
        column.append(subdiag)
        heights.append(column)
        inverse = 1.0 / subdiag
        coords.append([v * inverse for v in left])
        images.append([v * inverse for v in image])
    cosines, sines, target, rotated = [], [], [first], []
    for j in range(ITERS):
        column = list(heights[j])
        for e in range(j):
            upper, lower = column[e], column[e + 1]
            column[e] = cosines[e] * upper + sines[e] * lower
            column[e + 1] = cosines[e] * lower - sines[e] * upper
        upper, lower = column[j], column[j + 1]
        radius = jnp.sqrt(upper * upper + lower * lower)
        inverse = 1.0 / radius
        cosine, sine = upper * inverse, lower * inverse
        column[j] = radius
        kept = target[j]
        target[j] = cosine * kept
        target.append(-sine * kept)
        cosines.append(cosine)
        sines.append(sine)
        rotated.append(column)
    weights = [None] * ITERS
    for j in reversed(range(ITERS)):
        value = target[j]
        for later in range(j + 1, ITERS):
            value = value - rotated[later][j] * weights[later]
        weights[j] = value / rotated[j][j]
    answer = [None] * ITERS
    for j in range(ITERS):
        for k in range(j + 1):
            term = weights[j] * coords[j][k]
            answer[k] = term if answer[k] is None else answer[k] + term
    return answer, apply_to(answer)


def distance(n, o):
    return min(o, n - o)


def peers(nx, ny):
    inner = 4 if ny % 4 == 0 else 1
    offsets = [(a, b) for a in range(nx) for b in range(ny) if (a, b) != (0, 0)]

    def hops(offset):
        a, b = offset
        return distance(nx // 2 or 1, a // 2) + distance(inner, b % inner) + distance(ny // inner, b // inner)

    return sorted(offsets, key=lambda offset: (-hops(offset), offset))


def kernel(nx, ny, f_hbm, d_hbm, c_ref, wl_hbm, wa_hbm, even, odd, splats,
           diag, coef, kxs, block, band, own, near_lat, own_w, near_lat_w, packed, near_lon, near_corner,
           gram_acc, mine, slots,
           load_sem, lat_send, lat_recv, lon_send, lon_recv, red_sem, known):
    channels, lat, lon = f_hbm.shape
    both = 2 * channels
    total = nx * ny
    f32, bf16 = jnp.float32, jnp.bfloat16
    ix, iy = lax.axis_index("gx"), lax.axis_index("gy")
    east, west = lax.rem(ix + 1, nx), lax.rem(ix + nx - 1, nx)
    scale = 1.0 / WIDTH
    size = GROUP * channels
    edge = HALO
    rows_all = lat + 2 * HALO
    tiles = lat // HALF

    def field(k):
        return even.at[k // 2] if k % 2 == 0 else odd.at[k // 2]

    barrier = pltpu.get_barrier_semaphore()

    def greet(sem, a, b):
        def signal():
            pl.semaphore_signal(sem, inc=1, device_id=(lax.rem(ix + a, nx), iy + b), device_id_type=MESH)

        if b == 0:
            signal()
        else:
            pl.when(iy + b < ny if b > 0 else iy + b >= 0)(signal)

    def line(n):
        return [(0, b) for b in range(1, n + 1)] + [(0, -b) for b in range(1, n + 1)]

    def ring(n):
        return [(a, 0) for a in range(1, n + 1)] + [(nx - a, 0) for a in range(1, n + 1)]

    def answers(offsets):
        fixed = sum(1 for _, b in offsets if b == 0)
        reach = max(b for _, b in offsets)
        return fixed + jnp.minimum(ny - 1 - iy, reach) + jnp.minimum(iy, reach)

    close = line(1) + ring(1)
    rounds = [line(1), ring(1), line(2) + ring(2), line(4), line(8), [(a, 0) for a in range(1, nx)]]
    for a, b in close:
        greet(barrier, a, b)

    def tell(n):
        for a, b in rounds[n]:
            greet(known.at[n], a, b)

    def hear(n):
        pl.semaphore_wait(known.at[n], answers(rounds[n]))

    winds = [pltpu.make_async_copy(wl_hbm, own_w.at[0], load_sem.at[1]), pltpu.make_async_copy(wa_hbm, own_w.at[1], load_sem.at[1])]
    for copy in winds:
        copy.start()
    for c in range(channels):
        for q, src in enumerate((f_hbm, d_hbm)):
            pltpu.make_async_copy(src.at[c], own.at[:, q * channels + c, :], load_sem.at[0]).start()

    def spread(n):
        row = lax.broadcasted_iota(jnp.int32, (n, channels), 0)
        col = lax.broadcasted_iota(jnp.int32, (n, channels), 1)
        return jnp.where(lax.rem(row, channels) == col, 1.0, 0.0).astype(f32)

    wide = lax.dot_general(spread(size), c_ref[...], (((1,), (0,)), ((), ())), precision=HI, preferred_element_type=f32)
    wide = lax.dot_general(wide, spread(3 * size), (((1,), (1,)), ((), ())), precision=HI,
                           preferred_element_type=f32) * (COUPLE * scale)
    down = lax.broadcasted_iota(jnp.int32, (size, 3 * size), 0)
    across = lax.broadcasted_iota(jnp.int32, (size, 3 * size), 1)
    high = wide.astype(bf16).astype(f32)
    wide = jnp.where(across < 2 * size, high, wide - high)
    block[...] = jnp.where(down // channels == lax.rem(across, size) // channels, wide, 0.0).astype(bf16)
    down = lax.broadcasted_iota(jnp.int32, (256, 256), 0)
    across = lax.broadcasted_iota(jnp.int32, (256, 256), 1)
    shift = lax.rem(down, 128) - lax.rem(across, 128)
    sums = jnp.where((shift == 1) | (shift == -1), 1.0, 0.0)
    slopes = jnp.where(shift == 1, 8.0, 0.0) + jnp.where(shift == -1, -8.0, 0.0)
    slopes = slopes + jnp.where(shift == 2, -1.0, 0.0) + jnp.where(shift == -2, 1.0, 0.0)
    band[...] = jnp.where(across < 128, sums, slopes).astype(bf16)
    row_pos = (lax.broadcasted_iota(jnp.int32, (rows_all, 128), 0) + (iy * lat - edge)).astype(f32)
    phi = -math.pi / 2 + (row_pos + 0.5) * (math.pi / (lat * ny))
    kxs[...] = (DIFF_LON * scale) / (jnp.cos(phi) ** 2 + 0.1)
    gram_acc[...] = jnp.zeros(gram_acc.shape, f32)

    @pl.when(iy == 0)
    def _():
        near_lat[0] = jnp.zeros(near_lat.shape[1:], f32)
        near_lat_w[0] = jnp.zeros(near_lat_w.shape[1:], f32)
        near_corner[0] = jnp.zeros(near_corner.shape[1:], f32)
        near_corner[1] = jnp.zeros(near_corner.shape[1:], f32)

    @pl.when(iy == ny - 1)
    def _():
        near_lat[1] = jnp.zeros(near_lat.shape[1:], f32)
        near_lat_w[1] = jnp.zeros(near_lat_w.shape[1:], f32)
        near_corner[2] = jnp.zeros(near_corner.shape[1:], f32)
        near_corner[3] = jnp.zeros(near_corner.shape[1:], f32)

    def lat_copies(side, c):
        first = HALF * (1 - c) if side == 0 else HALF * c
        base = lat - HALO if side == 0 else 0
        to = (ix, iy + 1) if side == 0 else (ix, iy - 1)
        if c == 0:
            parts = [(first, HALF, 0, both)]
        elif side == 0:
            parts = [(first + 2, HALF - 2, 0, both), (first, 2, 0, channels)]
        else:
            parts = [(first, HALF - 2, 0, both), (first + HALF - 2, 2, 0, channels)]
        out = []
        for n, (start, count, sub, subs) in enumerate(parts):
            out.append(pltpu.make_async_remote_copy(
                src_ref=own.at[pl.ds(base + start, count), pl.ds(sub, subs), :],
                dst_ref=near_lat.at[side, pl.ds(start, count), pl.ds(sub, subs), :],
                send_sem=lat_send.at[side], recv_sem=lat_recv.at[side, c], device_id=to, device_id_type=MESH))
        out.append(pltpu.make_async_remote_copy(
            src_ref=own_w.at[:, pl.ds(base + first, HALF), :], dst_ref=near_lat_w.at[side, :, pl.ds(first, HALF), :],
            send_sem=lat_send.at[side], recv_sem=lat_recv.at[side, c], device_id=to, device_id_type=MESH))
        return out

    def tile_of(side, c):
        return 1 - c if side == 0 else c

    def corner_copy(side, ew, c):
        slot, tile = 2 * side + ew, tile_of(side, c)
        return pltpu.make_async_remote_copy(
            src_ref=packed.at[ew, tile + (tiles - 2 if side == 0 else 0)], dst_ref=near_corner.at[slot, tile],
            send_sem=lat_send.at[side], recv_sem=lat_recv.at[side, c],
            device_id=(east if ew == 0 else west, iy + 1 if side == 0 else iy - 1), device_id_type=MESH)

    def lon_copy(ew):
        return pltpu.make_async_remote_copy(
            src_ref=packed.at[ew], dst_ref=near_lon.at[ew], send_sem=lon_send.at[ew], recv_sem=lon_recv.at[ew],
            device_id=(east if ew == 0 else west, iy), device_id_type=MESH)

    def has(side):
        return iy < ny - 1 if side == 0 else iy > 0

    def from_side(side):
        return iy > 0 if side == 0 else iy < ny - 1

    lane = lax.broadcasted_iota(jnp.int32, (both, 128), 1)
    lane8 = lax.broadcasted_iota(jnp.int32, (8, 128), 1)

    def turn(x, n):
        n = n % 128
        return pltpu.roll(x, n, 1) if n else x

    def pack(n, _):
        for ew in range(2):
            cut = slice(lon - 128, lon) if ew == 0 else slice(0, 128)
            start = 112 if ew == 0 else 0
            base = HALF * n
            strip = turn(own[base, :, cut], -start)
            for j in range(1, HALF):
                strip = jnp.where((lane >= 16 * j) & (lane < 16 * j + 16), turn(own[base + j, :, cut], 16 * j - start), strip)
            packed[ew, n, 0:both, :] = strip
            rows = pl.ds(pl.multiple_of(base, 8), 8)
            packed[ew, n, both:both + 8, :] = jnp.where(
                lane8 < 16, turn(own_w[0, rows, cut], -start), turn(own_w[1, rows, cut], 16 - start))
        return 0

    def place_coef(e0, wl, wa, inside, chosen):
        kx = kxs[pl.ds(e0, 8), :]
        for t in chosen:
            cut = slice(128 * t, 128 * t + 128)
            l, a = wl[t] * (scale / 12.0), wa[t] * (scale / 12.0)
            planes = [-kx, l, 8.0 * a - DIFF_LAT * scale, -8.0 * a - DIFF_LAT * scale, a]
            for q, plane in enumerate(planes):
                if q == 0 and t != 1:
                    continue
                if inside is not None:
                    plane = plane * inside
                for j in range(8):
                    coef[e0 + j, q:q + 1, cut] = plane[j:j + 1, :]

    def centre(e):
        return (1.0 + 2.0 * DIFF_LAT) * scale - 2.0 * coef[e, 0:1, 128:256]

    def place_own(n, _):
        base = HALF * n
        rows = pl.ds(pl.multiple_of(base, 8), 8)
        wl, wa = ([None, turn(jnp.where(lane8 >= 64, own_w[q, rows, 0:128], own_w[q, rows, 128:256]), 64), None] for q in range(2))
        place_coef(pl.multiple_of(edge + base, 8), wl, wa, None, (1,))
        for j in range(HALF):
            r = base + j
            e = edge + r
            a, b = own[r, :, 0:128], own[r, :, 128:256]
            middle = centre(e)
            for t, piece in enumerate((turn(a, 16), turn(jnp.where(lane >= 64, a, b), 64), turn(b, 112))):
                cut = slice(128 * t, 128 * t + 128)
                even[0, e, :, cut] = piece[0:channels]
                diag[e, :, cut] = piece[channels:] * scale + middle
        return 0

    def place_lon(n, _):
        base = HALF * n
        rows = pl.ds(pl.multiple_of(base, 8), 8)
        w, e = near_lon[0, n, both:both + 8, :], near_lon[1, n, both:both + 8, :]
        wl, wa = ([jnp.where(lane8 < 16, turn(w, -16 * q), turn(own_w[q, rows, 0:128], 16)), None,
                   jnp.where(lane8 >= 112, turn(e, 112 - 16 * q), turn(own_w[q, rows, 128:256], 112))] for q in range(2))
        place_coef(pl.multiple_of(edge + base, 8), wl, wa, None, (0, 2))
        w, e = near_lon[0, n, 0:both, :], near_lon[1, n, 0:both, :]
        for j in range(HALF):
            r = edge + base + j
            middle = centre(r)
            for cut, keep, piece in ((slice(0, 128), lane < 16, turn(w, -16 * j)), (slice(256, 384), lane >= 112, turn(e, 112 - 16 * j))):
                even[0, r, :, cut] = jnp.where(keep[0:channels], piece[0:channels], even[0, r, :, cut])
                diag[r, :, cut] = jnp.where(keep[0:channels], piece[channels:] * scale + middle, diag[r, :, cut])
        return 0

    def place_halo(side, c):
        first = HALF * (1 - c) if side == 0 else HALF * c
        tile = tile_of(side, c)
        e0 = first if side == 0 else edge + lat + first
        inside = jnp.where(from_side(side), 1.0, 0.0).astype(f32)

        @pl.when(from_side(side))
        def _():
            whole = diag.at[pl.ds(0, 13)] if c == 0 else coef.at[pl.ds(0, 35), :, pl.ds(0, 256)]
            pltpu.make_async_copy(whole, whole, lat_recv.at[side, c]).wait()

        def three(a, b, w, e, lanes, at):
            return (jnp.where(lanes < 16, turn(w, -at), turn(a, 16)), turn(jnp.where(lanes >= 64, a, b), 64),
                    jnp.where(lanes >= 112, turn(e, 112 - at), turn(b, 112)))

        west_strip, east_strip = near_corner.at[2 * side, tile], near_corner.at[2 * side + 1, tile]
        span = slice(first, first + 8)
        wl, wa = (three(near_lat_w[side, q, span, 0:128], near_lat_w[side, q, span, 128:256],
                        west_strip[both:both + 8, :], east_strip[both:both + 8, :], lane8, 16 * q) for q in range(2))
        place_coef(e0, wl, wa, inside, range(WINDOWS))
        for j in range(HALF):
            middle = centre(e0 + j)
            pieces = three(near_lat[side, first + j, :, 0:128], near_lat[side, first + j, :, 128:256],
                           west_strip[0:both, :], east_strip[0:both, :], lane, 16 * j)
            for t, piece in enumerate(pieces):
                cut = slice(128 * t, 128 * t + 128)
                even[0, e0 + j, :, cut] = piece[0:channels]
                diag[e0 + j, :, cut] = piece[channels:] * scale + middle

    def advance(level, start, count):
        src, dst, theta = field(level), field(level + 1), THETA[level] * scale
        groups = [[start + GROUP * g + j for j in range(GROUP)] for g in range(count)]
        mixed, moved = [], []
        for picked in groups:
            stack = jnp.concatenate([src[e] for e in picked], axis=0)
            high = stack.astype(bf16)
            low = (stack - high.astype(f32)).astype(bf16)
            mixed.append(lax.dot_general(block[...], jnp.concatenate([high, low, high], axis=0), (((1,), (0,)), ((), ())),
                                         preferred_element_type=f32))
            sides = jnp.concatenate(
                [jnp.concatenate([high[:, 128 * t:128 * t + 128], low[:, 128 * t:128 * t + 128]], axis=1)
                 for t in range(WINDOWS)], axis=0)
            moved.append(lax.dot_general(sides, band[...], (((1,), (0,)), ((), ())), preferred_element_type=f32))
        for g, picked in enumerate(groups):
            for j, e in enumerate(picked):
                for t in range(WINDOWS):
                    cut = slice(128 * t, 128 * t + 128)
                    at = slice(size * t + channels * j, size * t + channels * (j + 1))

                    def weight(q):
                        return coef[e, q:q + 1, cut]

                    value = (diag[e, :, cut] - theta) * src[e, :, cut] + mixed[g][channels * j:channels * (j + 1), cut]
                    value = value + (coef[e, 0:1, 128:256] * moved[g][at, 0:128] + weight(1) * moved[g][at, 128:256])
                    value = value + weight(2) * src[e + 1, :, cut] + weight(3) * src[e - 1, :, cut]
                    dst[e, :, cut] = value + weight(4) * (src[e - 2, :, cut] - src[e + 2, :, cut])

    def interior():
        for k in range(ITERS - 1):
            count = (lat - 4 - 4 * k) // GROUP
            for g in range(0, count, 2):
                advance(k, edge + 2 + 2 * k + GROUP * g, min(2, count - g))

    def wedge(c):
        for k in range(ITERS):
            low = edge - HALF * (c + 1) + 2 + 2 * k
            for e0 in (low, rows_all - HALF - low):
                advance(k, e0, HALF // GROUP)

    def dots(lo, hi, spans):
        pairs = [(k, i) for k, i in PAIRS if lo <= k <= hi]

        def one(t, _):
            cut = pl.ds(pl.multiple_of(t * 128, 128), 128)
            acc = (jnp.zeros((8, 128), f32),) * len(pairs)
            for start, stop in spans:
                def part(n, acc):
                    acc = list(acc)
                    for j in range(4):
                        e = start + 4 * n + j
                        for h in range(channels // 8):
                            x = [field(k)[e, 8 * h:8 * h + 8, cut] for k in range(hi + 1)]
                            for n_, (k, i) in enumerate(pairs):
                                acc[n_] = acc[n_] + x[k] * x[i]
                    return tuple(acc)

                acc = lax.fori_loop(0, (stop - start) // 4, part, acc)
            low = jnp.where(t == 1, 32, 16)
            kept = (lane8 >= low) & (lane8 < 128 - low)
            for n, (k, i) in enumerate(pairs):
                at = k * (k + 1) // 2 + i
                gram_acc[at] = gram_acc[at] + jnp.where(kept, acc[n], 0.0)
            return 0

        lax.fori_loop(0, WINDOWS, one, 0)

    def rim_dots(first, last):
        for t in range(WINDOWS):
            cut = slice(128 * t, 128 * t + 128)
            acc = {}
            for p in range(HALF // 2):
                for e in (edge + 2 * p, edge + 2 * p + 1, edge + lat - 1 - 2 * p, edge + lat - 2 - 2 * p):
                    for h in range(channels // 8):
                        levels = range(first(p), last(p) + 1)
                        if not len(levels):
                            continue
                        x = [field(k)[e, 8 * h:8 * h + 8, cut] for k in range(last(p) + 1)]
                        for k in levels:
                            for i in range(k + 1):
                                term = x[k] * x[i]
                                acc[k, i] = acc[k, i] + term if (k, i) in acc else term
            low = 32 if t == 1 else 16
            kept = (lane8 >= low) & (lane8 < 128 - low)
            for (k, i), value in acc.items():
                at = k * (k + 1) // 2 + i
                gram_acc[at] = gram_acc[at] + jnp.where(kept, value, 0.0)

    pltpu.make_async_copy(own_w, own_w, load_sem.at[1]).wait()
    pltpu.make_async_copy(own, own, load_sem.at[0]).wait()
    lax.fori_loop(0, tiles, pack, 0)
    pl.semaphore_wait(barrier, answers(close))
    tell(0)
    tell(1)

    def send_lat(c):
        for side in range(2):
            @pl.when(has(side))
            def _():
                for copy in lat_copies(side, c):
                    copy.start()

    def send_corners(c):
        for side in range(2):
            @pl.when(has(side))
            def _():
                for ew in range(2):
                    corner_copy(side, ew, c).start()

    send_lat(0)
    for ew in range(2):
        lon_copy(ew).start()
    hear(0)
    send_corners(0)
    send_lat(1)
    send_corners(1)
    lax.fori_loop(0, tiles, place_own, 0)
    hear(1)
    tell(2)
    for ew in range(2):
        lon_copy(ew).wait_recv()
    lax.fori_loop(0, tiles, place_lon, 0)
    interior()
    hear(2)
    tell(3)
    ready = ITERS // 2
    dots(0, ready, ((edge + HALF, edge + lat - HALF),))
    for c in range(2):
        for side in range(2):
            place_halo(side, c)
        wedge(c)
        if c == 0:
            hear(3)
            tell(4)
            dots(0, ready, ((edge, edge + HALF), (edge + lat - HALF, edge + lat)))
            dots(ready + 1, ITERS, ((edge + HALF, edge + lat - HALF),))
            rim_dots(lambda p: ready + 1, lambda p: ready + p)
            hear(4)
            tell(5)
    rim_dots(lambda p: ready + 1 + p, lambda p: ITERS)

    hear(5)
    sums = jnp.concatenate(
        [jnp.sum(gram_acc[n], axis=0, keepdims=True) for n in range(len(PAIRS))]
        + [jnp.zeros((128 - len(PAIRS), 128), f32)], axis=0)
    flat = lax.dot_general(jnp.ones((8, 128), f32), sums, (((1,), (1,)), ((), ())), precision=HI,
                           preferred_element_type=f32)
    mine[...] = flat[0:1, :]
    slots[total - 1] = flat[0:1, :]

    for n, (a, b) in enumerate(peers(nx, ny)):
        pltpu.make_async_remote_copy(
            src_ref=mine, dst_ref=slots.at[n], send_sem=red_sem.at[0], recv_sem=red_sem.at[1],
            device_id=(lax.rem(ix + a, nx), lax.rem(iy + b, ny)), device_id_type=MESH).start()
    arrived = slots.at[pl.ds(0, total - 1)]
    pltpu.make_async_copy(arrived, arrived, red_sem.at[1]).wait()
    pltpu.make_async_copy(arrived, arrived, red_sem.at[0]).wait()
    parts = [slots[n] for n in range(4)]
    for n in range(4, total):
        parts[n % 4] = parts[n % 4] + slots[n]
    whole = (parts[0] + parts[1]) + (parts[2] + parts[3])
    gram = [[None] * (ITERS + 1) for _ in range(ITERS + 1)]
    for n, (k, i) in enumerate(PAIRS):
        gram[k][i] = gram[i][k] = jnp.broadcast_to(whole[:, n:n + 1], (8, 128))
    answer, applied = small_solve(gram)
    for k in range(ITERS):
        splats[k] = answer[k]
    for k in range(ITERS + 1):
        splats[ITERS + k] = applied[k]

    for ew in range(2):
        lon_copy(ew).wait_send()
    for side in range(2):
        @pl.when(has(side))
        def _():
            whole = even.at[0, pl.ds(0, 37), :, pl.ds(0, 256)]
            pltpu.make_async_copy(whole, whole, lat_send.at[side]).wait()


def finish(even, odd, splats, sol_hbm, res_hbm, outs, out_sem):
    channels, lat, _ = sol_hbm.shape
    lane = lax.broadcasted_iota(jnp.int32, (8, 128), 1)
    quarter = lat // 4
    for r in range(lat):
        for h in range(channels // 8):
            sub = slice(8 * h, 8 * h + 8)
            best, rest = [], []
            for t in range(WINDOWS):
                cut = slice(128 * t, 128 * t + 128)
                x = even[0, HALO + r, sub, cut]
                up = splats[0] * x
                down = x - splats[ITERS] * x
                for k in range(1, ITERS + 1):
                    x = (odd if k % 2 else even)[k // 2, HALO + r, sub, cut]
                    if k < ITERS:
                        up = up + splats[k] * x
                    down = down - splats[ITERS + k] * x
                best.append(up)
                rest.append(down)
            for q, (a, b, c) in enumerate((best, rest)):
                b = pltpu.roll(b, 64, 1)
                spread = pl.ds(8 * h * lat + r, 8, stride=lat)
                outs[q, 0, spread, :] = jnp.where(lane < 96, pltpu.roll(a, 112, 1), b)
                outs[q, 1, spread, :] = jnp.where(lane < 32, b, pltpu.roll(c, 16, 1))
        if (r + 1) % quarter == 0:
            rows = pl.ds(r + 1 - quarter, quarter)
            for q, dst in enumerate((sol_hbm, res_hbm)):
                for t in range(2):
                    src = outs.at[q, t].reshape(channels, lat, 128)
                    pltpu.make_async_copy(src.at[:, rows, :], dst.at[:, rows, pl.ds(128 * t, 128)], out_sem.at[q]).start()
    for q, dst in enumerate((sol_hbm, res_hbm)):
        pltpu.make_async_copy(dst, dst, out_sem.at[q]).wait()


def solution(mesh):
    nx, ny = mesh.shape["gx"], mesh.shape["gy"]

    def per_device(forcing, damping, coupling, wind_lon, wind_lat):
        channels, lat, lon = forcing.shape
        f32 = jnp.float32
        vmem = pl.BlockSpec(memory_space=pltpu.VMEM)
        hbm = pl.BlockSpec(memory_space=pltpu.HBM)
        dma = pltpu.SemaphoreType.DMA
        shape = jax.ShapeDtypeStruct((channels, lat, lon), f32)
        rows_all, lanes = lat + 2 * HALO, 128 * WINDOWS
        packed = 2 * channels + 8
        even, odd, splats = pl.pallas_call(
            functools.partial(kernel, nx, ny),
            out_shape=(
                pltpu.VMEM((ITERS // 2 + 1, rows_all, channels, lanes), f32),
                pltpu.VMEM((ITERS // 2, rows_all, channels, lanes), f32),
                pltpu.VMEM((2 * ITERS + 1, 8, 128), f32),
            ),
            in_specs=[hbm, hbm, vmem, hbm, hbm],
            out_specs=(vmem, vmem, vmem),
            scratch_shapes=[
                pltpu.VMEM((rows_all, channels, lanes), f32),
                pltpu.VMEM((rows_all, 8, lanes), f32),
                pltpu.VMEM((rows_all, 128), f32),
                pltpu.VMEM((GROUP * channels, 3 * GROUP * channels), jnp.bfloat16),
                pltpu.VMEM((256, 256), jnp.bfloat16),
                pltpu.VMEM((lat, 2 * channels, lon), f32),
                pltpu.VMEM((2, HALO, 2 * channels, lon), f32),
                pltpu.VMEM((2, lat, lon), f32),
                pltpu.VMEM((2, 2, HALO, lon), f32),
                pltpu.VMEM((2, lat // HALF, packed, 128), f32),
                pltpu.VMEM((2, lat // HALF, packed, 128), f32),
                pltpu.VMEM((4, 2, packed, 128), f32),
                pltpu.VMEM((len(PAIRS), 8, 128), f32),
                pltpu.VMEM((1, 128), f32),
                pltpu.VMEM((nx * ny, 1, 128), f32),
                dma((2,)),
                dma((2,)), dma((2, 2)), dma((2,)), dma((2,)), dma((2,)),
                pltpu.SemaphoreType.REGULAR((6,)),
            ],
            compiler_params=pltpu.CompilerParams(
                collective_id=0, has_side_effects=True, vmem_limit_bytes=52_800_000),
        )(forcing, damping, coupling, wind_lon, wind_lat)
        return pl.pallas_call(
            finish,
            out_shape=(shape, shape),
            in_specs=[vmem, vmem, vmem],
            out_specs=(hbm, hbm),
            scratch_shapes=[pltpu.VMEM((2, 2, channels * lat, 128), f32), dma((2,))],
            compiler_params=pltpu.CompilerParams(vmem_limit_bytes=16 * 1024 * 1024),
        )(even, odd, splats)

    return jax.shard_map(
        per_device,
        mesh=mesh,
        in_specs=(P(None, "gy", "gx"), P(None, "gy", "gx"), P(), P("gy", "gx"), P("gy", "gx")),
        out_specs=(P(None, "gy", "gx"), P(None, "gy", "gx")),
        check_vma=False,
    )
```

```python
import functools
import math

import jax
import jax.numpy as jnp
from jax import lax
from jax.experimental import pallas as pl
from jax.experimental.pallas import tpu as pltpu
from jax.sharding import PartitionSpec as P

ITERS = 8
COUPLE = 0.25
DIFF_LAT = 0.5
DIFF_LON = 0.5
GUARD = 1.0
MESH = pl.DeviceIdType.MESH
HI = lax.Precision.HIGHEST

MIDDLE = 9.0
RADIUS = 6.0
WIDTH = 3.0
THETA = [MIDDLE + RADIUS * math.cos(math.pi * (2 * k + 1) / (2 * ITERS)) for k in (7, 0, 4, 2, 6, 1, 5, 3)]
PAIRS = [(k, i) for k in range(ITERS + 1) for i in range(k + 1)]
GROUP = 4
HALO = 2 * ITERS
HALF = 8
WINDOWS = 3


def apply_to(coords):
    out = [None] * (len(coords) + 1)
    for k, value in enumerate(coords):
        low = THETA[k] * value if k < ITERS else value
        out[k] = low if out[k] is None else out[k] + low
        out[k + 1] = WIDTH * value
    return out


def small_solve(gram):
    first = jnp.sqrt(gram[0][0] + GUARD)
    coords = [[1.0 / first]]
    images = [[gram[i][0] * coords[0][0] for i in range(ITERS + 1)]]
    heights = []
    for j in range(ITERS):
        moved = apply_to(coords[j])
        column = []
        for i in range(j + 1):
            column.append(functools.reduce(lambda a, b: a + b, [images[i][k] * moved[k] for k in range(j + 2)]))
        left = list(moved)
        for i in range(j + 1):
            for k in range(i + 1):
                left[k] = left[k] - column[i] * coords[i][k]
        image = [
            functools.reduce(lambda a, b: a + b, [gram[r][k] * left[k] for k in range(j + 2)])
            for r in range(ITERS + 1)
        ]
        norm_sq = functools.reduce(lambda a, b: a + b, [image[k] * left[k] for k in range(j + 2)])
        subdiag = jnp.sqrt(jnp.maximum(norm_sq, 0.0) + GUARD)
        column.append(subdiag)
        heights.append(column)
        inverse = 1.0 / subdiag
        coords.append([v * inverse for v in left])
        images.append([v * inverse for v in image])
    cosines, sines, target, rotated = [], [], [first], []
    for j in range(ITERS):
        column = list(heights[j])
        for e in range(j):
            upper, lower = column[e], column[e + 1]
            column[e] = cosines[e] * upper + sines[e] * lower
            column[e + 1] = cosines[e] * lower - sines[e] * upper
        upper, lower = column[j], column[j + 1]
        radius = jnp.sqrt(upper * upper + lower * lower)
        inverse = 1.0 / radius
        cosine, sine = upper * inverse, lower * inverse
        column[j] = radius
        kept = target[j]
        target[j] = cosine * kept
        target.append(-sine * kept)
        cosines.append(cosine)
        sines.append(sine)
        rotated.append(column)
    weights = [None] * ITERS
    for j in reversed(range(ITERS)):
        value = target[j]
        for later in range(j + 1, ITERS):
            value = value - rotated[later][j] * weights[later]
        weights[j] = value / rotated[j][j]
    answer = [None] * ITERS
    for j in range(ITERS):
        for k in range(j + 1):
            term = weights[j] * coords[j][k]
            answer[k] = term if answer[k] is None else answer[k] + term
    return answer, apply_to(answer)


def distance(n, o):
    return min(o, n - o)


def peers(nx, ny):
    inner = 4 if ny % 4 == 0 else 1
    offsets = [(a, b) for a in range(nx) for b in range(ny) if (a, b) != (0, 0)]

    def hops(offset):
        a, b = offset
        return distance(nx // 2 or 1, a // 2) + distance(inner, b % inner) + distance(ny // inner, b // inner)

    return sorted(offsets, key=lambda offset: (-hops(offset), offset))


def kernel(nx, ny, f_hbm, d_hbm, c_ref, wl_hbm, wa_hbm, even, odd, splats,
           diag, coef, kxs, block, band, own, near_lat, own_w, near_lat_w, packed, near_lon, near_corner,
           gram_acc, mine, slots,
           load_sem, lat_send, lat_recv, lon_send, lon_recv, red_sem, known):
    channels, lat, lon = f_hbm.shape
    both = 2 * channels
    total = nx * ny
    f32, bf16 = jnp.float32, jnp.bfloat16
    ix, iy = lax.axis_index("gx"), lax.axis_index("gy")
    east, west = lax.rem(ix + 1, nx), lax.rem(ix + nx - 1, nx)
    scale = 1.0 / WIDTH
    size = GROUP * channels
    edge = HALO
    rows_all = lat + 2 * HALO
    tiles = lat // HALF

    def field(k):
        return even.at[k // 2] if k % 2 == 0 else odd.at[k // 2]

    barrier = pltpu.get_barrier_semaphore()

    def greet(sem, a, b):
        def signal():
            pl.semaphore_signal(sem, inc=1, device_id=(lax.rem(ix + a, nx), iy + b), device_id_type=MESH)

        if b == 0:
            signal()
        else:
            pl.when(iy + b < ny if b > 0 else iy + b >= 0)(signal)

    def line(n):
        return [(0, b) for b in range(1, n + 1)] + [(0, -b) for b in range(1, n + 1)]

    def ring(n):
        return [(a, 0) for a in range(1, n + 1)] + [(nx - a, 0) for a in range(1, n + 1)]

    def answers(offsets):
        fixed = sum(1 for _, b in offsets if b == 0)
        reach = max(b for _, b in offsets)
        return fixed + jnp.minimum(ny - 1 - iy, reach) + jnp.minimum(iy, reach)

    close = line(1) + ring(1)
    rounds = [line(1), ring(1), line(2) + ring(2), line(4), line(8), [(a, 0) for a in range(1, nx)]]
    for a, b in close:
        greet(barrier, a, b)

    def tell(n):
        for a, b in rounds[n]:
            greet(known.at[n], a, b)

    def hear(n):
        pl.semaphore_wait(known.at[n], answers(rounds[n]))

    winds = [pltpu.make_async_copy(wl_hbm, own_w.at[0], load_sem.at[1]), pltpu.make_async_copy(wa_hbm, own_w.at[1], load_sem.at[1])]
    for copy in winds:
        copy.start()
    for c in range(channels):
        for q, src in enumerate((f_hbm, d_hbm)):
            pltpu.make_async_copy(src.at[c], own.at[:, q * channels + c, :], load_sem.at[0]).start()

    def spread(n):
        row = lax.broadcasted_iota(jnp.int32, (n, channels), 0)
        col = lax.broadcasted_iota(jnp.int32, (n, channels), 1)
        return jnp.where(lax.rem(row, channels) == col, 1.0, 0.0).astype(f32)

    wide = lax.dot_general(spread(size), c_ref[...], (((1,), (0,)), ((), ())), precision=HI, preferred_element_type=f32)
    wide = lax.dot_general(wide, spread(3 * size), (((1,), (1,)), ((), ())), precision=HI,
                           preferred_element_type=f32) * (COUPLE * scale)
    down = lax.broadcasted_iota(jnp.int32, (size, 3 * size), 0)
    across = lax.broadcasted_iota(jnp.int32, (size, 3 * size), 1)
    high = wide.astype(bf16).astype(f32)
    wide = jnp.where(across < 2 * size, high, wide - high)
    block[...] = jnp.where(down // channels == lax.rem(across, size) // channels, wide, 0.0).astype(bf16)
    down = lax.broadcasted_iota(jnp.int32, (256, 256), 0)
    across = lax.broadcasted_iota(jnp.int32, (256, 256), 1)
    shift = lax.rem(down, 128) - lax.rem(across, 128)
    sums = jnp.where((shift == 1) | (shift == -1), 1.0, 0.0)
    slopes = jnp.where(shift == 1, 8.0, 0.0) + jnp.where(shift == -1, -8.0, 0.0)
    slopes = slopes + jnp.where(shift == 2, -1.0, 0.0) + jnp.where(shift == -2, 1.0, 0.0)
    band[...] = jnp.where(across < 128, sums, slopes).astype(bf16)
    row_pos = (lax.broadcasted_iota(jnp.int32, (rows_all, 128), 0) + (iy * lat - edge)).astype(f32)
    phi = -math.pi / 2 + (row_pos + 0.5) * (math.pi / (lat * ny))
    kxs[...] = (DIFF_LON * scale) / (jnp.cos(phi) ** 2 + 0.1)
    gram_acc[...] = jnp.zeros(gram_acc.shape, f32)

    @pl.when(iy == 0)
    def _():
        near_lat[0] = jnp.zeros(near_lat.shape[1:], f32)
        near_lat_w[0] = jnp.zeros(near_lat_w.shape[1:], f32)
        near_corner[0] = jnp.zeros(near_corner.shape[1:], f32)
        near_corner[1] = jnp.zeros(near_corner.shape[1:], f32)

    @pl.when(iy == ny - 1)
    def _():
        near_lat[1] = jnp.zeros(near_lat.shape[1:], f32)
        near_lat_w[1] = jnp.zeros(near_lat_w.shape[1:], f32)
        near_corner[2] = jnp.zeros(near_corner.shape[1:], f32)
        near_corner[3] = jnp.zeros(near_corner.shape[1:], f32)

    def lat_copies(side, c):
        first = HALF * (1 - c) if side == 0 else HALF * c
        base = lat - HALO if side == 0 else 0
        to = (ix, iy + 1) if side == 0 else (ix, iy - 1)
        if c == 0:
            parts = [(first, HALF, 0, both)]
        elif side == 0:
            parts = [(first + 2, HALF - 2, 0, both), (first, 2, 0, channels)]
        else:
            parts = [(first, HALF - 2, 0, both), (first + HALF - 2, 2, 0, channels)]
        out = []
        for n, (start, count, sub, subs) in enumerate(parts):
            out.append(pltpu.make_async_remote_copy(
                src_ref=own.at[pl.ds(base + start, count), pl.ds(sub, subs), :],
                dst_ref=near_lat.at[side, pl.ds(start, count), pl.ds(sub, subs), :],
                send_sem=lat_send.at[side], recv_sem=lat_recv.at[side, c], device_id=to, device_id_type=MESH))
        out.append(pltpu.make_async_remote_copy(
            src_ref=own_w.at[:, pl.ds(base + first, HALF), :], dst_ref=near_lat_w.at[side, :, pl.ds(first, HALF), :],
            send_sem=lat_send.at[side], recv_sem=lat_recv.at[side, c], device_id=to, device_id_type=MESH))
        return out

    def tile_of(side, c):
        return 1 - c if side == 0 else c

    def corner_copy(side, ew, c):
        slot, tile = 2 * side + ew, tile_of(side, c)
        return pltpu.make_async_remote_copy(
            src_ref=packed.at[ew, tile + (tiles - 2 if side == 0 else 0)], dst_ref=near_corner.at[slot, tile],
            send_sem=lat_send.at[side], recv_sem=lat_recv.at[side, c],
            device_id=(east if ew == 0 else west, iy + 1 if side == 0 else iy - 1), device_id_type=MESH)

    def lon_copy(ew):
        return pltpu.make_async_remote_copy(
            src_ref=packed.at[ew], dst_ref=near_lon.at[ew], send_sem=lon_send.at[ew], recv_sem=lon_recv.at[ew],
            device_id=(east if ew == 0 else west, iy), device_id_type=MESH)

    def has(side):
        return iy < ny - 1 if side == 0 else iy > 0

    def from_side(side):
        return iy > 0 if side == 0 else iy < ny - 1

    lane = lax.broadcasted_iota(jnp.int32, (both, 128), 1)
    lane8 = lax.broadcasted_iota(jnp.int32, (8, 128), 1)

    def turn(x, n):
        n = n % 128
        return pltpu.roll(x, n, 1) if n else x

    def pack(n, _):
        for ew in range(2):
            cut = slice(lon - 128, lon) if ew == 0 else slice(0, 128)
            start = 112 if ew == 0 else 0
            base = HALF * n
            strip = turn(own[base, :, cut], -start)
            for j in range(1, HALF):
                strip = jnp.where((lane >= 16 * j) & (lane < 16 * j + 16), turn(own[base + j, :, cut], 16 * j - start), strip)
            packed[ew, n, 0:both, :] = strip
            rows = pl.ds(pl.multiple_of(base, 8), 8)
            packed[ew, n, both:both + 8, :] = jnp.where(
                lane8 < 16, turn(own_w[0, rows, cut], -start), turn(own_w[1, rows, cut], 16 - start))
        return 0

    def place_coef(e0, wl, wa, inside, chosen):
        kx = kxs[pl.ds(e0, 8), :]
        for t in chosen:
            cut = slice(128 * t, 128 * t + 128)
            l, a = wl[t] * (scale / 12.0), wa[t] * (scale / 12.0)
            planes = [-kx, l, 8.0 * a - DIFF_LAT * scale, -8.0 * a - DIFF_LAT * scale, a]
            for q, plane in enumerate(planes):
                if q == 0 and t != 1:
                    continue
                if inside is not None:
                    plane = plane * inside
                for j in range(8):
                    coef[e0 + j, q:q + 1, cut] = plane[j:j + 1, :]

    def centre(e):
        return (1.0 + 2.0 * DIFF_LAT) * scale - 2.0 * coef[e, 0:1, 128:256]

    def place_own(n, _):
        base = HALF * n
        rows = pl.ds(pl.multiple_of(base, 8), 8)
        wl, wa = ([None, turn(jnp.where(lane8 >= 64, own_w[q, rows, 0:128], own_w[q, rows, 128:256]), 64), None] for q in range(2))
        place_coef(pl.multiple_of(edge + base, 8), wl, wa, None, (1,))
        for j in range(HALF):
            r = base + j
            e = edge + r
            a, b = own[r, :, 0:128], own[r, :, 128:256]
            middle = centre(e)
            for t, piece in enumerate((turn(a, 16), turn(jnp.where(lane >= 64, a, b), 64), turn(b, 112))):
                cut = slice(128 * t, 128 * t + 128)
                even[0, e, :, cut] = piece[0:channels]
                diag[e, :, cut] = piece[channels:] * scale + middle
        return 0

    def place_lon(n, _):
        base = HALF * n
        rows = pl.ds(pl.multiple_of(base, 8), 8)
        w, e = near_lon[0, n, both:both + 8, :], near_lon[1, n, both:both + 8, :]
        wl, wa = ([jnp.where(lane8 < 16, turn(w, -16 * q), turn(own_w[q, rows, 0:128], 16)), None,
                   jnp.where(lane8 >= 112, turn(e, 112 - 16 * q), turn(own_w[q, rows, 128:256], 112))] for q in range(2))
        place_coef(pl.multiple_of(edge + base, 8), wl, wa, None, (0, 2))
        w, e = near_lon[0, n, 0:both, :], near_lon[1, n, 0:both, :]
        for j in range(HALF):
            r = edge + base + j
            middle = centre(r)
            for cut, keep, piece in ((slice(0, 128), lane < 16, turn(w, -16 * j)), (slice(256, 384), lane >= 112, turn(e, 112 - 16 * j))):
                even[0, r, :, cut] = jnp.where(keep[0:channels], piece[0:channels], even[0, r, :, cut])
                diag[r, :, cut] = jnp.where(keep[0:channels], piece[channels:] * scale + middle, diag[r, :, cut])
        return 0

    def place_halo(side, c):
        first = HALF * (1 - c) if side == 0 else HALF * c
        tile = tile_of(side, c)
        e0 = first if side == 0 else edge + lat + first
        inside = jnp.where(from_side(side), 1.0, 0.0).astype(f32)

        @pl.when(from_side(side))
        def _():
            whole = diag.at[pl.ds(0, 13)] if c == 0 else coef.at[pl.ds(0, 35), :, pl.ds(0, 256)]
            pltpu.make_async_copy(whole, whole, lat_recv.at[side, c]).wait()

        def three(a, b, w, e, lanes, at):
            return (jnp.where(lanes < 16, turn(w, -at), turn(a, 16)), turn(jnp.where(lanes >= 64, a, b), 64),
                    jnp.where(lanes >= 112, turn(e, 112 - at), turn(b, 112)))

        west_strip, east_strip = near_corner.at[2 * side, tile], near_corner.at[2 * side + 1, tile]
        span = slice(first, first + 8)
        wl, wa = (three(near_lat_w[side, q, span, 0:128], near_lat_w[side, q, span, 128:256],
                        west_strip[both:both + 8, :], east_strip[both:both + 8, :], lane8, 16 * q) for q in range(2))
        place_coef(e0, wl, wa, inside, range(WINDOWS))
        for j in range(HALF):
            middle = centre(e0 + j)
            pieces = three(near_lat[side, first + j, :, 0:128], near_lat[side, first + j, :, 128:256],
                           west_strip[0:both, :], east_strip[0:both, :], lane, 16 * j)
            for t, piece in enumerate(pieces):
                cut = slice(128 * t, 128 * t + 128)
                even[0, e0 + j, :, cut] = piece[0:channels]
                diag[e0 + j, :, cut] = piece[channels:] * scale + middle

    def advance(level, start, count):
        src, dst, theta = field(level), field(level + 1), THETA[level] * scale
        groups = [[start + GROUP * g + j for j in range(GROUP)] for g in range(count)]
        mixed, moved = [], []
        for picked in groups:
            stack = jnp.concatenate([src[e] for e in picked], axis=0)
            high = stack.astype(bf16)
            low = (stack - high.astype(f32)).astype(bf16)
            mixed.append(lax.dot_general(block[...], jnp.concatenate([high, low, high], axis=0), (((1,), (0,)), ((), ())),
                                         preferred_element_type=f32))
            sides = jnp.concatenate(
                [jnp.concatenate([high[:, 128 * t:128 * t + 128], low[:, 128 * t:128 * t + 128]], axis=1)
                 for t in range(WINDOWS)], axis=0)
            moved.append(lax.dot_general(sides, band[...], (((1,), (0,)), ((), ())), preferred_element_type=f32))
        for g, picked in enumerate(groups):
            for j, e in enumerate(picked):
                for t in range(WINDOWS):
                    cut = slice(128 * t, 128 * t + 128)
                    at = slice(size * t + channels * j, size * t + channels * (j + 1))

                    def weight(q):
                        return coef[e, q:q + 1, cut]

                    value = (diag[e, :, cut] - theta) * src[e, :, cut] + mixed[g][channels * j:channels * (j + 1), cut]
                    value = value + (coef[e, 0:1, 128:256] * moved[g][at, 0:128] + weight(1) * moved[g][at, 128:256])
                    value = value + weight(2) * src[e + 1, :, cut] + weight(3) * src[e - 1, :, cut]
                    dst[e, :, cut] = value + weight(4) * (src[e - 2, :, cut] - src[e + 2, :, cut])

    def interior():
        for k in range(ITERS - 1):
            count = (lat - 4 - 4 * k) // GROUP
            for g in range(0, count, 2):
                advance(k, edge + 2 + 2 * k + GROUP * g, min(2, count - g))

    def wedge(c):
        for k in range(ITERS):
            low = edge - HALF * (c + 1) + 2 + 2 * k
            for e0 in (low, rows_all - HALF - low):
                advance(k, e0, HALF // GROUP)

    def dots(lo, hi, spans):
        pairs = [(k, i) for k, i in PAIRS if lo <= k <= hi]

        def one(t, _):
            cut = pl.ds(pl.multiple_of(t * 128, 128), 128)
            acc = (jnp.zeros((8, 128), f32),) * len(pairs)
            for start, stop in spans:
                def part(n, acc):
                    acc = list(acc)
                    for j in range(4):
                        e = start + 4 * n + j
                        for h in range(channels // 8):
                            x = [field(k)[e, 8 * h:8 * h + 8, cut] for k in range(hi + 1)]
                            for n_, (k, i) in enumerate(pairs):
                                acc[n_] = acc[n_] + x[k] * x[i]
                    return tuple(acc)

                acc = lax.fori_loop(0, (stop - start) // 4, part, acc)
            low = jnp.where(t == 1, 32, 16)
            kept = (lane8 >= low) & (lane8 < 128 - low)
            for n, (k, i) in enumerate(pairs):
                at = k * (k + 1) // 2 + i
                gram_acc[at] = gram_acc[at] + jnp.where(kept, acc[n], 0.0)
            return 0

        lax.fori_loop(0, WINDOWS, one, 0)

    def rim_dots(first, last):
        for t in range(WINDOWS):
            cut = slice(128 * t, 128 * t + 128)
            acc = {}
            for p in range(HALF // 2):
                for e in (edge + 2 * p, edge + 2 * p + 1, edge + lat - 1 - 2 * p, edge + lat - 2 - 2 * p):
                    for h in range(channels // 8):
                        levels = range(first(p), last(p) + 1)
                        if not len(levels):
                            continue
                        x = [field(k)[e, 8 * h:8 * h + 8, cut] for k in range(last(p) + 1)]
                        for k in levels:
                            for i in range(k + 1):
                                term = x[k] * x[i]
                                acc[k, i] = acc[k, i] + term if (k, i) in acc else term
            low = 32 if t == 1 else 16
            kept = (lane8 >= low) & (lane8 < 128 - low)
            for (k, i), value in acc.items():
                at = k * (k + 1) // 2 + i
                gram_acc[at] = gram_acc[at] + jnp.where(kept, value, 0.0)

    pltpu.make_async_copy(own_w, own_w, load_sem.at[1]).wait()
    pltpu.make_async_copy(own, own, load_sem.at[0]).wait()
    lax.fori_loop(0, tiles, pack, 0)
    pl.semaphore_wait(barrier, answers(close))
    tell(0)
    tell(1)

    def send_lat(c):
        for side in range(2):
            @pl.when(has(side))
            def _():
                for copy in lat_copies(side, c):
                    copy.start()

    def send_corners(c):
        for side in range(2):
            @pl.when(has(side))
            def _():
                for ew in range(2):
                    corner_copy(side, ew, c).start()

    send_lat(0)
    for ew in range(2):
        lon_copy(ew).start()
    hear(0)
    send_corners(0)
    send_lat(1)
    send_corners(1)
    lax.fori_loop(0, tiles, place_own, 0)
    hear(1)
    tell(2)
    for ew in range(2):
        lon_copy(ew).wait_recv()
    lax.fori_loop(0, tiles, place_lon, 0)
    interior()
    hear(2)
    tell(3)
    ready = ITERS // 2
    dots(0, ready, ((edge + HALF, edge + lat - HALF),))
    for c in range(2):
        for side in range(2):
            place_halo(side, c)
        if c == 0:
            hear(3)
            tell(4)
        wedge(c)
        if c == 0:
            dots(0, ready, ((edge, edge + HALF), (edge + lat - HALF, edge + lat)))
            dots(ready + 1, ITERS, ((edge + HALF, edge + lat - HALF),))
            rim_dots(lambda p: ready + 1, lambda p: ready + p)
            hear(4)
            tell(5)
    rim_dots(lambda p: ready + 1 + p, lambda p: ITERS)

    hear(5)
    sums = jnp.concatenate(
        [jnp.sum(gram_acc[n], axis=0, keepdims=True) for n in range(len(PAIRS))]
        + [jnp.zeros((128 - len(PAIRS), 128), f32)], axis=0)
    flat = lax.dot_general(jnp.ones((8, 128), f32), sums, (((1,), (1,)), ((), ())), precision=HI,
                           preferred_element_type=f32)
    mine[...] = flat[0:1, :]
    slots[total - 1] = flat[0:1, :]

    for n, (a, b) in enumerate(peers(nx, ny)):
        pltpu.make_async_remote_copy(
            src_ref=mine, dst_ref=slots.at[n], send_sem=red_sem.at[0], recv_sem=red_sem.at[1],
            device_id=(lax.rem(ix + a, nx), lax.rem(iy + b, ny)), device_id_type=MESH).start()
    arrived = slots.at[pl.ds(0, total - 1)]
    pltpu.make_async_copy(arrived, arrived, red_sem.at[1]).wait()
    pltpu.make_async_copy(arrived, arrived, red_sem.at[0]).wait()
    parts = [slots[n] for n in range(4)]
    for n in range(4, total):
        parts[n % 4] = parts[n % 4] + slots[n]
    whole = (parts[0] + parts[1]) + (parts[2] + parts[3])
    gram = [[None] * (ITERS + 1) for _ in range(ITERS + 1)]
    for n, (k, i) in enumerate(PAIRS):
        gram[k][i] = gram[i][k] = jnp.broadcast_to(whole[:, n:n + 1], (8, 128))
    answer, applied = small_solve(gram)
    for k in range(ITERS):
        splats[k] = answer[k]
    for k in range(ITERS + 1):
        splats[ITERS + k] = applied[k]

    for ew in range(2):
        lon_copy(ew).wait_send()
    for side in range(2):
        @pl.when(has(side))
        def _():
            whole = even.at[0, pl.ds(0, 37), :, pl.ds(0, 256)]
            pltpu.make_async_copy(whole, whole, lat_send.at[side]).wait()


def finish(even, odd, splats, sol_hbm, res_hbm, outs, out_sem):
    channels, lat, _ = sol_hbm.shape
    lane = lax.broadcasted_iota(jnp.int32, (8, 128), 1)
    quarter = lat // 4
    for r in range(lat):
        for h in range(channels // 8):
            sub = slice(8 * h, 8 * h + 8)
            best, rest = [], []
            for t in range(WINDOWS):
                cut = slice(128 * t, 128 * t + 128)
                x = even[0, HALO + r, sub, cut]
                up = splats[0] * x
                down = x - splats[ITERS] * x
                for k in range(1, ITERS + 1):
                    x = (odd if k % 2 else even)[k // 2, HALO + r, sub, cut]
                    if k < ITERS:
                        up = up + splats[k] * x
                    down = down - splats[ITERS + k] * x
                best.append(up)
                rest.append(down)
            for q, (a, b, c) in enumerate((best, rest)):
                b = pltpu.roll(b, 64, 1)
                spread = pl.ds(8 * h * lat + r, 8, stride=lat)
                outs[q, 0, spread, :] = jnp.where(lane < 96, pltpu.roll(a, 112, 1), b)
                outs[q, 1, spread, :] = jnp.where(lane < 32, b, pltpu.roll(c, 16, 1))
        if (r + 1) % quarter == 0:
            rows = pl.ds(r + 1 - quarter, quarter)
            for q, dst in enumerate((sol_hbm, res_hbm)):
                for t in range(2):
                    src = outs.at[q, t].reshape(channels, lat, 128)
                    pltpu.make_async_copy(src.at[:, rows, :], dst.at[:, rows, pl.ds(128 * t, 128)], out_sem.at[q]).start()
    for q, dst in enumerate((sol_hbm, res_hbm)):
        pltpu.make_async_copy(dst, dst, out_sem.at[q]).wait()


def solution(mesh):
    nx, ny = mesh.shape["gx"], mesh.shape["gy"]

    def per_device(forcing, damping, coupling, wind_lon, wind_lat):
        channels, lat, lon = forcing.shape
        f32 = jnp.float32
        vmem = pl.BlockSpec(memory_space=pltpu.VMEM)
        hbm = pl.BlockSpec(memory_space=pltpu.HBM)
        dma = pltpu.SemaphoreType.DMA
        shape = jax.ShapeDtypeStruct((channels, lat, lon), f32)
        rows_all, lanes = lat + 2 * HALO, 128 * WINDOWS
        packed = 2 * channels + 8
        even, odd, splats = pl.pallas_call(
            functools.partial(kernel, nx, ny),
            out_shape=(
                pltpu.VMEM((ITERS // 2 + 1, rows_all, channels, lanes), f32),
                pltpu.VMEM((ITERS // 2, rows_all, channels, lanes), f32),
                pltpu.VMEM((2 * ITERS + 1, 8, 128), f32),
            ),
            in_specs=[hbm, hbm, vmem, hbm, hbm],
            out_specs=(vmem, vmem, vmem),
            scratch_shapes=[
                pltpu.VMEM((rows_all, channels, lanes), f32),
                pltpu.VMEM((rows_all, 8, lanes), f32),
                pltpu.VMEM((rows_all, 128), f32),
                pltpu.VMEM((GROUP * channels, 3 * GROUP * channels), jnp.bfloat16),
                pltpu.VMEM((256, 256), jnp.bfloat16),
                pltpu.VMEM((lat, 2 * channels, lon), f32),
                pltpu.VMEM((2, HALO, 2 * channels, lon), f32),
                pltpu.VMEM((2, lat, lon), f32),
                pltpu.VMEM((2, 2, HALO, lon), f32),
                pltpu.VMEM((2, lat // HALF, packed, 128), f32),
                pltpu.VMEM((2, lat // HALF, packed, 128), f32),
                pltpu.VMEM((4, 2, packed, 128), f32),
                pltpu.VMEM((len(PAIRS), 8, 128), f32),
                pltpu.VMEM((1, 128), f32),
                pltpu.VMEM((nx * ny, 1, 128), f32),
                dma((2,)),
                dma((2,)), dma((2, 2)), dma((2,)), dma((2,)), dma((2,)),
                pltpu.SemaphoreType.REGULAR((6,)),
            ],
            compiler_params=pltpu.CompilerParams(
                collective_id=0, has_side_effects=True, vmem_limit_bytes=52_800_000),
        )(forcing, damping, coupling, wind_lon, wind_lat)
        return pl.pallas_call(
            finish,
            out_shape=(shape, shape),
            in_specs=[vmem, vmem, vmem],
            out_specs=(hbm, hbm),
            scratch_shapes=[pltpu.VMEM((2, 2, channels * lat, 128), f32), dma((2,))],
            compiler_params=pltpu.CompilerParams(vmem_limit_bytes=16 * 1024 * 1024),
        )(even, odd, splats)

    return jax.shard_map(
        per_device,
        mesh=mesh,
        in_specs=(P(None, "gy", "gx"), P(None, "gy", "gx"), P(), P("gy", "gx"), P("gy", "gx")),
        out_specs=(P(None, "gy", "gx"), P(None, "gy", "gx")),
        check_vma=False,
    )
```

```python
import functools
import math

import jax
import jax.numpy as jnp
from jax import lax
from jax.experimental import pallas as pl
from jax.experimental.pallas import tpu as pltpu
from jax.sharding import PartitionSpec as P

ITERS = 8
COUPLE = 0.25
DIFF_LAT = 0.5
DIFF_LON = 0.5
GUARD = 1.0
MESH = pl.DeviceIdType.MESH
HI = lax.Precision.HIGHEST

MIDDLE = 9.0
RADIUS = 6.0
WIDTH = 3.0
THETA = [MIDDLE + RADIUS * math.cos(math.pi * (2 * k + 1) / (2 * ITERS)) for k in (7, 0, 4, 2, 6, 1, 5, 3)]
PAIRS = [(k, i) for k in range(ITERS + 1) for i in range(k + 1)]
GROUP = 4
HALO = 2 * ITERS
HALF = 8
STEP = 4
WINDOWS = 3


def apply_to(coords):
    out = [None] * (len(coords) + 1)
    for k, value in enumerate(coords):
        low = THETA[k] * value if k < ITERS else value
        out[k] = low if out[k] is None else out[k] + low
        out[k + 1] = WIDTH * value
    return out


def small_solve(gram):
    first = jnp.sqrt(gram[0][0] + GUARD)
    coords = [[1.0 / first]]
    images = [[gram[i][0] * coords[0][0] for i in range(ITERS + 1)]]
    heights = []
    for j in range(ITERS):
        moved = apply_to(coords[j])
        column = []
        for i in range(j + 1):
            column.append(functools.reduce(lambda a, b: a + b, [images[i][k] * moved[k] for k in range(j + 2)]))
        left = list(moved)
        for i in range(j + 1):
            for k in range(i + 1):
                left[k] = left[k] - column[i] * coords[i][k]
        image = [
            functools.reduce(lambda a, b: a + b, [gram[r][k] * left[k] for k in range(j + 2)])
            for r in range(ITERS + 1)
        ]
        norm_sq = functools.reduce(lambda a, b: a + b, [image[k] * left[k] for k in range(j + 2)])
        subdiag = jnp.sqrt(jnp.maximum(norm_sq, 0.0) + GUARD)
        column.append(subdiag)
        heights.append(column)
        inverse = 1.0 / subdiag
        coords.append([v * inverse for v in left])
        images.append([v * inverse for v in image])
    cosines, sines, target, rotated = [], [], [first], []
    for j in range(ITERS):
        column = list(heights[j])
        for e in range(j):
            upper, lower = column[e], column[e + 1]
            column[e] = cosines[e] * upper + sines[e] * lower
            column[e + 1] = cosines[e] * lower - sines[e] * upper
        upper, lower = column[j], column[j + 1]
        radius = jnp.sqrt(upper * upper + lower * lower)
        inverse = 1.0 / radius
        cosine, sine = upper * inverse, lower * inverse
        column[j] = radius
        kept = target[j]
        target[j] = cosine * kept
        target.append(-sine * kept)
        cosines.append(cosine)
        sines.append(sine)
        rotated.append(column)
    weights = [None] * ITERS
    for j in reversed(range(ITERS)):
        value = target[j]
        for later in range(j + 1, ITERS):
            value = value - rotated[later][j] * weights[later]
        weights[j] = value / rotated[j][j]
    answer = [None] * ITERS
    for j in range(ITERS):
        for k in range(j + 1):
            term = weights[j] * coords[j][k]
            answer[k] = term if answer[k] is None else answer[k] + term
    return answer, apply_to(answer)


def distance(n, o):
    return min(o, n - o)


def peers(nx, ny):
    inner = 4 if ny % 4 == 0 else 1
    offsets = [(a, b) for a in range(nx) for b in range(ny) if (a, b) != (0, 0)]

    def hops(offset):
        a, b = offset
        return distance(nx // 2 or 1, a // 2) + distance(inner, b % inner) + distance(ny // inner, b // inner)

    return sorted(offsets, key=lambda offset: (-hops(offset), offset))


def kernel(nx, ny, f_hbm, d_hbm, c_ref, wl_hbm, wa_hbm, even, odd, splats,
           diag, coef, kxs, block, band, own, near_lat, own_w, near_lat_w, packed, near_lon, near_corner,
           gram_acc, mine, slots,
           load_sem, lat_send, lat_recv, lon_send, lon_recv, red_sem, known):
    channels, lat, lon = f_hbm.shape
    both = 2 * channels
    total = nx * ny
    f32, bf16 = jnp.float32, jnp.bfloat16
    ix, iy = lax.axis_index("gx"), lax.axis_index("gy")
    east, west = lax.rem(ix + 1, nx), lax.rem(ix + nx - 1, nx)
    scale = 1.0 / WIDTH
    size = GROUP * channels
    edge = HALO
    rows_all = lat + 2 * HALO
    tiles = lat // HALF

    def field(k):
        return even.at[k // 2] if k % 2 == 0 else odd.at[k // 2]

    barrier = pltpu.get_barrier_semaphore()

    def greet(sem, a, b):
        def signal():
            pl.semaphore_signal(sem, inc=1, device_id=(lax.rem(ix + a, nx), iy + b), device_id_type=MESH)

        if b == 0:
            signal()
        else:
            pl.when(iy + b < ny if b > 0 else iy + b >= 0)(signal)

    def line(n):
        return [(0, b) for b in range(1, n + 1)] + [(0, -b) for b in range(1, n + 1)]

    def ring(n):
        return [(a, 0) for a in range(1, n + 1)] + [(nx - a, 0) for a in range(1, n + 1)]

    close = line(1) + ring(1)
    rounds = [line(1), ring(1), line(2) + ring(2), [(0, 4), (0, -4)], [(0, 8), (0, -8)], [(a, 0) for a in range(1, nx)]]
    for a, b in close:
        greet(barrier, a, b)

    def tell(n):
        for a, b in rounds[n]:
            greet(known.at[n], a, b)

    def collect(sem, offsets):
        count = sum(1 for _, b in offsets if b == 0)
        for _, b in offsets:
            if b > 0:
                count = count + jnp.minimum(lax.div(ny - 1 - iy, b), 1) + jnp.minimum(lax.div(iy, b), 1)
        pl.semaphore_wait(sem, count)

    def hear(n):
        collect(known.at[n], rounds[n])

    winds = [pltpu.make_async_copy(wl_hbm, own_w.at[0], load_sem.at[1]), pltpu.make_async_copy(wa_hbm, own_w.at[1], load_sem.at[1])]
    for copy in winds:
        copy.start()
    for c in range(channels):
        for q, src in enumerate((f_hbm, d_hbm)):
            pltpu.make_async_copy(src.at[c], own.at[:, q * channels + c, :], load_sem.at[0]).start()

    def spread(n):
        row = lax.broadcasted_iota(jnp.int32, (n, channels), 0)
        col = lax.broadcasted_iota(jnp.int32, (n, channels), 1)
        return jnp.where(lax.rem(row, channels) == col, 1.0, 0.0).astype(f32)

    wide = lax.dot_general(spread(size), c_ref[...], (((1,), (0,)), ((), ())), precision=HI, preferred_element_type=f32)
    wide = lax.dot_general(wide, spread(3 * size), (((1,), (1,)), ((), ())), precision=HI,
                           preferred_element_type=f32) * (COUPLE * scale)
    down = lax.broadcasted_iota(jnp.int32, (size, 3 * size), 0)
    across = lax.broadcasted_iota(jnp.int32, (size, 3 * size), 1)
    high = wide.astype(bf16).astype(f32)
    wide = jnp.where(across < 2 * size, high, wide - high)
    block[...] = jnp.where(down // channels == lax.rem(across, size) // channels, wide, 0.0).astype(bf16)
    down = lax.broadcasted_iota(jnp.int32, (256, 256), 0)
    across = lax.broadcasted_iota(jnp.int32, (256, 256), 1)
    shift = lax.rem(down, 128) - lax.rem(across, 128)
    sums = jnp.where((shift == 1) | (shift == -1), 1.0, 0.0)
    slopes = jnp.where(shift == 1, 8.0, 0.0) + jnp.where(shift == -1, -8.0, 0.0)
    slopes = slopes + jnp.where(shift == 2, -1.0, 0.0) + jnp.where(shift == -2, 1.0, 0.0)
    band[...] = jnp.where(across < 128, sums, slopes).astype(bf16)
    row_pos = (lax.broadcasted_iota(jnp.int32, (rows_all, 128), 0) + (iy * lat - edge)).astype(f32)
    phi = -math.pi / 2 + (row_pos + 0.5) * (math.pi / (lat * ny))
    kxs[...] = (DIFF_LON * scale) / (jnp.cos(phi) ** 2 + 0.1)
    gram_acc[...] = jnp.zeros(gram_acc.shape, f32)

    @pl.when(iy == 0)
    def _():
        near_lat[0] = jnp.zeros(near_lat.shape[1:], f32)
        near_lat_w[0] = jnp.zeros(near_lat_w.shape[1:], f32)
        near_corner[0] = jnp.zeros(near_corner.shape[1:], f32)
        near_corner[1] = jnp.zeros(near_corner.shape[1:], f32)

    @pl.when(iy == ny - 1)
    def _():
        near_lat[1] = jnp.zeros(near_lat.shape[1:], f32)
        near_lat_w[1] = jnp.zeros(near_lat_w.shape[1:], f32)
        near_corner[2] = jnp.zeros(near_corner.shape[1:], f32)
        near_corner[3] = jnp.zeros(near_corner.shape[1:], f32)

    def lat_copies(side, c):
        first = HALO - STEP * (c + 1) if side == 0 else STEP * c
        base = lat - HALO if side == 0 else 0
        to = (ix, iy + 1) if side == 0 else (ix, iy - 1)
        if STEP * (c + 1) < HALO:
            parts = [(first, STEP, both)]
        elif side == 0:
            parts = [(first + 2, STEP - 2, both), (first, 2, channels)]
        else:
            parts = [(first, STEP - 2, both), (first + STEP - 2, 2, channels)]
        out = []
        for start, count, subs in parts:
            out.append(pltpu.make_async_remote_copy(
                src_ref=own.at[pl.ds(base + start, count), pl.ds(0, subs), :],
                dst_ref=near_lat.at[side, pl.ds(start, count), pl.ds(0, subs), :],
                send_sem=lat_send.at[side], recv_sem=lat_recv.at[side, c], device_id=to, device_id_type=MESH))
        if c % 2 == 0:
            tile = tile_of(side, c)
            out.append(pltpu.make_async_remote_copy(
                src_ref=own_w.at[:, pl.ds(base + HALF * tile, HALF), :], dst_ref=near_lat_w.at[side, :, pl.ds(HALF * tile, HALF), :],
                send_sem=lat_send.at[side], recv_sem=lat_recv.at[side, c], device_id=to, device_id_type=MESH))
        return out

    def tile_of(side, c):
        return 1 - c // 2 if side == 0 else c // 2

    def corner_copy(side, ew, c):
        slot, tile = 2 * side + ew, tile_of(side, c)
        return pltpu.make_async_remote_copy(
            src_ref=packed.at[ew, tile + (tiles - 2 if side == 0 else 0)], dst_ref=near_corner.at[slot, tile],
            send_sem=lat_send.at[side], recv_sem=lat_recv.at[side, c],
            device_id=(east if ew == 0 else west, iy + 1 if side == 0 else iy - 1), device_id_type=MESH)

    def lon_copy(ew):
        return pltpu.make_async_remote_copy(
            src_ref=packed.at[ew], dst_ref=near_lon.at[ew], send_sem=lon_send.at[ew], recv_sem=lon_recv.at[ew],
            device_id=(east if ew == 0 else west, iy), device_id_type=MESH)

    def has(side):
        return iy < ny - 1 if side == 0 else iy > 0

    def from_side(side):
        return iy > 0 if side == 0 else iy < ny - 1

    lane = lax.broadcasted_iota(jnp.int32, (both, 128), 1)
    lane8 = lax.broadcasted_iota(jnp.int32, (8, 128), 1)

    def turn(x, n):
        n = n % 128
        return pltpu.roll(x, n, 1) if n else x

    def pack(n, _):
        for ew in range(2):
            cut = slice(lon - 128, lon) if ew == 0 else slice(0, 128)
            start = 112 if ew == 0 else 0
            base = HALF * n
            strip = turn(own[base, :, cut], -start)
            for j in range(1, HALF):
                strip = jnp.where((lane >= 16 * j) & (lane < 16 * j + 16), turn(own[base + j, :, cut], 16 * j - start), strip)
            packed[ew, n, 0:both, :] = strip
            rows = pl.ds(pl.multiple_of(base, 8), 8)
            packed[ew, n, both:both + 8, :] = jnp.where(
                lane8 < 16, turn(own_w[0, rows, cut], -start), turn(own_w[1, rows, cut], 16 - start))
        return 0

    def place_coef(e0, wl, wa, inside, chosen):
        kx = kxs[pl.ds(e0, 8), :]
        for t in chosen:
            cut = slice(128 * t, 128 * t + 128)
            l, a = wl[t] * (scale / 12.0), wa[t] * (scale / 12.0)
            planes = [-kx, l, 8.0 * a - DIFF_LAT * scale, -8.0 * a - DIFF_LAT * scale, a]
            for q, plane in enumerate(planes):
                if q == 0 and t != 1:
                    continue
                if inside is not None:
                    plane = plane * inside
                for j in range(8):
                    coef[e0 + j, q:q + 1, cut] = plane[j:j + 1, :]

    def centre(e):
        return (1.0 + 2.0 * DIFF_LAT) * scale - 2.0 * coef[e, 0:1, 128:256]

    def place_own(n, _):
        base = HALF * n
        rows = pl.ds(pl.multiple_of(base, 8), 8)
        wl, wa = ([None, turn(jnp.where(lane8 >= 64, own_w[q, rows, 0:128], own_w[q, rows, 128:256]), 64), None] for q in range(2))
        place_coef(pl.multiple_of(edge + base, 8), wl, wa, None, (1,))
        for j in range(HALF):
            r = base + j
            e = edge + r
            a, b = own[r, :, 0:128], own[r, :, 128:256]
            middle = centre(e)
            for t, piece in enumerate((turn(a, 16), turn(jnp.where(lane >= 64, a, b), 64), turn(b, 112))):
                cut = slice(128 * t, 128 * t + 128)
                even[0, e, :, cut] = piece[0:channels]
                diag[e, :, cut] = piece[channels:] * scale + middle
        return 0

    def place_lon(n, _):
        base = HALF * n
        rows = pl.ds(pl.multiple_of(base, 8), 8)
        w, e = near_lon[0, n, both:both + 8, :], near_lon[1, n, both:both + 8, :]
        wl, wa = ([jnp.where(lane8 < 16, turn(w, -16 * q), turn(own_w[q, rows, 0:128], 16)), None,
                   jnp.where(lane8 >= 112, turn(e, 112 - 16 * q), turn(own_w[q, rows, 128:256], 112))] for q in range(2))
        place_coef(pl.multiple_of(edge + base, 8), wl, wa, None, (0, 2))
        w, e = near_lon[0, n, 0:both, :], near_lon[1, n, 0:both, :]
        for j in range(HALF):
            r = edge + base + j
            middle = centre(r)
            for cut, keep, piece in ((slice(0, 128), lane < 16, turn(w, -16 * j)), (slice(256, 384), lane >= 112, turn(e, 112 - 16 * j))):
                even[0, r, :, cut] = jnp.where(keep[0:channels], piece[0:channels], even[0, r, :, cut])
                diag[r, :, cut] = jnp.where(keep[0:channels], piece[channels:] * scale + middle, diag[r, :, cut])
        return 0

    def place_halo(side, c):
        first = HALO - STEP * (c + 1) if side == 0 else STEP * c
        tile = tile_of(side, c)
        shift = 0 if side == 0 else edge + lat
        inside = jnp.where(from_side(side), 1.0, 0.0).astype(f32)

        @pl.when(from_side(side))
        def _():
            if c % 2 == 0:
                whole = coef.at[pl.ds(0, 23), :, pl.ds(0, 256)]
            elif STEP * (c + 1) < HALO:
                whole = own.at[pl.ds(0, STEP)]
            else:
                whole = own.at[pl.ds(0, 3)]
            pltpu.make_async_copy(whole, whole, lat_recv.at[side, c]).wait()

        def three(a, b, w, e, lanes, at):
            return (jnp.where(lanes < 16, turn(w, -at), turn(a, 16)), turn(jnp.where(lanes >= 64, a, b), 64),
                    jnp.where(lanes >= 112, turn(e, 112 - at), turn(b, 112)))

        west_strip, east_strip = near_corner.at[2 * side, tile], near_corner.at[2 * side + 1, tile]
        if c % 2 == 0:
            span = slice(HALF * tile, HALF * tile + 8)
            wl, wa = (three(near_lat_w[side, q, span, 0:128], near_lat_w[side, q, span, 128:256],
                            west_strip[both:both + 8, :], east_strip[both:both + 8, :], lane8, 16 * q) for q in range(2))
            place_coef(shift + HALF * tile, wl, wa, inside, range(WINDOWS))
        for j in range(STEP):
            middle = centre(shift + first + j)
            pieces = three(near_lat[side, first + j, :, 0:128], near_lat[side, first + j, :, 128:256],
                           west_strip[0:both, :], east_strip[0:both, :], lane, 16 * ((first + j) % HALF))
            for t, piece in enumerate(pieces):
                cut = slice(128 * t, 128 * t + 128)
                even[0, shift + first + j, :, cut] = piece[0:channels]
                diag[shift + first + j, :, cut] = piece[channels:] * scale + middle

    def advance(level, start, count):
        src, dst, theta = field(level), field(level + 1), THETA[level] * scale
        groups = [[start + GROUP * g + j for j in range(GROUP)] for g in range(count)]
        mixed, moved = [], []
        for picked in groups:
            stack = jnp.concatenate([src[e] for e in picked], axis=0)
            high = stack.astype(bf16)
            low = (stack - high.astype(f32)).astype(bf16)
            mixed.append(lax.dot_general(block[...], jnp.concatenate([high, low, high], axis=0), (((1,), (0,)), ((), ())),
                                         preferred_element_type=f32))
            sides = jnp.concatenate(
                [jnp.concatenate([high[:, 128 * t:128 * t + 128], low[:, 128 * t:128 * t + 128]], axis=1)
                 for t in range(WINDOWS)], axis=0)
            moved.append(lax.dot_general(sides, band[...], (((1,), (0,)), ((), ())), preferred_element_type=f32))
        for g, picked in enumerate(groups):
            for j, e in enumerate(picked):
                at = [slice(size * t + channels * j, size * t + channels * (j + 1)) for t in range(WINDOWS)]
                sums = jnp.concatenate([moved[g][a, 0:128] for a in at], axis=1)
                slopes = jnp.concatenate([moved[g][a, 128:256] for a in at], axis=1)
                kx = jnp.concatenate([coef[e, 0:1, 128:256]] * WINDOWS, axis=1)

                def weight(q):
                    return coef[e, q:q + 1, :]

                value = (diag[e] - theta) * src[e] + mixed[g][channels * j:channels * (j + 1)]
                value = value + (kx * sums + weight(1) * slopes)
                value = value + weight(2) * src[e + 1] + weight(3) * src[e - 1]
                dst[e] = value + weight(4) * (src[e - 2] - src[e + 2])

    def interior():
        for k in range(ITERS - 1):
            count = (lat - 4 - 4 * k) // GROUP
            for g in range(0, count, 2):
                advance(k, edge + 2 + 2 * k + GROUP * g, min(2, count - g))

    def wedge(c):
        for k in range(ITERS):
            low = edge - STEP * (c + 1) + 2 + 2 * k
            for e0 in (low, rows_all - STEP - low):
                advance(k, e0, STEP // GROUP)

    def dots(c):
        for k in range(ITERS + 1):
            last = [p for p in range(lat // 4) if k <= p + 2 * (c + 1) and (c < 0 or k > p + 2 * c)]
            pairs = [e for p in last for e in (edge + 2 * p, edge + lat - 2 - 2 * p)]
            if not pairs:
                continue
            for group, low in (((0, 2), 16), ((1,), 32)):
                acc = [None] * (k + 1)
                for e in pairs:
                    for t in group:
                        x = [field(i)[e:e + 2, :, 128 * t:128 * t + 128] for i in range(k + 1)]
                        for i in range(k + 1):
                            term = x[k] * x[i]
                            acc[i] = term if acc[i] is None else acc[i] + term
                kept = (lane8 >= low) & (lane8 < 128 - low)
                for i in range(k + 1):
                    at = k * (k + 1) // 2 + i
                    value = acc[i][0] + acc[i][1]
                    gram_acc[at] = gram_acc[at] + jnp.where(kept, value[0:8] + value[8:16], 0.0)

    pltpu.make_async_copy(own_w, own_w, load_sem.at[1]).wait()
    pltpu.make_async_copy(own, own, load_sem.at[0]).wait()
    lax.fori_loop(0, tiles, pack, 0)
    collect(barrier, close)
    tell(0)
    tell(1)

    def send_lat(c):
        for side in range(2):
            @pl.when(has(side))
            def _():
                for copy in lat_copies(side, c):
                    copy.start()

    def send_corners(c):
        for side in range(2):
            @pl.when(has(side))
            def _():
                for ew in range(2):
                    corner_copy(side, ew, c).start()

    send_lat(0)
    for ew in range(2):
        lon_copy(ew).start()
    hear(0)
    send_corners(0)
    send_lat(1)
    send_lat(2)
    send_corners(2)
    send_lat(3)
    lax.fori_loop(0, tiles, place_own, 0)
    hear(1)
    tell(2)
    for ew in range(2):
        lon_copy(ew).wait_recv()
    lax.fori_loop(0, tiles, place_lon, 0)
    interior()
    hear(2)
    tell(3)
    dots(-1)
    for c in range(HALO // STEP):
        for side in range(2):
            place_halo(side, c)
        wedge(c)
        dots(c)
        if c == 0:
            hear(3)
            tell(4)
        if c == 2:
            hear(4)
            tell(5)
    hear(5)
    sums = jnp.concatenate(
        [jnp.sum(gram_acc[n], axis=0, keepdims=True) for n in range(len(PAIRS))]
        + [jnp.zeros((128 - len(PAIRS), 128), f32)], axis=0)
    flat = lax.dot_general(jnp.ones((8, 128), f32), sums, (((1,), (1,)), ((), ())), precision=HI,
                           preferred_element_type=f32)
    mine[...] = flat[0:1, :]
    slots[total - 1] = flat[0:1, :]

    for n, (a, b) in enumerate(peers(nx, ny)):
        pltpu.make_async_remote_copy(
            src_ref=mine, dst_ref=slots.at[n], send_sem=red_sem.at[0], recv_sem=red_sem.at[1],
            device_id=(lax.rem(ix + a, nx), lax.rem(iy + b, ny)), device_id_type=MESH).start()
    arrived = slots.at[pl.ds(0, total - 1)]
    pltpu.make_async_copy(arrived, arrived, red_sem.at[1]).wait()
    pltpu.make_async_copy(arrived, arrived, red_sem.at[0]).wait()
    parts = [slots[n] for n in range(4)]
    for n in range(4, total):
        parts[n % 4] = parts[n % 4] + slots[n]
    whole = (parts[0] + parts[1]) + (parts[2] + parts[3])
    gram = [[None] * (ITERS + 1) for _ in range(ITERS + 1)]
    for n, (k, i) in enumerate(PAIRS):
        gram[k][i] = gram[i][k] = jnp.broadcast_to(whole[:, n:n + 1], (8, 128))
    answer, applied = small_solve(gram)
    for k in range(ITERS):
        splats[k] = answer[k]
    for k in range(ITERS + 1):
        splats[ITERS + k] = applied[k]

    for ew in range(2):
        lon_copy(ew).wait_send()
    for side in range(2):
        @pl.when(has(side))
        def _():
            whole = even.at[0, pl.ds(0, 37), :, pl.ds(0, 256)]
            pltpu.make_async_copy(whole, whole, lat_send.at[side]).wait()


def finish(even, odd, splats, sol_hbm, res_hbm, outs, out_sem):
    channels, lat, _ = sol_hbm.shape
    lane = lax.broadcasted_iota(jnp.int32, (8, 128), 1)
    quarter = lat // 4
    for r in range(lat):
        for h in range(channels // 8):
            sub = slice(8 * h, 8 * h + 8)
            best, rest = [], []
            for t in range(WINDOWS):
                cut = slice(128 * t, 128 * t + 128)
                x = even[0, HALO + r, sub, cut]
                up = splats[0] * x
                down = x - splats[ITERS] * x
                for k in range(1, ITERS + 1):
                    x = (odd if k % 2 else even)[k // 2, HALO + r, sub, cut]
                    if k < ITERS:
                        up = up + splats[k] * x
                    down = down - splats[ITERS + k] * x
                best.append(up)
                rest.append(down)
            for q, (a, b, c) in enumerate((best, rest)):
                b = pltpu.roll(b, 64, 1)
                spread = pl.ds(8 * h * lat + r, 8, stride=lat)
                outs[q, 0, spread, :] = jnp.where(lane < 96, pltpu.roll(a, 112, 1), b)
                outs[q, 1, spread, :] = jnp.where(lane < 32, b, pltpu.roll(c, 16, 1))
        if (r + 1) % quarter == 0:
            rows = pl.ds(r + 1 - quarter, quarter)
            for q, dst in enumerate((sol_hbm, res_hbm)):
                for t in range(2):
                    src = outs.at[q, t].reshape(channels, lat, 128)
                    pltpu.make_async_copy(src.at[:, rows, :], dst.at[:, rows, pl.ds(128 * t, 128)], out_sem.at[q]).start()
    for q, dst in enumerate((sol_hbm, res_hbm)):
        pltpu.make_async_copy(dst, dst, out_sem.at[q]).wait()


def solution(mesh):
    nx, ny = mesh.shape["gx"], mesh.shape["gy"]

    def per_device(forcing, damping, coupling, wind_lon, wind_lat):
        channels, lat, lon = forcing.shape
        f32 = jnp.float32
        vmem = pl.BlockSpec(memory_space=pltpu.VMEM)
        hbm = pl.BlockSpec(memory_space=pltpu.HBM)
        dma = pltpu.SemaphoreType.DMA
        shape = jax.ShapeDtypeStruct((channels, lat, lon), f32)
        rows_all, lanes = lat + 2 * HALO, 128 * WINDOWS
        packed = 2 * channels + 8
        even, odd, splats = pl.pallas_call(
            functools.partial(kernel, nx, ny),
            out_shape=(
                pltpu.VMEM((ITERS // 2 + 1, rows_all, channels, lanes), f32),
                pltpu.VMEM((ITERS // 2, rows_all, channels, lanes), f32),
                pltpu.VMEM((2 * ITERS + 1, 8, 128), f32),
            ),
            in_specs=[hbm, hbm, vmem, hbm, hbm],
            out_specs=(vmem, vmem, vmem),
            scratch_shapes=[
                pltpu.VMEM((rows_all, channels, lanes), f32),
                pltpu.VMEM((rows_all, 8, lanes), f32),
                pltpu.VMEM((rows_all, 128), f32),
                pltpu.VMEM((GROUP * channels, 3 * GROUP * channels), jnp.bfloat16),
                pltpu.VMEM((256, 256), jnp.bfloat16),
                pltpu.VMEM((lat, 2 * channels, lon), f32),
                pltpu.VMEM((2, HALO, 2 * channels, lon), f32),
                pltpu.VMEM((2, lat, lon), f32),
                pltpu.VMEM((2, 2, HALO, lon), f32),
                pltpu.VMEM((2, lat // HALF, packed, 128), f32),
                pltpu.VMEM((2, lat // HALF, packed, 128), f32),
                pltpu.VMEM((4, 2, packed, 128), f32),
                pltpu.VMEM((len(PAIRS), 8, 128), f32),
                pltpu.VMEM((1, 128), f32),
                pltpu.VMEM((nx * ny, 1, 128), f32),
                dma((2,)),
                dma((2,)), dma((2, HALO // STEP)), dma((2,)), dma((2,)), dma((2,)),
                pltpu.SemaphoreType.REGULAR((6,)),
            ],
            compiler_params=pltpu.CompilerParams(
                collective_id=0, has_side_effects=True, vmem_limit_bytes=52_800_000),
        )(forcing, damping, coupling, wind_lon, wind_lat)
        return pl.pallas_call(
            finish,
            out_shape=(shape, shape),
            in_specs=[vmem, vmem, vmem],
            out_specs=(hbm, hbm),
            scratch_shapes=[pltpu.VMEM((2, 2, channels * lat, 128), f32), dma((2,))],
            compiler_params=pltpu.CompilerParams(vmem_limit_bytes=16 * 1024 * 1024),
        )(even, odd, splats)

    return jax.shard_map(
        per_device,
        mesh=mesh,
        in_specs=(P(None, "gy", "gx"), P(None, "gy", "gx"), P(), P("gy", "gx"), P("gy", "gx")),
        out_specs=(P(None, "gy", "gx"), P(None, "gy", "gx")),
        check_vma=False,
    )
```

```python
import functools
import math

import jax
import jax.numpy as jnp
from jax import lax
from jax.experimental import pallas as pl
from jax.experimental.pallas import tpu as pltpu
from jax.sharding import PartitionSpec as P

ITERS = 8
COUPLE = 0.25
DIFF_LAT = 0.5
DIFF_LON = 0.5
GUARD = 1.0
MESH = pl.DeviceIdType.MESH
HI = lax.Precision.HIGHEST

MIDDLE = 9.0
RADIUS = 6.0
WIDTH = 3.0
THETA = [MIDDLE + RADIUS * math.cos(math.pi * (2 * k + 1) / (2 * ITERS)) for k in (7, 0, 4, 2, 6, 1, 5, 3)]
PAIRS = [(k, i) for k in range(ITERS + 1) for i in range(k + 1)]
GROUP = 4
HALO = 2 * ITERS
HALF = 8
STEP = 4
WINDOWS = 3


def apply_to(coords):
    out = [None] * (len(coords) + 1)
    for k, value in enumerate(coords):
        low = THETA[k] * value if k < ITERS else value
        out[k] = low if out[k] is None else out[k] + low
        out[k + 1] = WIDTH * value
    return out


def small_solve(gram):
    first = jnp.sqrt(gram[0][0] + GUARD)
    coords = [[1.0 / first]]
    images = [[gram[i][0] * coords[0][0] for i in range(ITERS + 1)]]
    heights = []
    for j in range(ITERS):
        moved = apply_to(coords[j])
        column = []
        for i in range(j + 1):
            column.append(functools.reduce(lambda a, b: a + b, [images[i][k] * moved[k] for k in range(j + 2)]))
        left = list(moved)
        for i in range(j + 1):
            for k in range(i + 1):
                left[k] = left[k] - column[i] * coords[i][k]
        image = [
            functools.reduce(lambda a, b: a + b, [gram[r][k] * left[k] for k in range(j + 2)])
            for r in range(ITERS + 1)
        ]
        norm_sq = functools.reduce(lambda a, b: a + b, [image[k] * left[k] for k in range(j + 2)])
        subdiag = jnp.sqrt(jnp.maximum(norm_sq, 0.0) + GUARD)
        column.append(subdiag)
        heights.append(column)
        inverse = 1.0 / subdiag
        coords.append([v * inverse for v in left])
        images.append([v * inverse for v in image])
    cosines, sines, target, rotated = [], [], [first], []
    for j in range(ITERS):
        column = list(heights[j])
        for e in range(j):
            upper, lower = column[e], column[e + 1]
            column[e] = cosines[e] * upper + sines[e] * lower
            column[e + 1] = cosines[e] * lower - sines[e] * upper
        upper, lower = column[j], column[j + 1]
        radius = jnp.sqrt(upper * upper + lower * lower)
        inverse = 1.0 / radius
        cosine, sine = upper * inverse, lower * inverse
        column[j] = radius
        kept = target[j]
        target[j] = cosine * kept
        target.append(-sine * kept)
        cosines.append(cosine)
        sines.append(sine)
        rotated.append(column)
    weights = [None] * ITERS
    for j in reversed(range(ITERS)):
        value = target[j]
        for later in range(j + 1, ITERS):
            value = value - rotated[later][j] * weights[later]
        weights[j] = value / rotated[j][j]
    answer = [None] * ITERS
    for j in range(ITERS):
        for k in range(j + 1):
            term = weights[j] * coords[j][k]
            answer[k] = term if answer[k] is None else answer[k] + term
    return answer, apply_to(answer)


def distance(n, o):
    return min(o, n - o)


def peers(nx, ny):
    inner = 4 if ny % 4 == 0 else 1
    offsets = [(a, b) for a in range(nx) for b in range(ny) if (a, b) != (0, 0)]

    def hops(offset):
        a, b = offset
        return distance(nx // 2 or 1, a // 2) + distance(inner, b % inner) + distance(ny // inner, b // inner)

    return sorted(offsets, key=lambda offset: (-hops(offset), offset))


def kernel(nx, ny, f_hbm, d_hbm, c_ref, wl_hbm, wa_hbm, even, odd, splats,
           diag, coef, kxs, block, band, own, near_lat, own_w, near_lat_w, packed, near_lon, near_corner,
           gram_acc, mine, slots,
           load_sem, lat_send, lat_recv, lon_send, lon_recv, red_sem, known):
    channels, lat, lon = f_hbm.shape
    both = 2 * channels
    total = nx * ny
    f32, bf16 = jnp.float32, jnp.bfloat16
    ix, iy = lax.axis_index("gx"), lax.axis_index("gy")
    east, west = lax.rem(ix + 1, nx), lax.rem(ix + nx - 1, nx)
    scale = 1.0 / WIDTH
    size = GROUP * channels
    edge = HALO
    rows_all = lat + 2 * HALO
    tiles = lat // HALF

    def field(k):
        return even.at[k // 2] if k % 2 == 0 else odd.at[k // 2]

    barrier = pltpu.get_barrier_semaphore()

    def greet(sem, a, b):
        def signal():
            pl.semaphore_signal(sem, inc=1, device_id=(lax.rem(ix + a, nx), iy + b), device_id_type=MESH)

        if b == 0:
            signal()
        else:
            pl.when(iy + b < ny if b > 0 else iy + b >= 0)(signal)

    def line(n):
        return [(0, b) for b in range(1, n + 1)] + [(0, -b) for b in range(1, n + 1)]

    def ring(n):
        return [(a, 0) for a in range(1, n + 1)] + [(nx - a, 0) for a in range(1, n + 1)]

    close = line(1) + ring(1)
    rounds = [line(1), ring(1), line(2) + ring(2), [(0, 4), (0, -4)], [(0, 8), (0, -8)], [(a, 0) for a in range(1, nx)]]
    for a, b in close:
        greet(barrier, a, b)

    def tell(n):
        for a, b in rounds[n]:
            greet(known.at[n], a, b)

    def collect(sem, offsets):
        count = sum(1 for _, b in offsets if b == 0)
        for _, b in offsets:
            if b > 0:
                count = count + jnp.minimum(lax.div(ny - 1 - iy, b), 1) + jnp.minimum(lax.div(iy, b), 1)
        pl.semaphore_wait(sem, count)

    def hear(n):
        collect(known.at[n], rounds[n])

    winds = [pltpu.make_async_copy(wl_hbm, own_w.at[0], load_sem.at[1]), pltpu.make_async_copy(wa_hbm, own_w.at[1], load_sem.at[1])]
    for copy in winds:
        copy.start()
    for c in range(channels):
        for q, src in enumerate((f_hbm, d_hbm)):
            pltpu.make_async_copy(src.at[c], own.at[:, q * channels + c, :], load_sem.at[0]).start()

    def set_up():
        def spread(n):
            row = lax.broadcasted_iota(jnp.int32, (n, channels), 0)
            col = lax.broadcasted_iota(jnp.int32, (n, channels), 1)
            return jnp.where(lax.rem(row, channels) == col, 1.0, 0.0).astype(f32)

        wide = lax.dot_general(spread(size), c_ref[...], (((1,), (0,)), ((), ())), precision=HI, preferred_element_type=f32)
        wide = lax.dot_general(wide, spread(3 * size), (((1,), (1,)), ((), ())), precision=HI,
                               preferred_element_type=f32) * (COUPLE * scale)
        down = lax.broadcasted_iota(jnp.int32, (size, 3 * size), 0)
        across = lax.broadcasted_iota(jnp.int32, (size, 3 * size), 1)
        high = wide.astype(bf16).astype(f32)
        wide = jnp.where(across < 2 * size, high, wide - high)
        block[...] = jnp.where(down // channels == lax.rem(across, size) // channels, wide, 0.0).astype(bf16)
        down = lax.broadcasted_iota(jnp.int32, (256, 256), 0)
        across = lax.broadcasted_iota(jnp.int32, (256, 256), 1)
        shift = lax.rem(down, 128) - lax.rem(across, 128)
        sums = jnp.where((shift == 1) | (shift == -1), 1.0, 0.0)
        slopes = jnp.where(shift == 1, 8.0, 0.0) + jnp.where(shift == -1, -8.0, 0.0)
        slopes = slopes + jnp.where(shift == 2, -1.0, 0.0) + jnp.where(shift == -2, 1.0, 0.0)
        band[...] = jnp.where(across < 128, sums, slopes).astype(bf16)
        row_pos = (lax.broadcasted_iota(jnp.int32, (rows_all, 128), 0) + (iy * lat - edge)).astype(f32)
        phi = -math.pi / 2 + (row_pos + 0.5) * (math.pi / (lat * ny))
        kxs[...] = (DIFF_LON * scale) / (jnp.cos(phi) ** 2 + 0.1)
        gram_acc[...] = jnp.zeros(gram_acc.shape, f32)

        @pl.when(iy == 0)
        def _():
            near_lat[0] = jnp.zeros(near_lat.shape[1:], f32)
            near_lat_w[0] = jnp.zeros(near_lat_w.shape[1:], f32)
            near_corner[0] = jnp.zeros(near_corner.shape[1:], f32)
            near_corner[1] = jnp.zeros(near_corner.shape[1:], f32)

        @pl.when(iy == ny - 1)
        def _():
            near_lat[1] = jnp.zeros(near_lat.shape[1:], f32)
            near_lat_w[1] = jnp.zeros(near_lat_w.shape[1:], f32)
            near_corner[2] = jnp.zeros(near_corner.shape[1:], f32)
            near_corner[3] = jnp.zeros(near_corner.shape[1:], f32)

    def lat_copies(side, c):
        first = HALO - STEP * (c + 1) if side == 0 else STEP * c
        base = lat - HALO if side == 0 else 0
        to = (ix, iy + 1) if side == 0 else (ix, iy - 1)
        if STEP * (c + 1) < HALO:
            parts = [(first, STEP, both)]
        elif side == 0:
            parts = [(first + 2, STEP - 2, both), (first, 2, channels)]
        else:
            parts = [(first, STEP - 2, both), (first + STEP - 2, 2, channels)]
        out = []
        for start, count, subs in parts:
            out.append(pltpu.make_async_remote_copy(
                src_ref=own.at[pl.ds(base + start, count), pl.ds(0, subs), :],
                dst_ref=near_lat.at[side, pl.ds(start, count), pl.ds(0, subs), :],
                send_sem=lat_send.at[side], recv_sem=lat_recv.at[side, c], device_id=to, device_id_type=MESH))
        if c % 2 == 0:
            tile = tile_of(side, c)
            out.append(pltpu.make_async_remote_copy(
                src_ref=own_w.at[:, pl.ds(base + HALF * tile, HALF), :], dst_ref=near_lat_w.at[side, :, pl.ds(HALF * tile, HALF), :],
                send_sem=lat_send.at[side], recv_sem=lat_recv.at[side, c], device_id=to, device_id_type=MESH))
        return out

    def tile_of(side, c):
        return 1 - c // 2 if side == 0 else c // 2

    def corner_copy(side, ew, c):
        slot, tile = 2 * side + ew, tile_of(side, c)
        return pltpu.make_async_remote_copy(
            src_ref=packed.at[ew, tile + (tiles - 2 if side == 0 else 0)], dst_ref=near_corner.at[slot, tile],
            send_sem=lat_send.at[side], recv_sem=lat_recv.at[side, c],
            device_id=(east if ew == 0 else west, iy + 1 if side == 0 else iy - 1), device_id_type=MESH)

    def lon_copy(ew):
        return pltpu.make_async_remote_copy(
            src_ref=packed.at[ew], dst_ref=near_lon.at[ew], send_sem=lon_send.at[ew], recv_sem=lon_recv.at[ew],
            device_id=(east if ew == 0 else west, iy), device_id_type=MESH)

    def has(side):
        return iy < ny - 1 if side == 0 else iy > 0

    def from_side(side):
        return iy > 0 if side == 0 else iy < ny - 1

    lane = lax.broadcasted_iota(jnp.int32, (both, 128), 1)
    lane8 = lax.broadcasted_iota(jnp.int32, (8, 128), 1)

    def turn(x, n):
        n = n % 128
        return pltpu.roll(x, n, 1) if n else x

    def pack(n, _):
        for ew in range(2):
            cut = slice(lon - 128, lon) if ew == 0 else slice(0, 128)
            start = 112 if ew == 0 else 0
            base = HALF * n
            strip = turn(own[base, :, cut], -start)
            for j in range(1, HALF):
                strip = jnp.where((lane >= 16 * j) & (lane < 16 * j + 16), turn(own[base + j, :, cut], 16 * j - start), strip)
            packed[ew, n, 0:both, :] = strip
            rows = pl.ds(pl.multiple_of(base, 8), 8)
            packed[ew, n, both:both + 8, :] = jnp.where(
                lane8 < 16, turn(own_w[0, rows, cut], -start), turn(own_w[1, rows, cut], 16 - start))
        return 0

    def place_coef(e0, wl, wa, inside, chosen):
        kx = kxs[pl.ds(e0, 8), :]
        for t in chosen:
            cut = slice(128 * t, 128 * t + 128)
            l, a = wl[t] * (scale / 12.0), wa[t] * (scale / 12.0)
            planes = [-kx, l, 8.0 * a - DIFF_LAT * scale, -8.0 * a - DIFF_LAT * scale, a]
            for q, plane in enumerate(planes):
                if q == 0 and t != 1:
                    continue
                if inside is not None:
                    plane = plane * inside
                for j in range(8):
                    coef[e0 + j, q:q + 1, cut] = plane[j:j + 1, :]

    def centre(e):
        return (1.0 + 2.0 * DIFF_LAT) * scale - 2.0 * coef[e, 0:1, 128:256]

    def place_own(n, _):
        base = HALF * n
        rows = pl.ds(pl.multiple_of(base, 8), 8)
        wl, wa = ([None, turn(jnp.where(lane8 >= 64, own_w[q, rows, 0:128], own_w[q, rows, 128:256]), 64), None] for q in range(2))
        place_coef(pl.multiple_of(edge + base, 8), wl, wa, None, (1,))
        for j in range(HALF):
            r = base + j
            e = edge + r
            a, b = own[r, :, 0:128], own[r, :, 128:256]
            middle = centre(e)
            for t, piece in enumerate((turn(a, 16), turn(jnp.where(lane >= 64, a, b), 64), turn(b, 112))):
                cut = slice(128 * t, 128 * t + 128)
                even[0, e, :, cut] = piece[0:channels]
                diag[e, :, cut] = piece[channels:] * scale + middle
        return 0

    def place_lon(n, _):
        base = HALF * n
        rows = pl.ds(pl.multiple_of(base, 8), 8)
        w, e = near_lon[0, n, both:both + 8, :], near_lon[1, n, both:both + 8, :]
        wl, wa = ([jnp.where(lane8 < 16, turn(w, -16 * q), turn(own_w[q, rows, 0:128], 16)), None,
                   jnp.where(lane8 >= 112, turn(e, 112 - 16 * q), turn(own_w[q, rows, 128:256], 112))] for q in range(2))
        place_coef(pl.multiple_of(edge + base, 8), wl, wa, None, (0, 2))
        w, e = near_lon[0, n, 0:both, :], near_lon[1, n, 0:both, :]
        for j in range(HALF):
            r = edge + base + j
            middle = centre(r)
            for cut, keep, piece in ((slice(0, 128), lane < 16, turn(w, -16 * j)), (slice(256, 384), lane >= 112, turn(e, 112 - 16 * j))):
                even[0, r, :, cut] = jnp.where(keep[0:channels], piece[0:channels], even[0, r, :, cut])
                diag[r, :, cut] = jnp.where(keep[0:channels], piece[channels:] * scale + middle, diag[r, :, cut])
        return 0

    def place_halo(side, c):
        first = HALO - STEP * (c + 1) if side == 0 else STEP * c
        tile = tile_of(side, c)
        shift = 0 if side == 0 else edge + lat
        inside = jnp.where(from_side(side), 1.0, 0.0).astype(f32)

        @pl.when(from_side(side))
        def _():
            if c % 2 == 0:
                whole = coef.at[pl.ds(0, 23), :, pl.ds(0, 256)]
            elif STEP * (c + 1) < HALO:
                whole = own.at[pl.ds(0, STEP)]
            else:
                whole = own.at[pl.ds(0, 3)]
            pltpu.make_async_copy(whole, whole, lat_recv.at[side, c]).wait()

        def three(a, b, w, e, lanes, at):
            return (jnp.where(lanes < 16, turn(w, -at), turn(a, 16)), turn(jnp.where(lanes >= 64, a, b), 64),
                    jnp.where(lanes >= 112, turn(e, 112 - at), turn(b, 112)))

        west_strip, east_strip = near_corner.at[2 * side, tile], near_corner.at[2 * side + 1, tile]
        if c % 2 == 0:
            span = slice(HALF * tile, HALF * tile + 8)
            wl, wa = (three(near_lat_w[side, q, span, 0:128], near_lat_w[side, q, span, 128:256],
                            west_strip[both:both + 8, :], east_strip[both:both + 8, :], lane8, 16 * q) for q in range(2))
            place_coef(shift + HALF * tile, wl, wa, inside, range(WINDOWS))
        for j in range(STEP):
            middle = centre(shift + first + j)
            pieces = three(near_lat[side, first + j, :, 0:128], near_lat[side, first + j, :, 128:256],
                           west_strip[0:both, :], east_strip[0:both, :], lane, 16 * ((first + j) % HALF))
            for t, piece in enumerate(pieces):
                cut = slice(128 * t, 128 * t + 128)
                even[0, shift + first + j, :, cut] = piece[0:channels]
                diag[shift + first + j, :, cut] = piece[channels:] * scale + middle

    def advance(level, start, count):
        src, dst, theta = field(level), field(level + 1), THETA[level] * scale
        groups = [[start + GROUP * g + j for j in range(GROUP)] for g in range(count)]
        mixed, moved = [], []
        for picked in groups:
            stack = jnp.concatenate([src[e] for e in picked], axis=0)
            high = stack.astype(bf16)
            low = (stack - high.astype(f32)).astype(bf16)
            mixed.append(lax.dot_general(block[...], jnp.concatenate([high, low, high], axis=0), (((1,), (0,)), ((), ())),
                                         preferred_element_type=f32))
            sides = jnp.concatenate(
                [jnp.concatenate([high[:, 128 * t:128 * t + 128], low[:, 128 * t:128 * t + 128]], axis=1)
                 for t in range(WINDOWS)], axis=0)
            moved.append(lax.dot_general(sides, band[...], (((1,), (0,)), ((), ())), preferred_element_type=f32))
        for g, picked in enumerate(groups):
            for j, e in enumerate(picked):
                at = [slice(size * t + channels * j, size * t + channels * (j + 1)) for t in range(WINDOWS)]
                sums = jnp.concatenate([moved[g][a, 0:128] for a in at], axis=1)
                slopes = jnp.concatenate([moved[g][a, 128:256] for a in at], axis=1)
                kx = jnp.concatenate([coef[e, 0:1, 128:256]] * WINDOWS, axis=1)

                def weight(q):
                    return coef[e, q:q + 1, :]

                value = (diag[e] - theta) * src[e] + mixed[g][channels * j:channels * (j + 1)]
                value = value + (kx * sums + weight(1) * slopes)
                value = value + weight(2) * src[e + 1] + weight(3) * src[e - 1]
                dst[e] = value + weight(4) * (src[e - 2] - src[e + 2])

    def interior():
        for k in range(ITERS - 1):
            count = (lat - 4 - 4 * k) // GROUP
            for g in range(0, count, 2):
                advance(k, edge + 2 + 2 * k + GROUP * g, min(2, count - g))

    def wedge(c):
        for k in range(ITERS):
            low = edge - STEP * (c + 1) + 2 + 2 * k
            for e0 in (low, rows_all - STEP - low):
                advance(k, e0, STEP // GROUP)

    def dots(c):
        for k in range(ITERS + 1):
            last = [p for p in range(lat // 4) if k <= p + 2 * (c + 1) and (c < 0 or k > p + 2 * c)]
            pairs = [e for p in last for e in (edge + 2 * p, edge + lat - 2 - 2 * p)]
            if not pairs:
                continue
            for group, low in (((0, 2), 16), ((1,), 32)):
                acc = [None] * (k + 1)
                for e in pairs:
                    for t in group:
                        x = [field(i)[e:e + 2, :, 128 * t:128 * t + 128] for i in range(k + 1)]
                        for i in range(k + 1):
                            term = x[k] * x[i]
                            acc[i] = term if acc[i] is None else acc[i] + term
                kept = (lane8 >= low) & (lane8 < 128 - low)
                for i in range(k + 1):
                    at = k * (k + 1) // 2 + i
                    value = acc[i][0] + acc[i][1]
                    gram_acc[at] = gram_acc[at] + jnp.where(kept, value[0:8] + value[8:16], 0.0)

    pltpu.make_async_copy(own_w, own_w, load_sem.at[1]).wait()
    pltpu.make_async_copy(own, own, load_sem.at[0]).wait()
    collect(barrier, close)
    tell(0)
    tell(1)

    def send_lat(c):
        for side in range(2):
            @pl.when(has(side))
            def _():
                for copy in lat_copies(side, c):
                    copy.start()

    def send_corners(c):
        for side in range(2):
            @pl.when(has(side))
            def _():
                for ew in range(2):
                    corner_copy(side, ew, c).start()

    send_lat(0)
    lax.fori_loop(0, tiles, pack, 0)
    for ew in range(2):
        lon_copy(ew).start()
    set_up()
    hear(0)
    send_corners(0)
    send_lat(1)
    send_lat(2)
    send_corners(2)
    send_lat(3)
    lax.fori_loop(0, tiles, place_own, 0)
    hear(1)
    tell(2)
    for ew in range(2):
        lon_copy(ew).wait_recv()
    lax.fori_loop(0, tiles, place_lon, 0)
    interior()
    hear(2)
    tell(3)
    dots(-1)
    for c in range(HALO // STEP):
        for side in range(2):
            place_halo(side, c)
        wedge(c)
        dots(c)
        if c == 0:
            hear(3)
            tell(4)
        if c == 2:
            hear(4)
            tell(5)
    hear(5)
    sums = jnp.concatenate(
        [jnp.sum(gram_acc[n], axis=0, keepdims=True) for n in range(len(PAIRS))]
        + [jnp.zeros((128 - len(PAIRS), 128), f32)], axis=0)
    flat = lax.dot_general(jnp.ones((8, 128), f32), sums, (((1,), (1,)), ((), ())), precision=HI,
                           preferred_element_type=f32)
    mine[...] = flat[0:1, :]
    slots[total - 1] = flat[0:1, :]

    for n, (a, b) in enumerate(peers(nx, ny)):
        pltpu.make_async_remote_copy(
            src_ref=mine, dst_ref=slots.at[n], send_sem=red_sem.at[0], recv_sem=red_sem.at[1],
            device_id=(lax.rem(ix + a, nx), lax.rem(iy + b, ny)), device_id_type=MESH).start()
    arrived = slots.at[pl.ds(0, total - 1)]
    pltpu.make_async_copy(arrived, arrived, red_sem.at[1]).wait()
    pltpu.make_async_copy(arrived, arrived, red_sem.at[0]).wait()
    parts = [slots[n] for n in range(4)]
    for n in range(4, total):
        parts[n % 4] = parts[n % 4] + slots[n]
    whole = (parts[0] + parts[1]) + (parts[2] + parts[3])
    gram = [[None] * (ITERS + 1) for _ in range(ITERS + 1)]
    for n, (k, i) in enumerate(PAIRS):
        gram[k][i] = gram[i][k] = jnp.broadcast_to(whole[:, n:n + 1], (8, 128))
    answer, applied = small_solve(gram)
    for k in range(ITERS):
        splats[k] = answer[k]
    for k in range(ITERS + 1):
        splats[ITERS + k] = applied[k]

    for ew in range(2):
        lon_copy(ew).wait_send()
    for side in range(2):
        @pl.when(has(side))
        def _():
            whole = even.at[0, pl.ds(0, 37), :, pl.ds(0, 256)]
            pltpu.make_async_copy(whole, whole, lat_send.at[side]).wait()


def finish(even, odd, splats, sol_hbm, res_hbm, outs, out_sem):
    channels, lat, _ = sol_hbm.shape
    lane = lax.broadcasted_iota(jnp.int32, (8, 128), 1)
    quarter = lat // 4
    for r in range(lat):
        for h in range(channels // 8):
            sub = slice(8 * h, 8 * h + 8)
            best, rest = [], []
            for t in range(WINDOWS):
                cut = slice(128 * t, 128 * t + 128)
                x = even[0, HALO + r, sub, cut]
                up = splats[0] * x
                down = x - splats[ITERS] * x
                for k in range(1, ITERS + 1):
                    x = (odd if k % 2 else even)[k // 2, HALO + r, sub, cut]
                    if k < ITERS:
                        up = up + splats[k] * x
                    down = down - splats[ITERS + k] * x
                best.append(up)
                rest.append(down)
            for q, (a, b, c) in enumerate((best, rest)):
                b = pltpu.roll(b, 64, 1)
                spread = pl.ds(8 * h * lat + r, 8, stride=lat)
                outs[q, 0, spread, :] = jnp.where(lane < 96, pltpu.roll(a, 112, 1), b)
                outs[q, 1, spread, :] = jnp.where(lane < 32, b, pltpu.roll(c, 16, 1))
        if (r + 1) % quarter == 0:
            rows = pl.ds(r + 1 - quarter, quarter)
            for q, dst in enumerate((sol_hbm, res_hbm)):
                for t in range(2):
                    src = outs.at[q, t].reshape(channels, lat, 128)
                    pltpu.make_async_copy(src.at[:, rows, :], dst.at[:, rows, pl.ds(128 * t, 128)], out_sem.at[q]).start()
    for q, dst in enumerate((sol_hbm, res_hbm)):
        pltpu.make_async_copy(dst, dst, out_sem.at[q]).wait()


def solution(mesh):
    nx, ny = mesh.shape["gx"], mesh.shape["gy"]

    def per_device(forcing, damping, coupling, wind_lon, wind_lat):
        channels, lat, lon = forcing.shape
        f32 = jnp.float32
        vmem = pl.BlockSpec(memory_space=pltpu.VMEM)
        hbm = pl.BlockSpec(memory_space=pltpu.HBM)
        dma = pltpu.SemaphoreType.DMA
        shape = jax.ShapeDtypeStruct((channels, lat, lon), f32)
        rows_all, lanes = lat + 2 * HALO, 128 * WINDOWS
        packed = 2 * channels + 8
        even, odd, splats = pl.pallas_call(
            functools.partial(kernel, nx, ny),
            out_shape=(
                pltpu.VMEM((ITERS // 2 + 1, rows_all, channels, lanes), f32),
                pltpu.VMEM((ITERS // 2, rows_all, channels, lanes), f32),
                pltpu.VMEM((2 * ITERS + 1, 8, 128), f32),
            ),
            in_specs=[hbm, hbm, vmem, hbm, hbm],
            out_specs=(vmem, vmem, vmem),
            scratch_shapes=[
                pltpu.VMEM((rows_all, channels, lanes), f32),
                pltpu.VMEM((rows_all, 8, lanes), f32),
                pltpu.VMEM((rows_all, 128), f32),
                pltpu.VMEM((GROUP * channels, 3 * GROUP * channels), jnp.bfloat16),
                pltpu.VMEM((256, 256), jnp.bfloat16),
                pltpu.VMEM((lat, 2 * channels, lon), f32),
                pltpu.VMEM((2, HALO, 2 * channels, lon), f32),
                pltpu.VMEM((2, lat, lon), f32),
                pltpu.VMEM((2, 2, HALO, lon), f32),
                pltpu.VMEM((2, lat // HALF, packed, 128), f32),
                pltpu.VMEM((2, lat // HALF, packed, 128), f32),
                pltpu.VMEM((4, 2, packed, 128), f32),
                pltpu.VMEM((len(PAIRS), 8, 128), f32),
                pltpu.VMEM((1, 128), f32),
                pltpu.VMEM((nx * ny, 1, 128), f32),
                dma((2,)),
                dma((2,)), dma((2, HALO // STEP)), dma((2,)), dma((2,)), dma((2,)),
                pltpu.SemaphoreType.REGULAR((6,)),
            ],
            compiler_params=pltpu.CompilerParams(
                collective_id=0, has_side_effects=True, vmem_limit_bytes=52_800_000),
        )(forcing, damping, coupling, wind_lon, wind_lat)
        return pl.pallas_call(
            finish,
            out_shape=(shape, shape),
            in_specs=[vmem, vmem, vmem],
            out_specs=(hbm, hbm),
            scratch_shapes=[pltpu.VMEM((2, 2, channels * lat, 128), f32), dma((2,))],
            compiler_params=pltpu.CompilerParams(vmem_limit_bytes=16 * 1024 * 1024),
        )(even, odd, splats)

    return jax.shard_map(
        per_device,
        mesh=mesh,
        in_specs=(P(None, "gy", "gx"), P(None, "gy", "gx"), P(), P("gy", "gx"), P("gy", "gx")),
        out_specs=(P(None, "gy", "gx"), P(None, "gy", "gx")),
        check_vma=False,
    )
```

```python
import functools
import math

import jax
import jax.numpy as jnp
from jax import lax
from jax.experimental import pallas as pl
from jax.experimental.pallas import tpu as pltpu
from jax.sharding import PartitionSpec as P

ITERS = 8
COUPLE = 0.25
DIFF_LAT = 0.5
DIFF_LON = 0.5
GUARD = 1.0
MESH = pl.DeviceIdType.MESH
HI = lax.Precision.HIGHEST

MIDDLE = 9.0
RADIUS = 6.0
WIDTH = 3.0
THETA = [MIDDLE + RADIUS * math.cos(math.pi * (2 * k + 1) / (2 * ITERS)) for k in (7, 0, 4, 2, 6, 1, 5, 3)]
PAIRS = [(k, i) for k in range(ITERS + 1) for i in range(k + 1)]
GROUP = 4
HALO = 2 * ITERS
HALF = 8
STEP = 4
WINDOWS = 3


def apply_to(coords):
    out = [None] * (len(coords) + 1)
    for k, value in enumerate(coords):
        low = THETA[k] * value if k < ITERS else value
        out[k] = low if out[k] is None else out[k] + low
        out[k + 1] = WIDTH * value
    return out


def small_solve(gram):
    first = jnp.sqrt(gram[0][0] + GUARD)
    coords = [[1.0 / first]]
    images = [[gram[i][0] * coords[0][0] for i in range(ITERS + 1)]]
    heights = []
    for j in range(ITERS):
        moved = apply_to(coords[j])
        column = []
        for i in range(j + 1):
            column.append(functools.reduce(lambda a, b: a + b, [images[i][k] * moved[k] for k in range(j + 2)]))
        left = list(moved)
        for i in range(j + 1):
            for k in range(i + 1):
                left[k] = left[k] - column[i] * coords[i][k]
        image = [
            functools.reduce(lambda a, b: a + b, [gram[r][k] * left[k] for k in range(j + 2)])
            for r in range(ITERS + 1)
        ]
        norm_sq = functools.reduce(lambda a, b: a + b, [image[k] * left[k] for k in range(j + 2)])
        subdiag = jnp.sqrt(jnp.maximum(norm_sq, 0.0) + GUARD)
        column.append(subdiag)
        heights.append(column)
        inverse = 1.0 / subdiag
        coords.append([v * inverse for v in left])
        images.append([v * inverse for v in image])
    cosines, sines, target, rotated = [], [], [first], []
    for j in range(ITERS):
        column = list(heights[j])
        for e in range(j):
            upper, lower = column[e], column[e + 1]
            column[e] = cosines[e] * upper + sines[e] * lower
            column[e + 1] = cosines[e] * lower - sines[e] * upper
        upper, lower = column[j], column[j + 1]
        radius = jnp.sqrt(upper * upper + lower * lower)
        inverse = 1.0 / radius
        cosine, sine = upper * inverse, lower * inverse
        column[j] = radius
        kept = target[j]
        target[j] = cosine * kept
        target.append(-sine * kept)
        cosines.append(cosine)
        sines.append(sine)
        rotated.append(column)
    weights = [None] * ITERS
    for j in reversed(range(ITERS)):
        value = target[j]
        for later in range(j + 1, ITERS):
            value = value - rotated[later][j] * weights[later]
        weights[j] = value / rotated[j][j]
    answer = [None] * ITERS
    for j in range(ITERS):
        for k in range(j + 1):
            term = weights[j] * coords[j][k]
            answer[k] = term if answer[k] is None else answer[k] + term
    return answer, apply_to(answer)


def distance(n, o):
    return min(o, n - o)


def peers(nx, ny):
    inner = 4 if ny % 4 == 0 else 1
    offsets = [(a, b) for a in range(nx) for b in range(ny) if (a, b) != (0, 0)]

    def hops(offset):
        a, b = offset
        return distance(nx // 2 or 1, a // 2) + distance(inner, b % inner) + distance(ny // inner, b // inner)

    return sorted(offsets, key=lambda offset: (-hops(offset), offset))


def kernel(nx, ny, f_hbm, d_hbm, c_ref, wl_hbm, wa_hbm, even, odd, splats,
           diag, coef, kxs, block, band, own, near_lat, own_w, near_lat_w, packed, near_lon, near_corner,
           gram_acc, mine, slots,
           load_sem, lat_send, lat_recv, lon_send, lon_recv, red_sem, known):
    channels, lat, lon = f_hbm.shape
    both = 2 * channels
    total = nx * ny
    f32, bf16 = jnp.float32, jnp.bfloat16
    ix, iy = lax.axis_index("gx"), lax.axis_index("gy")
    east, west = lax.rem(ix + 1, nx), lax.rem(ix + nx - 1, nx)
    scale = 1.0 / WIDTH
    size = GROUP * channels
    edge = HALO
    rows_all = lat + 2 * HALO
    tiles = lat // HALF

    def field(k):
        return even.at[k // 2] if k % 2 == 0 else odd.at[k // 2]

    barrier = pltpu.get_barrier_semaphore()

    def greet(sem, a, b):
        def signal():
            pl.semaphore_signal(sem, inc=1, device_id=(lax.rem(ix + a, nx), iy + b), device_id_type=MESH)

        if b == 0:
            signal()
        else:
            pl.when(iy + b < ny if b > 0 else iy + b >= 0)(signal)

    def line(n):
        return [(0, b) for b in range(1, n + 1)] + [(0, -b) for b in range(1, n + 1)]

    def ring(n):
        return [(a, 0) for a in range(1, n + 1)] + [(nx - a, 0) for a in range(1, n + 1)]

    close = line(1) + ring(1)
    rounds = [line(1), ring(1), line(2) + ring(2), [(0, 4), (0, -4)], [(0, 8), (0, -8)], [(a, 0) for a in range(1, nx)]]
    for a, b in close:
        greet(barrier, a, b)

    def tell(n):
        for a, b in rounds[n]:
            greet(known.at[n], a, b)

    def collect(sem, offsets):
        count = sum(1 for _, b in offsets if b == 0)
        for _, b in offsets:
            if b > 0:
                count = count + jnp.minimum(lax.div(ny - 1 - iy, b), 1) + jnp.minimum(lax.div(iy, b), 1)
        pl.semaphore_wait(sem, count)

    def hear(n):
        collect(known.at[n], rounds[n])

    winds = [pltpu.make_async_copy(wl_hbm, own_w.at[0], load_sem.at[1]), pltpu.make_async_copy(wa_hbm, own_w.at[1], load_sem.at[1])]
    for copy in winds:
        copy.start()
    for c in range(channels):
        for q, src in enumerate((f_hbm, d_hbm)):
            pltpu.make_async_copy(src.at[c], own.at[:, q * channels + c, :], load_sem.at[0]).start()

    def set_up():
        def spread(n):
            row = lax.broadcasted_iota(jnp.int32, (n, channels), 0)
            col = lax.broadcasted_iota(jnp.int32, (n, channels), 1)
            return jnp.where(lax.rem(row, channels) == col, 1.0, 0.0).astype(f32)

        wide = lax.dot_general(spread(size), c_ref[...], (((1,), (0,)), ((), ())), precision=HI, preferred_element_type=f32)
        wide = lax.dot_general(wide, spread(3 * size), (((1,), (1,)), ((), ())), precision=HI,
                               preferred_element_type=f32) * (COUPLE * scale)
        down = lax.broadcasted_iota(jnp.int32, (size, 3 * size), 0)
        across = lax.broadcasted_iota(jnp.int32, (size, 3 * size), 1)
        for k in range(ITERS):
            moved = wide - jnp.where(lax.rem(across, size) == down, THETA[k] * scale, 0.0)
            high = moved.astype(bf16).astype(f32)
            moved = jnp.where(across < 2 * size, high, moved - high)
            block[k] = jnp.where(down // channels == lax.rem(across, size) // channels, moved, 0.0).astype(bf16)
        down = lax.broadcasted_iota(jnp.int32, (256, 256), 0)
        across = lax.broadcasted_iota(jnp.int32, (256, 256), 1)
        shift = lax.rem(down, 128) - lax.rem(across, 128)
        sums = jnp.where((shift == 1) | (shift == -1), 1.0, 0.0)
        slopes = jnp.where(shift == 1, 8.0, 0.0) + jnp.where(shift == -1, -8.0, 0.0)
        slopes = slopes + jnp.where(shift == 2, -1.0, 0.0) + jnp.where(shift == -2, 1.0, 0.0)
        band[...] = jnp.where(across < 128, sums, slopes).astype(bf16)
        row_pos = (lax.broadcasted_iota(jnp.int32, (rows_all, 128), 0) + (iy * lat - edge)).astype(f32)
        phi = -math.pi / 2 + (row_pos + 0.5) * (math.pi / (lat * ny))
        kxs[...] = (DIFF_LON * scale) / (jnp.cos(phi) ** 2 + 0.1)
        gram_acc[...] = jnp.zeros(gram_acc.shape, f32)

        @pl.when(iy == 0)
        def _():
            near_lat[0] = jnp.zeros(near_lat.shape[1:], f32)
            near_lat_w[0] = jnp.zeros(near_lat_w.shape[1:], f32)
            near_corner[0] = jnp.zeros(near_corner.shape[1:], f32)
            near_corner[1] = jnp.zeros(near_corner.shape[1:], f32)

        @pl.when(iy == ny - 1)
        def _():
            near_lat[1] = jnp.zeros(near_lat.shape[1:], f32)
            near_lat_w[1] = jnp.zeros(near_lat_w.shape[1:], f32)
            near_corner[2] = jnp.zeros(near_corner.shape[1:], f32)
            near_corner[3] = jnp.zeros(near_corner.shape[1:], f32)

    def lat_copies(side, c):
        first = HALO - STEP * (c + 1) if side == 0 else STEP * c
        base = lat - HALO if side == 0 else 0
        to = (ix, iy + 1) if side == 0 else (ix, iy - 1)
        if STEP * (c + 1) < HALO:
            parts = [(first, STEP, both)]
        elif side == 0:
            parts = [(first + 2, STEP - 2, both), (first, 2, channels)]
        else:
            parts = [(first, STEP - 2, both), (first + STEP - 2, 2, channels)]
        out = []
        for start, count, subs in parts:
            out.append(pltpu.make_async_remote_copy(
                src_ref=own.at[pl.ds(base + start, count), pl.ds(0, subs), :],
                dst_ref=near_lat.at[side, pl.ds(start, count), pl.ds(0, subs), :],
                send_sem=lat_send.at[side], recv_sem=lat_recv.at[side, c], device_id=to, device_id_type=MESH))
        if c % 2 == 0:
            tile = tile_of(side, c)
            out.append(pltpu.make_async_remote_copy(
                src_ref=own_w.at[:, pl.ds(base + HALF * tile, HALF), :], dst_ref=near_lat_w.at[side, :, pl.ds(HALF * tile, HALF), :],
                send_sem=lat_send.at[side], recv_sem=lat_recv.at[side, c], device_id=to, device_id_type=MESH))
        return out

    def tile_of(side, c):
        return 1 - c // 2 if side == 0 else c // 2

    def corner_copy(side, ew, c):
        slot, tile = 2 * side + ew, tile_of(side, c)
        return pltpu.make_async_remote_copy(
            src_ref=packed.at[ew, tile + (tiles - 2 if side == 0 else 0)], dst_ref=near_corner.at[slot, tile],
            send_sem=lat_send.at[side], recv_sem=lat_recv.at[side, c],
            device_id=(east if ew == 0 else west, iy + 1 if side == 0 else iy - 1), device_id_type=MESH)

    def lon_copy(ew):
        return pltpu.make_async_remote_copy(
            src_ref=packed.at[ew], dst_ref=near_lon.at[ew], send_sem=lon_send.at[ew], recv_sem=lon_recv.at[ew],
            device_id=(east if ew == 0 else west, iy), device_id_type=MESH)

    def has(side):
        return iy < ny - 1 if side == 0 else iy > 0

    def from_side(side):
        return iy > 0 if side == 0 else iy < ny - 1

    lane = lax.broadcasted_iota(jnp.int32, (both, 128), 1)
    lane8 = lax.broadcasted_iota(jnp.int32, (8, 128), 1)

    def turn(x, n):
        n = n % 128
        return pltpu.roll(x, n, 1) if n else x

    def pack(n, _):
        for ew in range(2):
            cut = slice(lon - 128, lon) if ew == 0 else slice(0, 128)
            start = 112 if ew == 0 else 0
            base = HALF * n
            strip = turn(own[base, :, cut], -start)
            for j in range(1, HALF):
                strip = jnp.where((lane >= 16 * j) & (lane < 16 * j + 16), turn(own[base + j, :, cut], 16 * j - start), strip)
            packed[ew, n, 0:both, :] = strip
            rows = pl.ds(pl.multiple_of(base, 8), 8)
            packed[ew, n, both:both + 8, :] = jnp.where(
                lane8 < 16, turn(own_w[0, rows, cut], -start), turn(own_w[1, rows, cut], 16 - start))
        return 0

    def place_coef(e0, wl, wa, inside, chosen):
        kx = kxs[pl.ds(e0, 8), :]
        for t in chosen:
            cut = slice(128 * t, 128 * t + 128)
            l, a = wl[t] * (scale / 12.0), wa[t] * (scale / 12.0)
            planes = [-kx, l, 8.0 * a - DIFF_LAT * scale, -8.0 * a - DIFF_LAT * scale, a]
            for q, plane in enumerate(planes):
                if q == 0 and t != 1:
                    continue
                if inside is not None:
                    plane = plane * inside
                for j in range(8):
                    coef[e0 + j, q:q + 1, cut] = plane[j:j + 1, :]

    def centre(e):
        return (1.0 + 2.0 * DIFF_LAT) * scale - 2.0 * coef[e, 0:1, 128:256]

    def place_own(n, _):
        base = HALF * n
        rows = pl.ds(pl.multiple_of(base, 8), 8)
        wl, wa = ([None, turn(jnp.where(lane8 >= 64, own_w[q, rows, 0:128], own_w[q, rows, 128:256]), 64), None] for q in range(2))
        place_coef(pl.multiple_of(edge + base, 8), wl, wa, None, (1,))
        for j in range(HALF):
            r = base + j
            e = edge + r
            a, b = own[r, :, 0:128], own[r, :, 128:256]
            middle = centre(e)
            for t, piece in enumerate((turn(a, 16), turn(jnp.where(lane >= 64, a, b), 64), turn(b, 112))):
                cut = slice(128 * t, 128 * t + 128)
                even[0, e, :, cut] = piece[0:channels]
                diag[e, :, cut] = piece[channels:] * scale + middle
        return 0

    def place_lon(n, _):
        base = HALF * n
        rows = pl.ds(pl.multiple_of(base, 8), 8)
        w, e = near_lon[0, n, both:both + 8, :], near_lon[1, n, both:both + 8, :]
        wl, wa = ([jnp.where(lane8 < 16, turn(w, -16 * q), turn(own_w[q, rows, 0:128], 16)), None,
                   jnp.where(lane8 >= 112, turn(e, 112 - 16 * q), turn(own_w[q, rows, 128:256], 112))] for q in range(2))
        place_coef(pl.multiple_of(edge + base, 8), wl, wa, None, (0, 2))
        w, e = near_lon[0, n, 0:both, :], near_lon[1, n, 0:both, :]
        for j in range(HALF):
            r = edge + base + j
            middle = centre(r)
            for cut, keep, piece in ((slice(0, 128), lane < 16, turn(w, -16 * j)), (slice(256, 384), lane >= 112, turn(e, 112 - 16 * j))):
                even[0, r, :, cut] = jnp.where(keep[0:channels], piece[0:channels], even[0, r, :, cut])
                diag[r, :, cut] = jnp.where(keep[0:channels], piece[channels:] * scale + middle, diag[r, :, cut])
        return 0

    def place_halo(side, c):
        first = HALO - STEP * (c + 1) if side == 0 else STEP * c
        tile = tile_of(side, c)
        shift = 0 if side == 0 else edge + lat
        inside = jnp.where(from_side(side), 1.0, 0.0).astype(f32)

        @pl.when(from_side(side))
        def _():
            if c % 2 == 0:
                whole = coef.at[pl.ds(0, 23), :, pl.ds(0, 256)]
            elif STEP * (c + 1) < HALO:
                whole = own.at[pl.ds(0, STEP)]
            else:
                whole = own.at[pl.ds(0, 3)]
            pltpu.make_async_copy(whole, whole, lat_recv.at[side, c]).wait()

        def three(a, b, w, e, lanes, at):
            return (jnp.where(lanes < 16, turn(w, -at), turn(a, 16)), turn(jnp.where(lanes >= 64, a, b), 64),
                    jnp.where(lanes >= 112, turn(e, 112 - at), turn(b, 112)))

        west_strip, east_strip = near_corner.at[2 * side, tile], near_corner.at[2 * side + 1, tile]
        if c % 2 == 0:
            span = slice(HALF * tile, HALF * tile + 8)
            wl, wa = (three(near_lat_w[side, q, span, 0:128], near_lat_w[side, q, span, 128:256],
                            west_strip[both:both + 8, :], east_strip[both:both + 8, :], lane8, 16 * q) for q in range(2))
            place_coef(shift + HALF * tile, wl, wa, inside, range(WINDOWS))
        for j in range(STEP):
            middle = centre(shift + first + j)
            pieces = three(near_lat[side, first + j, :, 0:128], near_lat[side, first + j, :, 128:256],
                           west_strip[0:both, :], east_strip[0:both, :], lane, 16 * ((first + j) % HALF))
            for t, piece in enumerate(pieces):
                cut = slice(128 * t, 128 * t + 128)
                even[0, shift + first + j, :, cut] = piece[0:channels]
                diag[shift + first + j, :, cut] = piece[channels:] * scale + middle

    def advance(level, start, count):
        src, dst = field(level), field(level + 1)
        groups = [[start + GROUP * g + j for j in range(GROUP)] for g in range(count)]
        mixed, moved = [], []
        for picked in groups:
            stack = jnp.concatenate([src[e] for e in picked], axis=0)
            high = stack.astype(bf16)
            low = (stack - high.astype(f32)).astype(bf16)
            mixed.append(lax.dot_general(block[level], jnp.concatenate([high, low, high], axis=0), (((1,), (0,)), ((), ())),
                                         preferred_element_type=f32))
            sides = jnp.concatenate(
                [jnp.concatenate([high[:, 128 * t:128 * t + 128], low[:, 128 * t:128 * t + 128]], axis=1)
                 for t in range(WINDOWS)], axis=0)
            moved.append(lax.dot_general(sides, band[...], (((1,), (0,)), ((), ())), preferred_element_type=f32))
        for g, picked in enumerate(groups):
            for j, e in enumerate(picked):
                at = [slice(size * t + channels * j, size * t + channels * (j + 1)) for t in range(WINDOWS)]
                sums = jnp.concatenate([moved[g][a, 0:128] for a in at], axis=1)
                slopes = jnp.concatenate([moved[g][a, 128:256] for a in at], axis=1)
                kx = jnp.concatenate([coef[e, 0:1, 128:256]] * WINDOWS, axis=1)

                def weight(q):
                    return coef[e, q:q + 1, :]

                value = diag[e] * src[e] + mixed[g][channels * j:channels * (j + 1)]
                value = value + (kx * sums + weight(1) * slopes)
                value = value + weight(2) * src[e + 1] + weight(3) * src[e - 1]
                dst[e] = value + weight(4) * (src[e - 2] - src[e + 2])

    def interior():
        for k in range(ITERS - 1):
            count = (lat - 4 - 4 * k) // GROUP
            for g in range(0, count, 2):
                advance(k, edge + 2 + 2 * k + GROUP * g, min(2, count - g))

    def wedge(c):
        for k in range(ITERS):
            low = edge - STEP * (c + 1) + 2 + 2 * k
            for e0 in (low, rows_all - STEP - low):
                advance(k, e0, STEP // GROUP)

    def dots(c):
        for k in range(ITERS + 1):
            last = [p for p in range(lat // 4) if k <= p + 2 * (c + 1) and (c < 0 or k > p + 2 * c)]
            pairs = [e for p in last for e in (edge + 2 * p, edge + lat - 2 - 2 * p)]
            if not pairs:
                continue
            for group, low in (((0, 2), 16), ((1,), 32)):
                acc = [None] * (k + 1)
                for e in pairs:
                    for t in group:
                        x = [field(i)[e:e + 2, :, 128 * t:128 * t + 128] for i in range(k + 1)]
                        for i in range(k + 1):
                            term = x[k] * x[i]
                            acc[i] = term if acc[i] is None else acc[i] + term
                kept = (lane8 >= low) & (lane8 < 128 - low)
                for i in range(k + 1):
                    at = k * (k + 1) // 2 + i
                    value = acc[i][0] + acc[i][1]
                    gram_acc[at] = gram_acc[at] + jnp.where(kept, value[0:8] + value[8:16], 0.0)

    pltpu.make_async_copy(own_w, own_w, load_sem.at[1]).wait()
    pltpu.make_async_copy(own, own, load_sem.at[0]).wait()
    collect(barrier, close)
    tell(0)
    tell(1)

    def send_lat(c):
        for side in range(2):
            @pl.when(has(side))
            def _():
                for copy in lat_copies(side, c):
                    copy.start()

    def send_corners(c):
        for side in range(2):
            @pl.when(has(side))
            def _():
                for ew in range(2):
                    corner_copy(side, ew, c).start()

    send_lat(0)
    lax.fori_loop(0, tiles, pack, 0)
    for ew in range(2):
        lon_copy(ew).start()
    set_up()
    hear(0)
    send_corners(0)
    send_lat(1)
    send_lat(2)
    send_corners(2)
    send_lat(3)
    lax.fori_loop(0, tiles, place_own, 0)
    hear(1)
    tell(2)
    for ew in range(2):
        lon_copy(ew).wait_recv()
    lax.fori_loop(0, tiles, place_lon, 0)
    interior()
    hear(2)
    tell(3)
    dots(-1)
    for c in range(HALO // STEP):
        for side in range(2):
            place_halo(side, c)
        wedge(c)
        dots(c)
        if c == 0:
            hear(3)
            tell(4)
        if c == 2:
            hear(4)
            tell(5)
    hear(5)
    sums = jnp.concatenate(
        [jnp.sum(gram_acc[n], axis=0, keepdims=True) for n in range(len(PAIRS))]
        + [jnp.zeros((128 - len(PAIRS), 128), f32)], axis=0)
    flat = lax.dot_general(jnp.ones((8, 128), f32), sums, (((1,), (1,)), ((), ())), precision=HI,
                           preferred_element_type=f32)
    mine[...] = flat[0:1, :]
    slots[total - 1] = flat[0:1, :]

    for n, (a, b) in enumerate(peers(nx, ny)):
        pltpu.make_async_remote_copy(
            src_ref=mine, dst_ref=slots.at[n], send_sem=red_sem.at[0], recv_sem=red_sem.at[1],
            device_id=(lax.rem(ix + a, nx), lax.rem(iy + b, ny)), device_id_type=MESH).start()
    arrived = slots.at[pl.ds(0, total - 1)]
    pltpu.make_async_copy(arrived, arrived, red_sem.at[1]).wait()
    pltpu.make_async_copy(arrived, arrived, red_sem.at[0]).wait()
    parts = [slots[n] for n in range(4)]
    for n in range(4, total):
        parts[n % 4] = parts[n % 4] + slots[n]
    whole = (parts[0] + parts[1]) + (parts[2] + parts[3])
    gram = [[None] * (ITERS + 1) for _ in range(ITERS + 1)]
    for n, (k, i) in enumerate(PAIRS):
        gram[k][i] = gram[i][k] = jnp.broadcast_to(whole[:, n:n + 1], (8, 128))
    answer, applied = small_solve(gram)
    for k in range(ITERS):
        splats[k] = answer[k]
    for k in range(ITERS + 1):
        splats[ITERS + k] = applied[k]

    for ew in range(2):
        lon_copy(ew).wait_send()
    for side in range(2):
        @pl.when(has(side))
        def _():
            whole = even.at[0, pl.ds(0, 37), :, pl.ds(0, 256)]
            pltpu.make_async_copy(whole, whole, lat_send.at[side]).wait()


def finish(even, odd, splats, sol_hbm, res_hbm, outs, out_sem):
    channels, lat, _ = sol_hbm.shape
    lane = lax.broadcasted_iota(jnp.int32, (8, 128), 1)
    quarter = lat // 4
    for r in range(lat):
        for h in range(channels // 8):
            sub = slice(8 * h, 8 * h + 8)
            best, rest = [], []
            for t in range(WINDOWS):
                cut = slice(128 * t, 128 * t + 128)
                x = even[0, HALO + r, sub, cut]
                up = splats[0] * x
                down = x - splats[ITERS] * x
                for k in range(1, ITERS + 1):
                    x = (odd if k % 2 else even)[k // 2, HALO + r, sub, cut]
                    if k < ITERS:
                        up = up + splats[k] * x
                    down = down - splats[ITERS + k] * x
                best.append(up)
                rest.append(down)
            for q, (a, b, c) in enumerate((best, rest)):
                b = pltpu.roll(b, 64, 1)
                spread = pl.ds(8 * h * lat + r, 8, stride=lat)
                outs[q, 0, spread, :] = jnp.where(lane < 96, pltpu.roll(a, 112, 1), b)
                outs[q, 1, spread, :] = jnp.where(lane < 32, b, pltpu.roll(c, 16, 1))
        if (r + 1) % quarter == 0:
            rows = pl.ds(r + 1 - quarter, quarter)
            for q, dst in enumerate((sol_hbm, res_hbm)):
                for t in range(2):
                    src = outs.at[q, t].reshape(channels, lat, 128)
                    pltpu.make_async_copy(src.at[:, rows, :], dst.at[:, rows, pl.ds(128 * t, 128)], out_sem.at[q]).start()
    for q, dst in enumerate((sol_hbm, res_hbm)):
        pltpu.make_async_copy(dst, dst, out_sem.at[q]).wait()


def solution(mesh):
    nx, ny = mesh.shape["gx"], mesh.shape["gy"]

    def per_device(forcing, damping, coupling, wind_lon, wind_lat):
        channels, lat, lon = forcing.shape
        f32 = jnp.float32
        vmem = pl.BlockSpec(memory_space=pltpu.VMEM)
        hbm = pl.BlockSpec(memory_space=pltpu.HBM)
        dma = pltpu.SemaphoreType.DMA
        shape = jax.ShapeDtypeStruct((channels, lat, lon), f32)
        rows_all, lanes = lat + 2 * HALO, 128 * WINDOWS
        packed = 2 * channels + 8
        even, odd, splats = pl.pallas_call(
            functools.partial(kernel, nx, ny),
            out_shape=(
                pltpu.VMEM((ITERS // 2 + 1, rows_all, channels, lanes), f32),
                pltpu.VMEM((ITERS // 2, rows_all, channels, lanes), f32),
                pltpu.VMEM((2 * ITERS + 1, 8, 128), f32),
            ),
            in_specs=[hbm, hbm, vmem, hbm, hbm],
            out_specs=(vmem, vmem, vmem),
            scratch_shapes=[
                pltpu.VMEM((rows_all, channels, lanes), f32),
                pltpu.VMEM((rows_all, 8, lanes), f32),
                pltpu.VMEM((rows_all, 128), f32),
                pltpu.VMEM((ITERS, GROUP * channels, 3 * GROUP * channels), jnp.bfloat16),
                pltpu.VMEM((256, 256), jnp.bfloat16),
                pltpu.VMEM((lat, 2 * channels, lon), f32),
                pltpu.VMEM((2, HALO, 2 * channels, lon), f32),
                pltpu.VMEM((2, lat, lon), f32),
                pltpu.VMEM((2, 2, HALO, lon), f32),
                pltpu.VMEM((2, lat // HALF, packed, 128), f32),
                pltpu.VMEM((2, lat // HALF, packed, 128), f32),
                pltpu.VMEM((4, 2, packed, 128), f32),
                pltpu.VMEM((len(PAIRS), 8, 128), f32),
                pltpu.VMEM((1, 128), f32),
                pltpu.VMEM((nx * ny, 1, 128), f32),
                dma((2,)),
                dma((2,)), dma((2, HALO // STEP)), dma((2,)), dma((2,)), dma((2,)),
                pltpu.SemaphoreType.REGULAR((6,)),
            ],
            compiler_params=pltpu.CompilerParams(
                collective_id=0, has_side_effects=True, vmem_limit_bytes=52_800_000),
        )(forcing, damping, coupling, wind_lon, wind_lat)
        return pl.pallas_call(
            finish,
            out_shape=(shape, shape),
            in_specs=[vmem, vmem, vmem],
            out_specs=(hbm, hbm),
            scratch_shapes=[pltpu.VMEM((2, 2, channels * lat, 128), f32), dma((2,))],
            compiler_params=pltpu.CompilerParams(vmem_limit_bytes=16 * 1024 * 1024),
        )(even, odd, splats)

    return jax.shard_map(
        per_device,
        mesh=mesh,
        in_specs=(P(None, "gy", "gx"), P(None, "gy", "gx"), P(), P("gy", "gx"), P("gy", "gx")),
        out_specs=(P(None, "gy", "gx"), P(None, "gy", "gx")),
        check_vma=False,
    )
```
